32 devices in a mesh: dp: 16 (over z, y, x), seq: 2 (over core).
Axes of the slice: x: 2, y: 2, z: 4, core: 2. Of those that a mesh axis runs over, the one named last changes fastest.
Arguments:
- tokens: bfloat16 [16, 1024, 768], P('dp', 'seq'), may hold values from -6 to 6
- segment_ids: int32 [16, 1024], P('dp', 'seq'), may hold values from 0 to 7, never falling along the last dimension, each value on 1 to 512 neighbouring positions
- norm1_gain: bfloat16 [768], replicated, may hold values from 0.25 to 1.75
- w_query: bfloat16 [768, 768], replicated, may hold values from -0.21875 to 0.21875
- w_key: bfloat16 [768, 768], replicated, may hold values from -0.21875 to 0.21875
- w_value: bfloat16 [768, 768], replicated, may hold values from -0.21875 to 0.21875
- w_out: bfloat16 [768, 768], replicated, may hold values from -0.875 to 0.875
- norm2_gain: bfloat16 [768], replicated, may hold values from 0.25 to 1.75
- w_gate: bfloat16 [768, 2048], replicated, may hold values from -0.21875 to 0.21875
- w_up: bfloat16 [768, 2048], replicated, may hold values from -0.21875 to 0.21875
- w_down: bfloat16 [2048, 768], replicated, may hold values from -0.125 to 0.125
- out_grad: bfloat16 [16, 1024, 768], P('dp', 'seq'), may hold values from -6 to 6
Outputs:
- block_out: bfloat16 [16, 1024, 768], P('dp', 'seq')
- input_grad: bfloat16 [16, 1024, 768], P('dp', 'seq')
- norm1_gain_grad: float32 [768], P(('dp', 'seq'))
- query_grad: float32 [768, 768], P(None, ('dp', 'seq'))
- key_grad: float32 [768, 768], P(None, ('dp', 'seq'))
- value_grad: float32 [768, 768], P(None, ('dp', 'seq'))
- out_proj_grad: float32 [768, 768], P(None, ('dp', 'seq'))
- norm2_gain_grad: float32 [768], P(('dp', 'seq'))
- gate_grad: float32 [768, 2048], P(None, ('dp', 'seq'))
- up_grad: float32 [768, 2048], P(None, ('dp', 'seq'))
- down_grad: float32 [2048, 768], P(None, ('dp', 'seq'))
The draws below stay inside these ranges and needn't reach their ends.
Inputs may be any that keep to these rules, and one draw needn't show every extreme that they name: `segment_ids`: in each sequence the ids never fall and each of the 8 ids marks one document of 1 to 512 tokens; some document has exactly 512.
All inputs are finite; a program needn't handle non-finite values.
Results may differ from the reference program's by a relative error of at most 0.013.
Values may be sent and summed in bfloat16 or wider, within the bound.
A program may use at most 192 MiB of HBM per device.

```python
import math
import jax
import jax.numpy as jnp
import numpy as np
from jax import lax

D = 768
H = 12
HD = 64
FF = 2048
L = 1024
DOCS = 8
B = 16
DOC_MOST = 512


def with_spikes(drawn, stream_key, source, target, blocks, factor):
    def block_of(axis_at):
        return (jnp.arange(drawn.shape[axis_at]) // (drawn.shape[axis_at] // blocks)).reshape((-1,) + (1,) * (drawn.ndim - 1 - axis_at))

    one_side = jax.random.permutation(stream_key, blocks)[block_of(target)]
    far = (block_of(target) + blocks // 2) % blocks
    return jnp.where((block_of(source) == one_side) | (block_of(source) == far), factor * drawn, drawn)


def shard_levels(own_key, dims, cuts, low, largest):
    loudness = 1.0
    for position, blocks in cuts:
        heights = jax.random.uniform(jax.random.fold_in(jax.random.fold_in(own_key, 6), position), (blocks,), jnp.float32, low / len(cuts), largest / len(cuts))
        loudness = loudness * jnp.repeat(jnp.exp(heights), dims[position] // blocks).reshape((-1,) + (1,) * (len(dims) - 1 - position))
    return loudness


def split_up(number_of, total, most, lean):
    weights = [(1 << 20) // math.isqrt(grade ** lean) + 1 for grade in range(2, number_of + 1)]
    surplus, given = total - most - (number_of - 1), [1] * (number_of - 1)
    while surplus > 0:
        free = [i for i in range(number_of - 1) if given[i] < most]
        whole, remaining = sum([weights[i] for i in free]), surplus
        for i in free:
            more = min(most - given[i], max(1, remaining * weights[i] // whole), surplus)
            given[i] = given[i] + more
            surplus = surplus - more
    return np.array([most] + given)


def ragged(key, number_of, total, bound, lean):
    if number_of == 2:
        one = jax.random.randint(key, (), max(1, total - bound), min(bound, total - 1) + 1)
        return jnp.stack([one, total - one])
    lengths = jnp.asarray(split_up(number_of, total, bound, lean), jnp.int32)
    twos = (number_of - 1) // 2
    giver, sink = lengths[1:1 + 2 * twos:2], lengths[2:2 + 2 * twos:2]
    margin = jnp.minimum(giver - 1, bound - sink)
    passed = jax.random.randint(jax.random.fold_in(key, 1), (twos,), 0, 1 << 20) % (margin + 1)
    lengths = lengths.at[1:1 + 2 * twos:2].set(giver - passed).at[2:2 + 2 * twos:2].set(sink + passed)
    return lengths[jax.random.permutation(jax.random.fold_in(key, 2), number_of)]


def normal_values(key, shape, deviation, bound, cuts=(), held_as=jnp.bfloat16):
    values = deviation * jax.random.normal(key, shape, jnp.float32)
    if cuts:
        values = values * shard_levels(key, shape, cuts, -0.22, 0.18)
    return jnp.clip(values, -bound, bound).astype(held_as)


def heavy_noise(rng, shape, width, limit, pieces, heavy, held_as=jnp.bfloat16):
    drawn = width * jax.random.normal(rng, shape, jnp.float32)
    if pieces:
        drawn = drawn * shard_levels(rng, shape, pieces, -0.22, 0.18)
    return jnp.clip(with_spikes(drawn, jax.random.fold_in(rng, 3), *heavy), -limit, limit).astype(held_as)


def setup_inputs(seed: int = 0) -> dict:
    key_list = jax.random.split(jax.random.key(seed), 13)
    tokens = normal_values(key_list[0], (B, L, D), 1.0, 6.0, ((0, 16), (1, 2)))
    segment_ids = jax.vmap(lambda own: jnp.searchsorted(jnp.cumsum(ragged(own, DOCS, L, DOC_MOST, 2)), jnp.arange(L), side="right"))(jax.random.split(key_list[1], B)).reshape((B, L)).astype(jnp.int32)
    norm1_gain = jnp.clip(1.0 + 0.15 * jax.random.normal(key_list[2], (D,), jnp.float32), 0.25, 1.75).astype(jnp.bfloat16)
    w_query = normal_values(key_list[3], (D, D), D ** -0.5, 0.21875)
    w_key = normal_values(key_list[4], (D, D), D ** -0.5, 0.21875)
    w_value = normal_values(key_list[5], (D, D), D ** -0.5, 0.21875)
    w_out = normal_values(key_list[6], (D, D), (D // 16) ** -0.5, 0.875)
    norm2_gain = jnp.clip(1.0 + 0.15 * jax.random.normal(key_list[7], (D,), jnp.float32), 0.25, 1.75).astype(jnp.bfloat16)
    w_gate = normal_values(key_list[8], (D, FF), D ** -0.5, 0.21875)
    w_up = normal_values(key_list[9], (D, FF), D ** -0.5, 0.21875)
    w_down = normal_values(key_list[10], (FF, D), FF ** -0.5, 0.125)
    out_grad = heavy_noise(key_list[11], (B, L, D), 1.0, 6.0, ((0, 16), (1, 2)), (0, 2, 16, 2.0))
    return {"tokens": tokens, "segment_ids": segment_ids, "norm1_gain": norm1_gain, "w_query": w_query, "w_key": w_key, "w_value": w_value, "w_out": w_out, "norm2_gain": norm2_gain, "w_gate": w_gate, "w_up": w_up, "w_down": w_down, "out_grad": out_grad}


EPS = 1e-06
SCALE = 0.125
NEG = -1e+30
BASE = 10000.0

@jax.custom_vjp
def low(v):
    return lax.optimization_barrier(v.astype(jnp.bfloat16)).astype(jnp.float32)

@jax.custom_vjp
def low_back(v):
    return v

def low_keep(v):
    return (low(v), None)

def low_pass(kept, grad):
    return (grad,)

def back_keep(v):
    return (v, None)

def back_low(kept, grad):
    return (low(grad),)
low.defvjp(low_keep, low_pass)
low_back.defvjp(back_keep, back_low)

def matmul(left, right):
    return jnp.dot(left, right, precision=lax.Precision.HIGHEST, preferred_element_type=jnp.float32)

def rms_norm(values, gain):
    return values * lax.rsqrt(lax.optimization_barrier(jnp.mean(values * values, axis=-1, keepdims=True)) + EPS) * gain

def rope_tables(seg_row, doc_count, head_size):
    length = seg_row.shape[0]
    onehot = (seg_row[:, None] == jnp.arange(doc_count, dtype=jnp.int32)[None, :]).astype(jnp.int32)
    counts = lax.optimization_barrier(jnp.sum(onehot, axis=0))
    starts = jnp.cumsum(counts) - counts
    first_index = lax.optimization_barrier(jnp.sum(onehot * starts[None, :], axis=1))
    places = (jnp.arange(length, dtype=jnp.int32) - first_index).astype(jnp.float32)
    freqs = BASE ** (-jnp.arange(head_size // 2, dtype=jnp.float32) * (2.0 / head_size))
    angles = places[:, None] * freqs[None, :]
    return (jnp.cos(angles), jnp.sin(angles))

def rotate(heads, cosine, sine_table):
    half_size = heads.shape[-1] // 2
    lower_half = heads[..., :half_size]
    upper_half = heads[..., half_size:]
    cos_wide = cosine[:, None, :]
    sin_wide = sine_table[:, None, :]
    return jnp.concatenate([lower_half * cos_wide - upper_half * sin_wide, upper_half * cos_wide + lower_half * sin_wide], axis=-1)

def layer(values, seg_row, gain_first, w_query, w_key, w_value, w_out, gain_second, w_gate, w_up, w_down):
    length = values.shape[0]
    normed1 = low(rms_norm(values, gain_first))
    query_proj = low_back(low(matmul(normed1, w_query)))
    key_proj = low_back(low(matmul(normed1, w_key)))
    value_proj = low_back(low(matmul(normed1, w_value)))
    cosine, sine_table = rope_tables(seg_row, DOCS, HD)
    q_rot = low(rotate(query_proj.reshape(length, H, HD), cosine, sine_table))
    k_rot = low(rotate(key_proj.reshape(length, H, HD), cosine, sine_table))
    v_heads = value_proj.reshape(length, H, HD)
    places = jnp.arange(length, dtype=jnp.int32)
    allowed = (seg_row[:, None] == seg_row[None, :]) & (places[:, None] >= places[None, :])
    scores = low_back(jnp.einsum('qhd,khd->hqk', q_rot, k_rot, precision=lax.Precision.HIGHEST) * SCALE)
    scores = jnp.where(allowed[None], scores, NEG)
    attn_probs = low(jax.nn.softmax(scores, axis=-1))
    attended = jnp.einsum('hqk,khd->qhd', attn_probs, v_heads, precision=lax.Precision.HIGHEST).reshape(length, H * HD)
    attended = low_back(low(attended))
    residual = values + low_back(matmul(attended, w_out))
    normed2 = low(rms_norm(residual, gain_second))
    gate_proj = low_back(matmul(normed2, w_gate))
    up_proj = low_back(matmul(normed2, w_up))
    hidden = low(jax.nn.silu(gate_proj) * up_proj)
    return residual + matmul(hidden, w_down)

def reference(tokens, segment_ids, norm1_gain, w_query, w_key, w_value, w_out, norm2_gain, w_gate, w_up, w_down, out_grad):
    params = tuple((weight.astype(jnp.float32) for weight in (norm1_gain, w_query, w_key, w_value, w_out, norm2_gain, w_gate, w_up, w_down)))

    def one_row(totals, packed):
        row_tokens, seg_row, row_grad = packed

        def forward(values, *weights):
            return layer(values, seg_row, *weights)
        result, pullback = jax.vjp(forward, row_tokens.astype(jnp.float32), *params)
        grads = pullback(row_grad.astype(jnp.float32))
        totals = tuple((summed + added for summed, added in zip(totals, grads[1:])))
        return (totals, (result.astype(jnp.bfloat16), grads[0].astype(jnp.bfloat16)))
    zeros = tuple((jnp.zeros_like(weight) for weight in params))
    totals, outputs = lax.scan(one_row, zeros, (tokens, segment_ids, out_grad))
    return (outputs[0], outputs[1], totals[0], totals[1], totals[2], totals[3], totals[4], totals[5], totals[6], totals[7], totals[8])
```

```python
import functools

import jax
import jax.numpy as jnp
import numpy as np
from jax import lax
from jax.experimental import pallas as pl
from jax.experimental.pallas import tpu as pltpu
from jax.sharding import PartitionSpec as P

HD = 64
EPS = 1e-06
SCALE = 0.125
NEG = -1e30
BASE = 10000.0
AX = ("dp", "seq")
BF = jnp.bfloat16
F32 = jnp.float32
TB = 256
LANES = 128


def nn(a, b):
    return lax.dot_general(a, b, (((1,), (0,)), ((), ())), preferred_element_type=F32)


def nt(a, b):
    return lax.dot_general(a, b, (((1,), (1,)), ((), ())), preferred_element_type=F32)


def tn(a, b):
    return lax.dot_general(a, b, (((0,), (0,)), ((), ())), preferred_element_type=F32)


def small_tables(length):
    freqs = BASE ** (-np.arange(HD // 2, dtype=np.float64) * (2.0 / HD))
    lane_freqs = np.tile(freqs, 4)[None, :]
    fine = np.arange(64, dtype=np.float64)[:, None] * lane_freqs
    coarse = 64.0 * np.arange(length // 64, dtype=np.float64)[:, None] * lane_freqs
    return tuple(
        np.asarray(t, np.float32) for t in (np.cos(fine), np.sin(fine), np.cos(coarse), np.sin(coarse))
    )


def angle_block(tables, sub):
    cos_f, sin_f, cos_c, sin_c = tables
    ca = cos_c[pl.ds(sub, 1), :]
    sa = sin_c[pl.ds(sub, 1), :]
    cb = cos_f[...]
    sb = sin_f[...]
    low_half = (lax.broadcasted_iota(jnp.int32, (64, LANES), 1) % HD) < HD // 2
    cosine = ca * cb - sa * sb
    sine = sa * cb + ca * sb
    return cosine, jnp.where(low_half, -sine, sine), low_half


def rotate(v, cosine, sine, low_half):
    partner = jnp.where(low_half, pltpu.roll(v, LANES - HD // 2, 1), pltpu.roll(v, HD // 2, 1))
    return v * cosine + partner * sine


def window(block):
    return max(0, (block - 2) * TB)


def bias_of(seg_col, seg_row, block):
    first = window(block)
    keys = (block + 1) * TB - first
    rows = seg_col[pl.ds(block * TB, TB), :]
    cols = seg_row[:, pl.ds(first, keys)]
    q_at = block * TB + lax.broadcasted_iota(jnp.int32, (TB, keys), 0)
    k_at = first + lax.broadcasted_iota(jnp.int32, (TB, keys), 1)
    return jnp.where((rows == cols) & (k_at <= q_at), 0.0, NEG).astype(F32)


def forward_attention(
    core, own_ref, other_ref, gain_ref, wq_ref, wk_ref, wv_ref, cos_f, sin_f, cos_c, sin_c, seg_col, seg_row,
    normed_ref, q_ref, k_ref, v_ref, att_ref, lse_ref, bias_ref,
):
    s = core[0]
    half_tokens, width = own_ref.shape
    length = 2 * half_tokens
    cols = wq_ref.shape[1]
    tables = (cos_f, sin_f, cos_c, sin_c)

    def project(t, carry):
        rows = pl.ds(pl.multiple_of(t * TB, TB), TB)
        part = t // (half_tokens // TB)
        local = pl.ds(pl.multiple_of((t % (half_tokens // TB)) * TB, TB), TB)
        x = jnp.where(part == s, own_ref[local, :], other_ref[local, :]).astype(F32)
        r = lax.rsqrt(jnp.mean(x * x, axis=-1, keepdims=True) + EPS)
        normed = (x * r * gain_ref[...]).astype(BF)
        normed_ref[rows, :] = normed
        v_ref[rows, :] = nn(normed, wv_ref[...]).astype(BF)
        q = nn(normed, wq_ref[...]).astype(BF).astype(F32)
        k = nn(normed, wk_ref[...]).astype(BF).astype(F32)
        for sub in range(TB // 64):
            cosine, sine, low_half = angle_block(tables, t * (TB // 64) + sub)
            at = pl.ds(pl.multiple_of(t * TB + sub * 64, 64), 64)
            for tile in range(cols // LANES):
                lanes = slice(tile * LANES, (tile + 1) * LANES)
                part_rows = slice(sub * 64, (sub + 1) * 64)
                q_ref[at, lanes] = (rotate(q[part_rows, lanes], cosine, sine, low_half).astype(BF) * BF(SCALE)).astype(BF)
                k_ref[at, lanes] = rotate(k[part_rows, lanes], cosine, sine, low_half).astype(BF)
        return carry

    lax.fori_loop(0, length // TB, project, 0)

    for block in range(length // TB):
        first = window(block)
        keys = (block + 1) * TB - first
        bias_ref[:, :keys] = bias_of(seg_col, seg_row, block)
        rows = pl.ds(block * TB, TB)
        span = pl.ds(first, keys)

        def head(h, carry):
            lanes = pl.ds(pl.multiple_of((h // 2) * LANES, LANES), LANES)
            lane = lax.broadcasted_iota(jnp.int32, (1, LANES), 1)
            mine = (lane // HD) == (h % 2)
            q = q_ref[rows, lanes]
            qm = jnp.where(mine, q, jnp.zeros_like(q))
            scores = nt(qm, k_ref[span, lanes]) + bias_ref[:, :keys]
            peak = jnp.max(scores, axis=-1, keepdims=True)
            weights = jnp.exp(scores - peak)
            total = jnp.sum(weights, axis=-1, keepdims=True)
            probs = (weights * (1.0 / total)).astype(BF)
            result = nn(probs, v_ref[span, lanes]).astype(BF)
            att_ref[rows, lanes] = jnp.where(mine, result, att_ref[rows, lanes])
            lse_ref[rows, :] = jnp.where(lane == h, peak + jnp.log(total), lse_ref[rows, :])
            return carry

        lax.fori_loop(0, cols // HD, head, 0)


def feed_forward(
    core, slots_a, slots_b, own_ref, other_ref, att_own, att_other, gain_ref, wo_ref, wg_ref, wu_ref, wd_ref,
    dy_own, dy_other,
    res_ref, out_keep, out_send, dn_ref, pack_ref, normed, hidden, d_gate, d_up, dy_all,
):
    s = core[0]
    half_tokens, width = own_ref.shape
    length = 2 * half_tokens
    cols = att_own.shape[1]
    own_rows = pl.ds(pl.multiple_of(s * cols, cols), cols)
    other_rows = pl.ds(pl.multiple_of((1 - s) * cols, cols), cols)

    def block(t, carry):
        rows = pl.ds(pl.multiple_of(t * TB, TB), TB)
        part = t // (half_tokens // TB)
        local = pl.ds(pl.multiple_of((t % (half_tokens // TB)) * TB, TB), TB)
        is_own = part == s
        x = jnp.where(is_own, own_ref[local, :], other_ref[local, :]).astype(F32)
        dy = jnp.where(is_own, dy_own[local, :], dy_other[local, :])
        dy_all[rows, :] = dy
        residual = x + (nn(att_own[rows, :], wo_ref[own_rows, :]) + nn(att_other[rows, :], wo_ref[other_rows, :]))
        res_ref[rows, :] = residual
        r = lax.rsqrt(jnp.mean(residual * residual, axis=-1, keepdims=True) + EPS)
        n2 = (residual * r * gain_ref[...]).astype(BF)
        normed[rows, :] = n2
        gate = nn(n2, wg_ref[...])
        up = nn(n2, wu_ref[...])
        sig = 1.0 / (1.0 + jnp.exp(-gate))
        act = gate * sig
        hid = (act * up).astype(BF)
        hidden[rows, :] = hid
        down = nn(hid, wd_ref[...])

        @pl.when(is_own)
        def _():
            out_keep[local, :] = residual + down

        @pl.when(jnp.logical_not(is_own))
        def _():
            out_send[local, :] = down.astype(BF)

        d_hidden = nt(dy, wd_ref[...])
        dg = (d_hidden * up * (sig * (1.0 + gate * (1.0 - sig)))).astype(BF)
        du = (d_hidden * act).astype(BF)
        d_gate[rows, :] = dg
        d_up[rows, :] = du
        dn_ref[rows, :] = (nt(dg, wg_ref[...]) + nt(du, wu_ref[...])).astype(BF)
        return carry

    lax.fori_loop(0, length // TB, block, 0)

    wide = wg_ref.shape[1] // 8
    pieces = width // LANES

    def gate_up(o, carry):
        cut = pl.ds(pl.multiple_of(o * wide, wide), wide)
        slot = slots_b[o]
        for which, source in ((0, d_gate), (1, d_up)):
            grad = tn(source[:, cut], normed[...]).astype(BF)
            for piece in range(pieces):
                pack_ref[slot, pl.ds((which * pieces + piece) * wide, wide), :] = grad[:, piece * LANES : (piece + 1) * LANES]
        return carry

    lax.fori_loop(0, 8, gate_up, 0)
    low = width // 16
    base = 2 * pieces * wide
    deep = hidden.shape[1] // LANES
    for piece in range(deep):
        grad = tn(dy_all[...], hidden[:, piece * LANES : (piece + 1) * LANES]).astype(BF)
        for o in range(16):
            slot = slots_a[o]
            at = pl.multiple_of(base + (slot % 2) * (deep * low) + piece * low, 16)
            pack_ref[slot // 2, pl.ds(at, low), :] = grad[o * low : (o + 1) * low, :]


def backward_attention(
    core, slots_a, slots_b, own_ref, other_ref, gain_one, gain_two, wq_ref, wk_ref, wv_ref, wo_ref, dy_own, dy_other,
    res_ref, dn_own, dn_other, att_ref, normed_ref, q_ref, k_ref, v_ref, lse_ref, cos_f, sin_f, cos_c, sin_c, seg_col, seg_row,
    d_res, dn_keep, dn_send, pack_ref, d_branch, d_att, dq, dk, dv, dq_low, dk_low, dv_low, gains, bias_ref,
):
    s = core[0]
    half_tokens, width = own_ref.shape
    length = 2 * half_tokens
    cols = att_ref.shape[1]
    tables = (cos_f, sin_f, cos_c, sin_c)
    gains[...] = jnp.zeros_like(gains)

    def norm_two(t, carry):
        rows = pl.ds(pl.multiple_of(t * TB, TB), TB)
        part = t // (half_tokens // TB)
        local = pl.ds(pl.multiple_of((t % (half_tokens // TB)) * TB, TB), TB)
        is_own = part == s
        dy = jnp.where(is_own, dy_own[local, :], dy_other[local, :]).astype(F32)
        residual = res_ref[rows, :]
        dn = dn_own[rows, :].astype(F32) + dn_other[rows, :].astype(F32)
        r = lax.rsqrt(jnp.mean(residual * residual, axis=-1, keepdims=True) + EPS)
        scaled = residual * r
        e = gain_two[...] * dn
        gains[0:1, :] += jnp.sum(dn * scaled, axis=0, keepdims=True)
        grad = dy + r * (e - scaled * (r * jnp.mean(e * residual, axis=-1, keepdims=True)))
        low = grad.astype(BF)
        d_branch[rows, :] = low

        @pl.when(is_own)
        def _():
            d_res[local, :] = grad

        d_att[rows, :] = nt(low, wo_ref[...]).astype(BF)
        return carry

    lax.fori_loop(0, length // TB, norm_two, 0)

    dk[...] = jnp.zeros_like(dk)
    dv[...] = jnp.zeros_like(dv)
    for block in range(length // TB):
        first = window(block)
        keys = (block + 1) * TB - first
        bias_ref[:, :keys] = bias_of(seg_col, seg_row, block)
        rows = pl.ds(block * TB, TB)
        span = pl.ds(first, keys)

        def head(h, carry):
            lanes = pl.ds(pl.multiple_of((h // 2) * LANES, LANES), LANES)
            lane = lax.broadcasted_iota(jnp.int32, (1, LANES), 1)
            mine = (lane // HD) == (h % 2)
            q = q_ref[rows, lanes]
            qm = jnp.where(mine, q, jnp.zeros_like(q))
            do = d_att[rows, lanes]
            dom = jnp.where(mine, do, jnp.zeros_like(do))
            lse = jnp.sum(jnp.where(lane == h, lse_ref[rows, :], 0.0), axis=-1, keepdims=True)
            k = k_ref[span, lanes]
            probs = jnp.exp(nt(qm, k) + (bias_ref[:, :keys] - lse))
            d_probs = nt(dom, v_ref[span, lanes])
            delta = jnp.sum(probs * d_probs, axis=-1, keepdims=True)
            ds = (probs * (d_probs - delta)).astype(BF)
            part = nn(ds, k)
            dq[rows, lanes] = jnp.where(mine, part, dq[rows, lanes])
            dk[span, lanes] += tn(ds, qm)
            dv[span, lanes] += tn(probs.astype(BF), dom)
            return carry

        lax.fori_loop(0, cols // HD, head, 0)

    def finish(t, carry):
        rows = pl.ds(pl.multiple_of(t * TB, TB), TB)
        part = t // (half_tokens // TB)
        local = pl.ds(pl.multiple_of((t % (half_tokens // TB)) * TB, TB), TB)
        is_own = part == s
        for sub in range(TB // 64):
            cosine, sine, low_half = angle_block(tables, t * (TB // 64) + sub)
            at = pl.ds(pl.multiple_of(t * TB + sub * 64, 64), 64)
            for tile in range(cols // LANES):
                lanes = slice(tile * LANES, (tile + 1) * LANES)
                dq_low[at, lanes] = (rotate(dq[at, lanes], cosine, -sine, low_half) * SCALE).astype(BF)
                dk_low[at, lanes] = rotate(dk[at, lanes], cosine, -sine, low_half).astype(BF)
        dv_low[rows, :] = dv[rows, :].astype(BF)
        dn = nt(dq_low[rows, :], wq_ref[...]) + nt(dk_low[rows, :], wk_ref[...]) + nt(dv_low[rows, :], wv_ref[...])
        x = jnp.where(is_own, own_ref[local, :], other_ref[local, :]).astype(F32)
        r = lax.rsqrt(jnp.mean(x * x, axis=-1, keepdims=True) + EPS)
        gains[1:2, :] += jnp.sum(dn * (x * r), axis=0, keepdims=True)

        @pl.when(is_own)
        def _():
            dn_keep[local, :] = dn

        @pl.when(jnp.logical_not(is_own))
        def _():
            dn_send[local, :] = dn.astype(BF)

        return carry

    lax.fori_loop(0, length // TB, finish, 0)

    low = width // 16
    pieces = width // LANES
    for which, source in ((0, dq_low), (1, dk_low), (2, dv_low)):
        for piece in range(pieces):
            grad = tn(source[...], normed_ref[:, piece * LANES : (piece + 1) * LANES]).astype(BF)
            for o in range(8):
                at = (which * pieces + piece) * low
                pack_ref[slots_b[o], pl.ds(at, low), :] = grad[o * low : (o + 1) * low, :]
    turned = jnp.transpose(gains[...])
    turned_low = turned.astype(BF)
    rest = (turned - turned_low.astype(F32)).astype(BF)
    lane = lax.broadcasted_iota(jnp.int32, (1, LANES), 1)
    both = jnp.where(lane < LANES // 2, turned_low, pltpu.roll(rest.astype(F32), LANES // 2, 1).astype(BF))
    at_b = 3 * pieces * low
    size_a = (cols // LANES + 1) * low
    base = at_b + low
    for piece in range(cols // LANES):
        grad = tn(d_branch[...], att_ref[:, piece * LANES : (piece + 1) * LANES]).astype(BF)
        for o in range(16):
            slot = slots_a[o]
            at = pl.multiple_of(base + (slot % 2) * size_a + piece * low, 16)
            pack_ref[slot // 2, pl.ds(at, low), :] = grad[o * low : (o + 1) * low, :]
    for o in range(16):
        slot = slots_a[o]
        at = pl.multiple_of(base + (slot % 2) * size_a + (cols // LANES) * low, 16)
        pack_ref[slot // 2, pl.ds(at, low), :] = both[o * low : (o + 1) * low, :]

        @pl.when(s == o // 8)
        def _():
            pack_ref[slots_b[o % 8], pl.ds(at_b, low), :] = both[o * low : (o + 1) * low, :]


BIG = pltpu.CompilerParams(vmem_limit_bytes=60 * 1024 * 1024)


def shape(*dims, dtype=BF):
    return jax.ShapeDtypeStruct(dims, dtype)


def flat(dp, core):
    return 2 * dp + core


def swap_cores(chips):
    return [(flat(d, c), flat(d, 1 - c)) for d in range(chips) for c in range(2)]


ORDER = ((0, 1, 2, 3), (1, 0, 2, 3))


def swap_chips(step):
    return [(flat(d, c), flat(d ^ (1 << ORDER[c][step]), c)) for d in range(16) for c in range(2)]


def to_owner_half():
    return [(flat(d, c), flat(d ^ 8, c)) for d in range(16) for c in range(2) if d // 8 != c]


def slot_tables(chip, core, chips):
    if chips != 16:
        return jnp.arange(16, dtype=jnp.int32), jnp.arange(8, dtype=jnp.int32)
    owner = jnp.arange(16, dtype=jnp.int32)
    away = owner ^ chip
    x, y, z0, z1 = away & 1, (away >> 1) & 1, (away >> 2) & 1, (away >> 3) & 1
    first = jnp.where(core == 0, x, y)
    second = jnp.where(core == 0, y, x)
    slots_a = first * 8 + second * 4 + z0 * 2 + z1
    near = slots_a // 2
    return slots_a, jnp.where(core == 0, near[:8], near[8:])


def halve(pack):
    for step in range(3):
        half = pack.shape[0] // 2
        pack3 = pack.reshape(2, half, *pack.shape[1:])
        got = lax.ppermute(pack3[1], AX, swap_chips(step))
        total = pack3[0].astype(F32) + got.astype(F32)
        pack = total.astype(BF) if step < 2 else total
    return pack[0]


def last_step(total, size_b):
    kind_b = total[:size_b]
    kind_a = total[size_b:].reshape(2, -1, LANES)
    got_a = lax.ppermute(kind_a[1].astype(BF), AX, swap_chips(3))
    got_b = lax.ppermute(kind_b.astype(BF), AX, to_owner_half())
    return kind_a[0] + got_a.astype(F32), kind_b + got_b.astype(F32)


def shards(
    tokens, segment_ids, norm1_gain, w_query, w_key, w_value, w_out, norm2_gain, w_gate, w_up, w_down, out_grad,
    *, chips,
):
    seqs, half_tokens, width = tokens.shape
    length = 2 * half_tokens
    cols = w_query.shape[1] // 2
    ff = w_gate.shape[1] // 2
    core = lax.axis_index("seq")
    chip = lax.axis_index("dp")
    core_id = core.reshape(1).astype(jnp.int32)
    pairs = swap_cores(chips)
    own = tokens.reshape(half_tokens, width)
    dy_own = out_grad.reshape(half_tokens, width)
    ids = segment_ids.reshape(1, half_tokens)
    other = lax.ppermute(own, AX, pairs)
    ids_other = lax.ppermute(ids, AX, pairs)
    dy_other = lax.ppermute(dy_own, AX, pairs)
    seg_row = jnp.where(core == 0, jnp.concatenate([ids, ids_other], 1), jnp.concatenate([ids_other, ids], 1))
    seg_col = seg_row.reshape(length, 1)
    gain_one = norm1_gain.astype(F32).reshape(1, width)
    gain_two = norm2_gain.astype(F32).reshape(1, width)
    tables = tuple(jnp.asarray(t) for t in small_tables(length))
    slots_a, slots_b = slot_tables(chip, core, chips)
    half_w = pl.BlockSpec((width, cols), lambda g, c: (0, c[0]))
    half_wide = pl.BlockSpec((width, ff), lambda g, c, a, b: (0, c[0]))
    whole = lambda a: pl.BlockSpec(a.shape, lambda g, *_: (0,) * len(a.shape))

    def out_block(s):
        return pl.BlockSpec(s.shape, lambda g, *_: (0,) * len(s.shape))

    outs = (
        shape(length, width), shape(length, cols), shape(length, cols), shape(length, cols), shape(length, cols),
        shape(length, LANES, dtype=F32),
    )
    normed1, q, k, v, att, lse = pl.pallas_call(
        forward_attention,
        out_shape=outs,
        grid_spec=pltpu.PrefetchScalarGridSpec(
            num_scalar_prefetch=1,
            grid=(1,),
            in_specs=[whole(own), whole(other), whole(gain_one), half_w, half_w, half_w]
            + [whole(t) for t in tables]
            + [whole(seg_col), whole(seg_row)],
            out_specs=[out_block(o) for o in outs],
            scratch_shapes=[pltpu.VMEM((TB, 3 * TB), F32)],
        ),
        compiler_params=BIG,
        name="attention_forward",
    )(core_id, own, other, gain_one, w_query, w_key, w_value, *tables, seg_col, seg_row)
    att_other = lax.ppermute(att, AX, pairs)

    rows_one = 2 * (width // LANES) * (ff // 8) + 2 * (ff // LANES) * (width // 16)
    outs = (
        shape(length, width, dtype=F32), shape(half_tokens, width, dtype=F32), shape(half_tokens, width),
        shape(length, width), shape(8, rows_one, LANES),
    )
    residual, out_keep, out_send, dn, pack_one = pl.pallas_call(
        feed_forward,
        out_shape=outs,
        grid_spec=pltpu.PrefetchScalarGridSpec(
            num_scalar_prefetch=3,
            grid=(1,),
            in_specs=[whole(own), whole(other), whole(att), whole(att), whole(gain_two), whole(w_out), half_wide, half_wide,
                      pl.BlockSpec((ff, width), lambda g, c, a, b: (c[0], 0)), whole(own), whole(own)],
            out_specs=[out_block(o) for o in outs],
            scratch_shapes=[
                pltpu.VMEM((length, width), BF), pltpu.VMEM((length, ff), BF), pltpu.VMEM((length, ff), BF),
                pltpu.VMEM((length, ff), BF), pltpu.VMEM((length, width), BF),
            ],
        ),
        compiler_params=BIG,
        name="feed_forward",
    )(core_id, slots_a, slots_b, own, other, att, att_other, gain_two, w_out, w_gate, w_up, w_down, dy_own, dy_other)
    out_other = lax.ppermute(out_send, AX, pairs)
    block_out = (out_keep + out_other.astype(F32)).astype(BF)
    dn_other = lax.ppermute(dn, AX, pairs)

    low = width // 16
    size_b2 = 3 * (width // LANES) * low + low
    size_a2 = (cols // LANES + 1) * low
    outs = (
        shape(half_tokens, width, dtype=F32), shape(half_tokens, width, dtype=F32), shape(half_tokens, width),
        shape(8, size_b2 + 2 * size_a2, LANES),
    )
    half_w3 = pl.BlockSpec((width, cols), lambda g, c, a, b: (0, c[0]))
    inputs = (own, other, gain_one, gain_two, w_query, w_key, w_value, w_out, dy_own, dy_other, residual, dn, dn_other,
              att, normed1, q, k, v, lse, *tables, seg_col, seg_row)
    specs = [whole(a) for a in inputs]
    specs[4] = specs[5] = specs[6] = half_w3
    specs[7] = pl.BlockSpec((cols, width), lambda g, c, a, b: (c[0], 0))
    d_res, dn_keep, dn_send, pack_two = pl.pallas_call(
        backward_attention,
        out_shape=outs,
        grid_spec=pltpu.PrefetchScalarGridSpec(
            num_scalar_prefetch=3,
            grid=(1,),
            in_specs=specs,
            out_specs=[out_block(o) for o in outs],
            scratch_shapes=[
                pltpu.VMEM((length, width), BF), pltpu.VMEM((length, cols), BF),
                pltpu.VMEM((length, cols), F32), pltpu.VMEM((length, cols), F32), pltpu.VMEM((length, cols), F32),
                pltpu.VMEM((length, cols), BF), pltpu.VMEM((length, cols), BF), pltpu.VMEM((length, cols), BF),
                pltpu.VMEM((LANES, width), F32), pltpu.VMEM((TB, 3 * TB), F32),
            ],
        ),
        compiler_params=BIG,
        name="attention_backward",
    )(core_id, slots_a, slots_b, *inputs)
    dn1 = dn_keep + lax.ppermute(dn_send, AX, pairs).astype(F32)
    x = own.astype(F32)
    r = lax.rsqrt(jnp.mean(x * x, axis=-1, keepdims=True) + EPS)
    e = gain_one * dn1
    input_grad = (d_res + r * e - x * (r * r * r) * jnp.mean(e * x, axis=-1, keepdims=True)).astype(BF)

    pieces = width // LANES
    wide = ff // 8
    size_b1 = 2 * pieces * wide
    size_a1 = (ff // LANES) * low

    if chips == 16:
        one_a, one_b = last_step(halve(pack_one), size_b1)
        two_a, two_b = last_step(halve(pack_two), size_b2)
        holds = (chip >> 3) == core

        def share(a):
            parts = a.reshape(a.shape[0], 2, a.shape[1] // 2, LANES)
            mine = jnp.where(core == 0, parts[:, 0], parts[:, 1])
            theirs = jnp.where(core == 0, parts[:, 1], parts[:, 0])
            return mine, lax.ppermute(theirs, AX, pairs)

        def both(a):
            mine, got = share(a)
            return jnp.where(core == 0, mine, got), jnp.where(core == 0, got, mine)

        def one(a):
            mine, got = share(a)
            return jnp.where(holds, mine, got)

        down_lo, down_hi = both(one_a.reshape(ff // LANES, low, LANES))
        kind_a = two_a.reshape(cols // LANES + 1, low, LANES)
        out_lo, out_hi = both(kind_a)
        gates = one(one_b.reshape(2 * pieces, wide, LANES))
        rest = one(two_b.reshape(3 * pieces + 1, low, LANES))

        def turn(a):
            return jnp.transpose(a, (0, 2, 1)).reshape(-1, a.shape[1])

        tiles = cols // LANES
        gain1 = out_lo[tiles] + out_hi[tiles]
        gain1 = gain1[:, 1] + gain1[:, 1 + LANES // 2]
        gain2 = rest[3 * pieces]
        gain2 = gain2[:, 0] + gain2[:, LANES // 2]
        summed = (
            gain1,
            turn(rest[:pieces]),
            turn(rest[pieces : 2 * pieces]),
            turn(rest[2 * pieces : 3 * pieces]),
            turn(jnp.concatenate([out_lo[:tiles], out_hi[:tiles]])),
            gain2,
            turn(gates[:pieces]),
            turn(gates[pieces:]),
            turn(jnp.concatenate([down_lo, down_hi])),
        )
    else:
        def plain_b(rows, count, size, at):
            part = rows[:, at : at + count * size].reshape(8, count, size, LANES)
            part = jnp.transpose(part, (1, 3, 0, 2)).reshape(count * LANES, 8 * size).astype(F32)
            zero = jnp.zeros_like(part)
            return jnp.where(core == 0, jnp.concatenate([part, zero], 1), jnp.concatenate([zero, part], 1))

        def plain_a(rows, count, at, each):
            part = rows[:, at:].reshape(8, 2, each, low, LANES)[:, :, :count].reshape(16, count, low, LANES)
            part = jnp.transpose(part, (1, 3, 0, 2)).reshape(count * LANES, 16 * low).astype(F32)
            zero = jnp.zeros_like(part)
            return jnp.where(core == 0, jnp.concatenate([part, zero], 0), jnp.concatenate([zero, part], 0))

        def scatter(a):
            return lax.psum_scatter(a, AX, scatter_dimension=1, tiled=True)

        tiles = cols // LANES
        gain_a = pack_two[:, size_b2:].reshape(16, tiles + 1, low, LANES)[:, tiles].astype(F32)
        gain_a = gain_a[:, :, : LANES // 2] + gain_a[:, :, LANES // 2 :]
        gain_a = gain_a.reshape(width, LANES // 2)
        gain1 = gain_a[:, 1].reshape(1, width)
        gain2 = jnp.where(core == 0, gain_a[:, 0], 0.0).reshape(1, width)
        n = pieces * low
        summed = (
            scatter(gain1).reshape(-1),
            scatter(plain_b(pack_two, pieces, low, 0)),
            scatter(plain_b(pack_two, pieces, low, n)),
            scatter(plain_b(pack_two, pieces, low, 2 * n)),
            scatter(plain_a(pack_two, tiles, size_b2, tiles + 1)),
            scatter(gain2).reshape(-1),
            scatter(plain_b(pack_one, pieces, wide, 0)),
            scatter(plain_b(pack_one, pieces, wide, pieces * wide)),
            scatter(plain_a(pack_one, ff // LANES, size_b1, ff // LANES)),
        )
    return (block_out.reshape(seqs, half_tokens, width), input_grad.reshape(seqs, half_tokens, width), *summed)


def solution(mesh):
    placed = (P("dp", "seq", None), P("dp", "seq"), *([P()] * 9), P("dp", "seq", None))
    column = P(None, AX)
    return jax.shard_map(
        functools.partial(shards, chips=mesh.shape["dp"]),
        mesh=mesh,
        in_specs=placed,
        out_specs=(
            P("dp", "seq", None), P("dp", "seq", None), P(AX), column, column, column, column, P(AX), column, column, column,
        ),
        check_vma=False,
    )
```

```python
import functools

import jax
import jax.numpy as jnp
import numpy as np
from jax import lax
from jax.experimental import pallas as pl
from jax.experimental.pallas import tpu as pltpu
from jax.sharding import PartitionSpec as P

HD = 64
EPS = 1e-06
SCALE = 0.125
NEG = -1e30
BASE = 10000.0
AX = ("dp", "seq")
BF = jnp.bfloat16
F32 = jnp.float32
TB = 256
LANES = 128


def nn(a, b):
    return lax.dot_general(a, b, (((1,), (0,)), ((), ())), preferred_element_type=F32)


def nt(a, b):
    return lax.dot_general(a, b, (((1,), (1,)), ((), ())), preferred_element_type=F32)


def tn(a, b):
    return lax.dot_general(a, b, (((0,), (0,)), ((), ())), preferred_element_type=F32)


def small_tables(length):
    freqs = BASE ** (-np.arange(HD // 2, dtype=np.float64) * (2.0 / HD))
    lane_freqs = np.tile(freqs, 4)[None, :]
    fine = np.arange(64, dtype=np.float64)[:, None] * lane_freqs
    coarse = 64.0 * np.arange(length // 64, dtype=np.float64)[:, None] * lane_freqs
    return tuple(
        np.asarray(t, np.float32) for t in (np.cos(fine), np.sin(fine), np.cos(coarse), np.sin(coarse))
    )


def angle_block(tables, sub):
    cos_f, sin_f, cos_c, sin_c = tables
    ca = cos_c[pl.ds(sub, 1), :]
    sa = sin_c[pl.ds(sub, 1), :]
    cb = cos_f[...]
    sb = sin_f[...]
    low_half = (lax.broadcasted_iota(jnp.int32, (64, LANES), 1) % HD) < HD // 2
    cosine = ca * cb - sa * sb
    sine = sa * cb + ca * sb
    return cosine, jnp.where(low_half, -sine, sine), low_half


def rotate(v, cosine, sine, low_half):
    partner = jnp.where(low_half, pltpu.roll(v, LANES - HD // 2, 1), pltpu.roll(v, HD // 2, 1))
    return v * cosine + partner * sine


def window(block):
    return max(0, (block - 2) * TB)


def bias_of(seg_col, seg_row, block):
    first = window(block)
    keys = (block + 1) * TB - first
    rows = seg_col[pl.ds(block * TB, TB), :]
    cols = seg_row[:, pl.ds(first, keys)]
    q_at = block * TB + lax.broadcasted_iota(jnp.int32, (TB, keys), 0)
    k_at = first + lax.broadcasted_iota(jnp.int32, (TB, keys), 1)
    return jnp.where((rows == cols) & (k_at <= q_at), 0.0, NEG).astype(F32)


def forward_attention(
    core, own_ref, other_ref, gain_ref, wq_ref, wk_ref, wv_ref, cos_f, sin_f, cos_c, sin_c, seg_col, seg_row,
    normed_ref, q_ref, k_ref, v_ref, att_ref, lse_ref, bias_ref,
):
    s = core[0]
    half_tokens, width = own_ref.shape
    length = 2 * half_tokens
    cols = wq_ref.shape[1]
    tables = (cos_f, sin_f, cos_c, sin_c)

    def project(t, carry):
        rows = pl.ds(pl.multiple_of(t * TB, TB), TB)
        part = t // (half_tokens // TB)
        local = pl.ds(pl.multiple_of((t % (half_tokens // TB)) * TB, TB), TB)
        x = jnp.where(part == s, own_ref[local, :], other_ref[local, :]).astype(F32)
        r = lax.rsqrt(jnp.mean(x * x, axis=-1, keepdims=True) + EPS)
        normed = (x * r * gain_ref[...]).astype(BF)
        normed_ref[rows, :] = normed
        v_ref[rows, :] = nn(normed, wv_ref[...]).astype(BF)
        q = nn(normed, wq_ref[...]).astype(BF).astype(F32)
        k = nn(normed, wk_ref[...]).astype(BF).astype(F32)
        for sub in range(TB // 64):
            cosine, sine, low_half = angle_block(tables, t * (TB // 64) + sub)
            at = pl.ds(pl.multiple_of(t * TB + sub * 64, 64), 64)
            for tile in range(cols // LANES):
                lanes = slice(tile * LANES, (tile + 1) * LANES)
                part_rows = slice(sub * 64, (sub + 1) * 64)
                q_ref[at, lanes] = (rotate(q[part_rows, lanes], cosine, sine, low_half).astype(BF) * BF(SCALE)).astype(BF)
                k_ref[at, lanes] = rotate(k[part_rows, lanes], cosine, sine, low_half).astype(BF)
        return carry

    lax.fori_loop(0, length // TB, project, 0)

    for block in range(length // TB):
        first = window(block)
        keys = (block + 1) * TB - first
        bias_ref[:, :keys] = bias_of(seg_col, seg_row, block)
        rows = pl.ds(block * TB, TB)
        span = pl.ds(first, keys)

        def head(h, carry):
            lanes = pl.ds(pl.multiple_of((h // 2) * LANES, LANES), LANES)
            lane = lax.broadcasted_iota(jnp.int32, (1, LANES), 1)
            mine = (lane // HD) == (h % 2)
            q = q_ref[rows, lanes]
            qm = jnp.where(mine, q, jnp.zeros_like(q))
            scores = nt(qm, k_ref[span, lanes]) + bias_ref[:, :keys]
            peak = jnp.max(scores, axis=-1, keepdims=True)
            weights = jnp.exp(scores - peak)
            total = jnp.sum(weights, axis=-1, keepdims=True)
            probs = (weights * (1.0 / total)).astype(BF)
            result = nn(probs, v_ref[span, lanes]).astype(BF)
            att_ref[rows, lanes] = jnp.where(mine, result, att_ref[rows, lanes])
            lse_ref[rows, :] = jnp.where(lane == h, peak + jnp.log(total), lse_ref[rows, :])
            return carry

        lax.fori_loop(0, cols // HD, head, 0)


def feed_forward(
    core, slots_a, slots_b, own_ref, other_ref, att_own, att_other, gain_ref, wo_ref, wg_ref, wu_ref, wd_ref,
    dy_own, dy_other,
    res_ref, out_keep, out_send, dn_ref, pack_ref, normed, hidden, d_gate, d_up, dy_all,
):
    s = core[0]
    half_tokens, width = own_ref.shape
    length = 2 * half_tokens
    cols = att_own.shape[1]
    own_rows = pl.ds(pl.multiple_of(s * cols, cols), cols)
    other_rows = pl.ds(pl.multiple_of((1 - s) * cols, cols), cols)

    def block(t, carry):
        rows = pl.ds(pl.multiple_of(t * TB, TB), TB)
        part = t // (half_tokens // TB)
        local = pl.ds(pl.multiple_of((t % (half_tokens // TB)) * TB, TB), TB)
        is_own = part == s
        x = jnp.where(is_own, own_ref[local, :], other_ref[local, :]).astype(F32)
        dy = jnp.where(is_own, dy_own[local, :], dy_other[local, :])
        dy_all[rows, :] = dy
        residual = x + (nn(att_own[rows, :], wo_ref[own_rows, :]) + nn(att_other[rows, :], wo_ref[other_rows, :]))
        res_ref[rows, :] = residual
        r = lax.rsqrt(jnp.mean(residual * residual, axis=-1, keepdims=True) + EPS)
        n2 = (residual * r * gain_ref[...]).astype(BF)
        normed[rows, :] = n2
        gate = nn(n2, wg_ref[...])
        up = nn(n2, wu_ref[...])
        sig = 1.0 / (1.0 + jnp.exp(-gate))
        act = gate * sig
        hid = (act * up).astype(BF)
        hidden[rows, :] = hid
        down = nn(hid, wd_ref[...])

        @pl.when(is_own)
        def _():
            out_keep[local, :] = residual + down

        @pl.when(jnp.logical_not(is_own))
        def _():
            out_send[local, :] = down.astype(BF)

        d_hidden = nt(dy, wd_ref[...])
        dg = (d_hidden * up * (sig * (1.0 + gate * (1.0 - sig)))).astype(BF)
        du = (d_hidden * act).astype(BF)
        d_gate[rows, :] = dg
        d_up[rows, :] = du
        dn_ref[rows, :] = (nt(dg, wg_ref[...]) + nt(du, wu_ref[...])).astype(BF)
        return carry

    lax.fori_loop(0, length // TB, block, 0)

    wide = wg_ref.shape[1] // 8
    pieces = width // LANES

    def gate_up(o, carry):
        cut = pl.ds(pl.multiple_of(o * wide, wide), wide)
        slot = slots_b[o]
        for which, source in ((0, d_gate), (1, d_up)):
            grad = tn(source[:, cut], normed[...]).astype(BF)
            for piece in range(pieces):
                pack_ref[slot, pl.ds((which * pieces + piece) * wide, wide), :] = grad[:, piece * LANES : (piece + 1) * LANES]
        return carry

    lax.fori_loop(0, 8, gate_up, 0)
    low = width // 16
    base = 2 * pieces * wide
    deep = hidden.shape[1] // LANES
    for piece in range(deep):
        grad = tn(dy_all[...], hidden[:, piece * LANES : (piece + 1) * LANES]).astype(BF)
        for o in range(16):
            slot = slots_a[o]
            at = pl.multiple_of(base + (slot % 2) * (deep * low) + piece * low, 16)
            pack_ref[slot // 2, pl.ds(at, low), :] = grad[o * low : (o + 1) * low, :]


def backward_attention(
    core, slots_a, slots_b, own_ref, other_ref, gain_one, gain_two, wq_ref, wk_ref, wv_ref, wo_ref, dy_own, dy_other,
    res_ref, dn_own, dn_other, att_ref, normed_ref, q_ref, k_ref, v_ref, lse_ref, cos_f, sin_f, cos_c, sin_c, seg_col, seg_row,
    d_res, dn_keep, dn_send, pack_ref, d_branch, d_att, dq, dk, dv, dq_low, dk_low, dv_low, gains, bias_ref,
):
    s = core[0]
    half_tokens, width = own_ref.shape
    length = 2 * half_tokens
    cols = att_ref.shape[1]
    tables = (cos_f, sin_f, cos_c, sin_c)
    gains[...] = jnp.zeros_like(gains)

    def norm_two(t, carry):
        rows = pl.ds(pl.multiple_of(t * TB, TB), TB)
        part = t // (half_tokens // TB)
        local = pl.ds(pl.multiple_of((t % (half_tokens // TB)) * TB, TB), TB)
        is_own = part == s
        dy = jnp.where(is_own, dy_own[local, :], dy_other[local, :]).astype(F32)
        residual = res_ref[rows, :]
        dn = dn_own[rows, :].astype(F32) + dn_other[rows, :].astype(F32)
        r = lax.rsqrt(jnp.mean(residual * residual, axis=-1, keepdims=True) + EPS)
        scaled = residual * r
        e = gain_two[...] * dn
        gains[0:1, :] += jnp.sum(dn * scaled, axis=0, keepdims=True)
        grad = dy + r * (e - scaled * (r * jnp.mean(e * residual, axis=-1, keepdims=True)))
        low = grad.astype(BF)
        d_branch[rows, :] = low

        @pl.when(is_own)
        def _():
            d_res[local, :] = grad

        d_att[rows, :] = nt(low, wo_ref[...]).astype(BF)
        return carry

    lax.fori_loop(0, length // TB, norm_two, 0)

    dk[...] = jnp.zeros_like(dk)
    dv[...] = jnp.zeros_like(dv)
    for block in range(length // TB):
        first = window(block)
        keys = (block + 1) * TB - first
        bias_ref[:, :keys] = bias_of(seg_col, seg_row, block)
        rows = pl.ds(block * TB, TB)
        span = pl.ds(first, keys)

        def head(h, carry):
            lanes = pl.ds(pl.multiple_of((h // 2) * LANES, LANES), LANES)
            lane = lax.broadcasted_iota(jnp.int32, (1, LANES), 1)
            mine = (lane // HD) == (h % 2)
            q = q_ref[rows, lanes]
            qm = jnp.where(mine, q, jnp.zeros_like(q))
            do = d_att[rows, lanes]
            dom = jnp.where(mine, do, jnp.zeros_like(do))
            lse = jnp.sum(jnp.where(lane == h, lse_ref[rows, :], 0.0), axis=-1, keepdims=True)
            k = k_ref[span, lanes]
            probs = jnp.exp(nt(qm, k) + (bias_ref[:, :keys] - lse))
            d_probs = nt(dom, v_ref[span, lanes])
            delta = jnp.sum(probs * d_probs, axis=-1, keepdims=True)
            ds = (probs * (d_probs - delta)).astype(BF)
            part = nn(ds, k)
            dq[rows, lanes] = jnp.where(mine, part, dq[rows, lanes])
            dk[span, lanes] += tn(ds, qm)
            dv[span, lanes] += tn(probs.astype(BF), dom)
            return carry

        lax.fori_loop(0, cols // HD, head, 0)

    def finish(t, carry):
        rows = pl.ds(pl.multiple_of(t * TB, TB), TB)
        part = t // (half_tokens // TB)
        local = pl.ds(pl.multiple_of((t % (half_tokens // TB)) * TB, TB), TB)
        is_own = part == s
        for sub in range(TB // 64):
            cosine, sine, low_half = angle_block(tables, t * (TB // 64) + sub)
            at = pl.ds(pl.multiple_of(t * TB + sub * 64, 64), 64)
            for tile in range(cols // LANES):
                lanes = slice(tile * LANES, (tile + 1) * LANES)
                dq_low[at, lanes] = (rotate(dq[at, lanes], cosine, -sine, low_half) * SCALE).astype(BF)
                dk_low[at, lanes] = rotate(dk[at, lanes], cosine, -sine, low_half).astype(BF)
        dv_low[rows, :] = dv[rows, :].astype(BF)
        dn = nt(dq_low[rows, :], wq_ref[...]) + nt(dk_low[rows, :], wk_ref[...]) + nt(dv_low[rows, :], wv_ref[...])
        x = jnp.where(is_own, own_ref[local, :], other_ref[local, :]).astype(F32)
        r = lax.rsqrt(jnp.mean(x * x, axis=-1, keepdims=True) + EPS)
        gains[1:2, :] += jnp.sum(dn * (x * r), axis=0, keepdims=True)

        @pl.when(is_own)
        def _():
            dn_keep[local, :] = dn

        @pl.when(jnp.logical_not(is_own))
        def _():
            dn_send[local, :] = dn.astype(BF)

        return carry

    lax.fori_loop(0, length // TB, finish, 0)

    low = width // 16
    pieces = width // LANES
    for which, source in ((0, dq_low), (1, dk_low), (2, dv_low)):
        for piece in range(pieces):
            grad = tn(source[...], normed_ref[:, piece * LANES : (piece + 1) * LANES]).astype(BF)
            for o in range(8):
                at = (which * pieces + piece) * low
                pack_ref[slots_b[o], pl.ds(at, low), :] = grad[o * low : (o + 1) * low, :]
    turned = jnp.transpose(gains[...])
    turned_low = turned.astype(BF)
    rest = (turned - turned_low.astype(F32)).astype(BF)
    lane = lax.broadcasted_iota(jnp.int32, (1, LANES), 1)
    both = jnp.where(lane < LANES // 2, turned_low, pltpu.roll(rest.astype(F32), LANES // 2, 1).astype(BF))
    at_b = 3 * pieces * low
    size_a = (cols // LANES + 1) * low
    base = at_b + low
    for piece in range(cols // LANES):
        grad = tn(d_branch[...], att_ref[:, piece * LANES : (piece + 1) * LANES]).astype(BF)
        for o in range(16):
            slot = slots_a[o]
            at = pl.multiple_of(base + (slot % 2) * size_a + piece * low, 16)
            pack_ref[slot // 2, pl.ds(at, low), :] = grad[o * low : (o + 1) * low, :]
    for o in range(16):
        slot = slots_a[o]
        at = pl.multiple_of(base + (slot % 2) * size_a + (cols // LANES) * low, 16)
        pack_ref[slot // 2, pl.ds(at, low), :] = both[o * low : (o + 1) * low, :]

        @pl.when(s == o // 8)
        def _():
            pack_ref[slots_b[o % 8], pl.ds(at_b, low), :] = both[o * low : (o + 1) * low, :]


BIG = pltpu.CompilerParams(vmem_limit_bytes=60 * 1024 * 1024)


def shape(*dims, dtype=BF):
    return jax.ShapeDtypeStruct(dims, dtype)


def flat(dp, core):
    return 2 * dp + core


def swap_cores(chips):
    return [(flat(d, c), flat(d, 1 - c)) for d in range(chips) for c in range(2)]


ORDER = ((0, 1, 2, 3), (1, 0, 2, 3))


def swap_chips(step):
    return [(flat(d, c), flat(d ^ (1 << ORDER[c][step]), c)) for d in range(16) for c in range(2)]


def to_owner_half():
    return [(flat(d, c), flat(d ^ 8, c)) for d in range(16) for c in range(2) if d // 8 != c]


def slot_tables(chip, core, chips):
    if chips != 16:
        return jnp.arange(16, dtype=jnp.int32), jnp.arange(8, dtype=jnp.int32)
    owner = jnp.arange(16, dtype=jnp.int32)
    away = owner ^ chip
    x, y, z0, z1 = away & 1, (away >> 1) & 1, (away >> 2) & 1, (away >> 3) & 1
    first = jnp.where(core == 0, x, y)
    second = jnp.where(core == 0, y, x)
    slots_a = first * 8 + second * 4 + z0 * 2 + z1
    near = slots_a // 2
    return slots_a, jnp.where(core == 0, near[:8], near[8:])


def halve(pack):
    for step in range(3):
        half = pack.shape[0] // 2
        pack3 = pack.reshape(2, half, *pack.shape[1:])
        got = lax.ppermute(pack3[1], AX, swap_chips(step))
        total = pack3[0].astype(F32) + got.astype(F32)
        pack = total.astype(BF) if step < 2 else total
    return pack[0]


def last_step(total, size_b):
    kind_b = total[:size_b]
    kind_a = total[size_b:].reshape(2, -1, LANES)
    got_a = lax.ppermute(kind_a[1].astype(BF), AX, swap_chips(3))
    got_b = lax.ppermute(kind_b.astype(BF), AX, to_owner_half())
    return kind_a[0] + got_a.astype(F32), kind_b + got_b.astype(F32)


def shards(
    tokens, segment_ids, norm1_gain, w_query, w_key, w_value, w_out, norm2_gain, w_gate, w_up, w_down, out_grad,
    *, chips,
):
    seqs, half_tokens, width = tokens.shape
    length = 2 * half_tokens
    cols = w_query.shape[1] // 2
    ff = w_gate.shape[1] // 2
    core = lax.axis_index("seq")
    chip = lax.axis_index("dp")
    core_id = core.reshape(1).astype(jnp.int32)
    pairs = swap_cores(chips)
    own = tokens.reshape(half_tokens, width)
    dy_own = out_grad.reshape(half_tokens, width)
    ids = segment_ids.reshape(1, half_tokens)
    other = lax.ppermute(own, AX, pairs)
    ids_other = lax.ppermute(ids, AX, pairs)
    dy_other = lax.ppermute(dy_own, AX, pairs)
    seg_row = jnp.where(core == 0, jnp.concatenate([ids, ids_other], 1), jnp.concatenate([ids_other, ids], 1))
    seg_col = seg_row.reshape(length, 1)
    gain_one = norm1_gain.astype(F32).reshape(1, width)
    gain_two = norm2_gain.astype(F32).reshape(1, width)
    tables = tuple(jnp.asarray(t) for t in small_tables(length))
    slots_a, slots_b = slot_tables(chip, core, chips)
    half_w = pl.BlockSpec((width, cols), lambda g, c: (0, c[0]))
    half_wide = pl.BlockSpec((width, ff), lambda g, c, a, b: (0, c[0]))
    whole = lambda a: pl.BlockSpec(a.shape, lambda g, *_: (0,) * len(a.shape))

    def out_block(s):
        return pl.BlockSpec(s.shape, lambda g, *_: (0,) * len(s.shape))

    outs = (
        shape(length, width), shape(length, cols), shape(length, cols), shape(length, cols), shape(length, cols),
        shape(length, LANES, dtype=F32),
    )
    normed1, q, k, v, att, lse = pl.pallas_call(
        forward_attention,
        out_shape=outs,
        grid_spec=pltpu.PrefetchScalarGridSpec(
            num_scalar_prefetch=1,
            grid=(1,),
            in_specs=[whole(own), whole(other), whole(gain_one), half_w, half_w, half_w]
            + [whole(t) for t in tables]
            + [whole(seg_col), whole(seg_row)],
            out_specs=[out_block(o) for o in outs],
            scratch_shapes=[pltpu.VMEM((TB, 3 * TB), F32)],
        ),
        compiler_params=BIG,
        name="attention_forward",
    )(core_id, own, other, gain_one, w_query, w_key, w_value, *tables, seg_col, seg_row)
    att_other = lax.ppermute(att, AX, pairs)

    rows_one = 2 * (width // LANES) * (ff // 8) + 2 * (ff // LANES) * (width // 16)
    outs = (
        shape(length, width, dtype=F32), shape(half_tokens, width, dtype=F32), shape(half_tokens, width),
        shape(length, width), shape(8, rows_one, LANES),
    )
    residual, out_keep, out_send, dn, pack_one = pl.pallas_call(
        feed_forward,
        out_shape=outs,
        grid_spec=pltpu.PrefetchScalarGridSpec(
            num_scalar_prefetch=3,
            grid=(1,),
            in_specs=[whole(own), whole(other), whole(att), whole(att), whole(gain_two), whole(w_out), half_wide, half_wide,
                      pl.BlockSpec((ff, width), lambda g, c, a, b: (c[0], 0)), whole(own), whole(own)],
            out_specs=[out_block(o) for o in outs],
            scratch_shapes=[
                pltpu.VMEM((length, width), BF), pltpu.VMEM((length, ff), BF), pltpu.VMEM((length, ff), BF),
                pltpu.VMEM((length, ff), BF), pltpu.VMEM((length, width), BF),
            ],
        ),
        compiler_params=BIG,
        name="feed_forward",
    )(core_id, slots_a, slots_b, own, other, att, att_other, gain_two, w_out, w_gate, w_up, w_down, dy_own, dy_other)
    out_other = lax.ppermute(out_send, AX, pairs)
    block_out = (out_keep + out_other.astype(F32)).astype(BF)
    dn_other = lax.ppermute(dn, AX, pairs)

    low = width // 16
    size_b2 = 3 * (width // LANES) * low + low
    size_a2 = (cols // LANES + 1) * low
    outs = (
        shape(half_tokens, width, dtype=F32), shape(half_tokens, width, dtype=F32), shape(half_tokens, width),
        shape(8, size_b2 + 2 * size_a2, LANES),
    )
    half_w3 = pl.BlockSpec((width, cols), lambda g, c, a, b: (0, c[0]))
    inputs = (own, other, gain_one, gain_two, w_query, w_key, w_value, w_out, dy_own, dy_other, residual, dn, dn_other,
              att, normed1, q, k, v, lse, *tables, seg_col, seg_row)
    specs = [whole(a) for a in inputs]
    specs[4] = specs[5] = specs[6] = half_w3
    specs[7] = pl.BlockSpec((cols, width), lambda g, c, a, b: (c[0], 0))
    d_res, dn_keep, dn_send, pack_two = pl.pallas_call(
        backward_attention,
        out_shape=outs,
        grid_spec=pltpu.PrefetchScalarGridSpec(
            num_scalar_prefetch=3,
            grid=(1,),
            in_specs=specs,
            out_specs=[out_block(o) for o in outs],
            scratch_shapes=[
                pltpu.VMEM((length, width), BF), pltpu.VMEM((length, cols), BF),
                pltpu.VMEM((length, cols), F32), pltpu.VMEM((length, cols), F32), pltpu.VMEM((length, cols), F32),
                pltpu.VMEM((length, cols), BF), pltpu.VMEM((length, cols), BF), pltpu.VMEM((length, cols), BF),
                pltpu.VMEM((LANES, width), F32), pltpu.VMEM((TB, 3 * TB), F32),
            ],
        ),
        compiler_params=BIG,
        name="attention_backward",
    )(core_id, slots_a, slots_b, *inputs)
    dn1 = dn_keep + lax.ppermute(dn_send, AX, pairs).astype(F32)
    x = own.astype(F32)
    r = lax.rsqrt(jnp.mean(x * x, axis=-1, keepdims=True) + EPS)
    e = gain_one * dn1
    input_grad = (d_res + r * e - x * (r * r * r) * jnp.mean(e * x, axis=-1, keepdims=True)).astype(BF)

    pieces = width // LANES
    wide = ff // 8
    size_b1 = 2 * pieces * wide
    size_a1 = (ff // LANES) * low

    if chips == 16:
        one_a, one_b = last_step(halve(pack_one), size_b1)
        two_a, two_b = last_step(halve(pack_two), size_b2)
        holds = (chip >> 3) == core

        def share(a):
            parts = a.reshape(a.shape[0], 2, a.shape[1] // 2, LANES)
            mine = jnp.where(core == 0, parts[:, 0], parts[:, 1])
            theirs = jnp.where(core == 0, parts[:, 1], parts[:, 0])
            return mine, lax.ppermute(theirs, AX, pairs)

        def both(a):
            mine, got = share(a)
            return jnp.where(core == 0, mine, got), jnp.where(core == 0, got, mine)

        def one(a):
            mine, got = share(a)
            return jnp.where(holds, mine, got)

        down_lo, down_hi = both(one_a.reshape(ff // LANES, low, LANES))
        kind_a = two_a.reshape(cols // LANES + 1, low, LANES)
        out_lo, out_hi = both(kind_a)
        gates = one(one_b.reshape(2 * pieces, wide, LANES))
        rest = one(two_b.reshape(3 * pieces + 1, low, LANES))

        def turn(a):
            return jnp.transpose(a, (0, 2, 1)).reshape(-1, a.shape[1])

        tiles = cols // LANES
        gain1 = out_lo[tiles] + out_hi[tiles]
        gain1 = gain1[:, 1] + gain1[:, 1 + LANES // 2]
        gain2 = rest[3 * pieces]
        gain2 = gain2[:, 0] + gain2[:, LANES // 2]
        summed = (
            gain1,
            turn(rest[:pieces]),
            turn(rest[pieces : 2 * pieces]),
            turn(rest[2 * pieces : 3 * pieces]),
            turn(jnp.concatenate([out_lo[:tiles], out_hi[:tiles]])),
            gain2,
            turn(gates[:pieces]),
            turn(gates[pieces:]),
            turn(jnp.concatenate([down_lo, down_hi])),
        )
    else:
        def plain_b(rows, count, size, at):
            part = rows[:, at : at + count * size].reshape(8, count, size, LANES)
            part = jnp.transpose(part, (1, 3, 0, 2)).reshape(count * LANES, 8 * size).astype(F32)
            zero = jnp.zeros_like(part)
            return jnp.where(core == 0, jnp.concatenate([part, zero], 1), jnp.concatenate([zero, part], 1))

        def plain_a(rows, count, at, each):
            part = rows[:, at:].reshape(8, 2, each, low, LANES)[:, :, :count].reshape(16, count, low, LANES)
            part = jnp.transpose(part, (1, 3, 0, 2)).reshape(count * LANES, 16 * low).astype(F32)
            zero = jnp.zeros_like(part)
            return jnp.where(core == 0, jnp.concatenate([part, zero], 0), jnp.concatenate([zero, part], 0))

        def scatter(a):
            return lax.psum_scatter(a, AX, scatter_dimension=1, tiled=True)

        tiles = cols // LANES
        gain_a = pack_two[:, size_b2:].reshape(16, tiles + 1, low, LANES)[:, tiles].astype(F32)
        gain_a = gain_a[:, :, : LANES // 2] + gain_a[:, :, LANES // 2 :]
        gain_a = gain_a.reshape(width, LANES // 2)
        gain1 = gain_a[:, 1].reshape(1, width)
        gain2 = jnp.where(core == 0, gain_a[:, 0], 0.0).reshape(1, width)
        n = pieces * low
        summed = (
            scatter(gain1).reshape(-1),
            scatter(plain_b(pack_two, pieces, low, 0)),
            scatter(plain_b(pack_two, pieces, low, n)),
            scatter(plain_b(pack_two, pieces, low, 2 * n)),
            scatter(plain_a(pack_two, tiles, size_b2, tiles + 1)),
            scatter(gain2).reshape(-1),
            scatter(plain_b(pack_one, pieces, wide, 0)),
            scatter(plain_b(pack_one, pieces, wide, pieces * wide)),
            scatter(plain_a(pack_one, ff // LANES, size_b1, ff // LANES)),
        )
    return (block_out.reshape(seqs, half_tokens, width), input_grad.reshape(seqs, half_tokens, width), *summed)


MESH = pl.DeviceIdType.MESH


def bit(value, place):
    return (value // (1 << place)) % 2


def other_bit(a, b):
    return a + b - 2 * a * b


def layout_of(width, cols, ff):
    low, wide = width // 16, ff // 8
    table, row, final = {}, 0, 0
    for name, kind, pieces, each in (
        ("gate", "B", width // LANES, wide), ("up", "B", width // LANES, wide), ("down", "A", ff // LANES, low),
        ("out", "A", cols // LANES, low), ("query", "B", width // LANES, low), ("key", "B", width // LANES, low),
        ("value", "B", width // LANES, low), ("gains", "A", 1, low),
    ):
        rows = pieces * each * (2 if kind == "A" else 1)
        table[name] = (row, rows, kind, pieces, each, final)
        row, final = row + rows, final + pieces * each // 2
    return table, row, final


def block_kernel(
    x_hbm, ids_hbm, dy_hbm, wq_hbm, wk_hbm, wv_hbm, wo_hbm, wg_hbm, wu_hbm, wd_hbm, gain_one, gain_two,
    cos_f, sin_f, cos_c, sin_c,
    block_out, input_grad, final_out,
    xs, dys, ids, seg_col, wq, wk, wv, wo, wg, wu, wd, normed1, q_ref, k_ref, v_ref, att, att_other, lse_ref, bias_ref,
    res_ref, normed2, hidden, d_gate, d_up, dn_own, dn_other, out_keep, out_send, out_got, dv_ref, dn_keep, dn_got,
    gains, pack, got1, got2, got3, got4, acc, final, final_got,
    load_sem, pair_send, pair_recv, hop_send, hop_recv,
):
    core = lax.axis_index("seq")
    chip = lax.axis_index("dp")
    half_tokens, width = x_hbm.shape
    length = 2 * half_tokens
    cols = wq.shape[1]
    ff = wg.shape[1]
    blocks = length // TB
    half_blocks = half_tokens // TB
    tables = (cos_f, sin_f, cos_c, sin_c)
    chunks, _, _ = layout_of(width, cols, ff)
    names = list(chunks)
    low = width // 16

    bx, by, bz, bw = (bit(chip, i) for i in range(4))
    step_x, step_y = 1 - 2 * bx, 2 * (1 - 2 * by)
    partners = (
        chip + (1 - core) * step_x + core * step_y,
        chip + core * step_x + (1 - core) * step_y,
        chip + 4 * (1 - 2 * bz),
        chip + 8 * (1 - 2 * bw),
    )
    holds = bw == core

    def slot_of(owner):
        kx, ky, kz = other_bit(bx, owner & 1), other_bit(by, (owner >> 1) & 1), other_bit(bz, (owner >> 2) & 1)
        first = (1 - core) * kx + core * ky
        second = core * kx + (1 - core) * ky
        return first * 4 + second * 2 + kz, other_bit(bw, (owner >> 3) & 1)

    def owner_of(first, second, third):
        kx = (1 - core) * first + core * second
        ky = core * first + (1 - core) * second
        return other_bit(bx, kx) + 2 * other_bit(by, ky) + 4 * other_bit(bz, third)

    barrier = pltpu.get_barrier_semaphore()
    everyone = [{"dp": chip, "seq": 1 - core}] + [{"dp": p, "seq": core} for p in partners]
    for device in everyone:
        pl.semaphore_signal(barrier, inc=1, device_id=device, device_id_type=MESH)

    own_rows = pl.ds(pl.multiple_of(core * half_tokens, half_tokens), half_tokens)
    own_cols = pl.ds(pl.multiple_of(core * cols, cols), cols)
    own_ff = pl.ds(pl.multiple_of(core * ff, ff), ff)

    def load(i, src, dst):
        return pltpu.make_async_copy(src, dst, load_sem.at[i])

    loads = [
        load(0, x_hbm, xs.at[own_rows]),
        load(1, wv_hbm.at[:, own_cols], wv),
        load(2, wq_hbm.at[:, own_cols], wq),
        load(3, wk_hbm.at[:, own_cols], wk),
        load(4, ids_hbm, ids.at[:, own_rows]),
        load(5, wo_hbm, wo),
        load(6, wg_hbm.at[:, own_ff], wg),
        load(7, wu_hbm.at[:, own_ff], wu),
        load(8, wd_hbm.at[own_ff, :], wd),
        load(9, dy_hbm, dys.at[own_rows]),
    ]
    for copy in loads:
        copy.start()

    def to_pair(i, src, dst):
        return pltpu.make_async_remote_copy(
            src_ref=src, dst_ref=dst, send_sem=pair_send.at[i], recv_sem=pair_recv.at[i],
            device_id={"dp": chip, "seq": 1 - core}, device_id_type=MESH,
        )

    send_x = to_pair(0, x_hbm, xs.at[own_rows])
    send_ids = to_pair(1, ids_hbm, ids.at[:, own_rows])
    send_dy = to_pair(2, dy_hbm, dys.at[own_rows])

    def rows_of(t):
        return pl.ds(pl.multiple_of(t * TB, TB), TB)

    def send_att(t):
        return to_pair(3 + t, att.at[rows_of(t)], att_other.at[rows_of(t)])

    def send_dn(t):
        return to_pair(7 + t, dn_own.at[rows_of(t)], dn_other.at[rows_of(t)])

    def send_out(t):
        return to_pair(11 + t, out_send.at[rows_of(t)], out_got.at[rows_of(t)])

    def send_dn1(t):
        return to_pair(13 + t, out_send.at[rows_of(t)], dn_got.at[rows_of(t)])

    def write_out(t):
        return pltpu.make_async_copy(out_got.at[rows_of(t)], block_out.at[rows_of(t)], load_sem.at[3 + t])

    def write_grad(t):
        return pltpu.make_async_copy(dn_got.at[rows_of(t)], input_grad.at[rows_of(t)], load_sem.at[5 + t])

    def send_final(i, first, count):
        rows = pl.ds(first, count)
        return to_pair(15 + i, final.at[1 - core, rows], final_got.at[rows])


    def hop(name, step):
        row, count, kind = chunks[name][:3]
        at = 4 * names.index(name) + step
        rows = pl.ds(row, count)
        if step < 3:
            n = 4 >> step
            src, dst = pack.at[pl.ds(n, n), rows], (got1, got2, got3)[step].at[:, rows]
        elif kind == "B":
            src, dst = pack.at[0, rows], got4.at[rows]
        else:
            src, dst = pack.at[0, pl.ds(row + count // 2, count // 2)], got4.at[pl.ds(row, count // 2)]
        return pltpu.make_async_remote_copy(
            src_ref=src, dst_ref=dst, send_sem=hop_send.at[at], recv_sem=hop_recv.at[at],
            device_id={"dp": partners[step], "seq": core}, device_id_type=MESH,
        )

    def start(name, step):
        if step == 3 and chunks[name][2] == "B":
            @pl.when(jnp.logical_not(holds))
            def _():
                hop(name, step).start()
        else:
            hop(name, step).start()

    def advance(name, step):
        row, count, kind, pieces, each, at = chunks[name]
        if step < 3:
            hop(name, step).wait_recv()
            n = 4 >> step
            size = 384 if count % 384 == 0 else (288 if count % 288 == 0 else count)
            source = (got1, got2, got3)[step]
            per = count // size

            def add(i, carry):
                slab = i // per
                rows = pl.ds(pl.multiple_of(row + (i % per) * size, 16), size)
                total = pack[slab, rows, :].astype(F32) + source[slab, rows, :].astype(F32)
                pack[slab, rows, :] = total.astype(BF)
                if step == 2:
                    acc[rows, :] = total
                return carry

            lax.fori_loop(0, n * per, add, 0)
            start(name, step + 1)
            return
        half = each // 2
        if kind == "B":
            @pl.when(holds)
            def _():
                hop(name, step).wait_recv()
                for p in range(pieces):
                    for c in range(2):
                        rows = pl.ds(row + p * each + c * half, half)
                        final[c, pl.ds(at + p * half, half), :] = acc[rows, :] + got4[rows, :].astype(F32)

            @pl.when(jnp.logical_not(holds))
            def _():
                hop(name, step).wait_send()
                for p in range(pieces):
                    for c in range(2):
                        final[c, pl.ds(at + p * half, half), :] = acc[pl.ds(row + p * each + c * half, half), :]
        else:
            hop(name, step).wait_recv()
            for p in range(pieces):
                for c in range(2):
                    rows = pl.ds(row + p * each + c * half, half)
                    final[c, pl.ds(at + p * half, half), :] = acc[rows, :] + got4[rows, :].astype(F32)

    def drain(name):
        for step in range(3):
            hop(name, step).wait_send()
        if chunks[name][2] == "A":
            hop(name, 3).wait_send()


    pl.semaphore_wait(barrier, len(everyone))
    send_x.start()
    send_ids.start()
    send_dy.start()
    for copy in loads[:4]:
        copy.wait()

    def project(j, carry):
        t = (core * half_blocks + j) % blocks

        @pl.when(j == half_blocks)
        def _():
            send_x.wait_recv()

        rows = rows_of(t)
        x = xs[rows, :].astype(F32)
        r = lax.rsqrt(jnp.mean(x * x, axis=-1, keepdims=True) + EPS)
        normed = (x * r * gain_one[...]).astype(BF)
        normed1[rows, :] = normed
        v_ref[rows, :] = nn(normed, wv[...]).astype(BF)
        q = nn(normed, wq[...]).astype(BF).astype(F32)
        k = nn(normed, wk[...]).astype(BF).astype(F32)
        for sub in range(TB // 64):
            cosine, sine, low_half = angle_block(tables, t * (TB // 64) + sub)
            at = pl.ds(pl.multiple_of(t * TB + sub * 64, 64), 64)
            for tile in range(cols // LANES):
                lanes = slice(tile * LANES, (tile + 1) * LANES)
                part = slice(sub * 64, (sub + 1) * 64)
                q_ref[at, lanes] = (rotate(q[part, lanes], cosine, sine, low_half).astype(BF) * BF(SCALE)).astype(BF)
                k_ref[at, lanes] = rotate(k[part, lanes], cosine, sine, low_half).astype(BF)
        return carry

    lax.fori_loop(0, blocks, project, 0)
    loads[4].wait()
    send_ids.wait_recv()
    seg_col[...] = jnp.transpose(jnp.broadcast_to(ids[...].astype(F32), (LANES, length)))

    def set_bias(block):
        first = window(block)
        keys = (block + 1) * TB - first
        rows = seg_col[pl.ds(block * TB, TB), 0:1]
        columns = ids[:, pl.ds(first, keys)].astype(F32)
        q_at = block * TB + lax.broadcasted_iota(jnp.int32, (TB, keys), 0)
        k_at = first + lax.broadcasted_iota(jnp.int32, (TB, keys), 1)
        bias_ref[:, :keys] = jnp.where((rows == columns) & (k_at <= q_at), 0.0, NEG).astype(F32)

    lane = lax.broadcasted_iota(jnp.int32, (1, LANES), 1)
    for block in range(blocks):
        first = window(block)
        keys = (block + 1) * TB - first
        set_bias(block)
        rows = pl.ds(block * TB, TB)
        span = pl.ds(first, keys)

        def head(h, carry, rows=rows, span=span, keys=keys):
            lanes = pl.ds(pl.multiple_of((h // 2) * LANES, LANES), LANES)
            mine = (lane // HD) == (h % 2)
            q = q_ref[rows, lanes]
            qm = jnp.where(mine, q, jnp.zeros_like(q))
            scores = nt(qm, k_ref[span, lanes]) + bias_ref[:, :keys]
            peak = jnp.max(scores, axis=-1, keepdims=True)
            weights = jnp.exp(scores - peak)
            total = jnp.sum(weights, axis=-1, keepdims=True)
            probs = (weights * (1.0 / total)).astype(BF)
            result = nn(probs, v_ref[span, lanes]).astype(BF)
            att[rows, lanes] = jnp.where(mine, result, att[rows, lanes])
            lse_ref[rows, :] = jnp.where(lane == h, peak + jnp.log(total), lse_ref[rows, :])
            return carry

        lax.fori_loop(0, cols // HD, head, 0)
        send_att(block).start()


    for copy in loads[5:]:
        copy.wait()
    send_dy.wait_recv()
    other_cols = pl.ds(pl.multiple_of((1 - core) * cols, cols), cols)

    def feed(t, carry):
        rows = rows_of(t)
        local = rows_of(t % half_blocks)
        is_own = t // half_blocks == core
        send_att(t).wait_recv()
        x = xs[rows, :].astype(F32)
        dy = dys[rows, :]
        residual = x + (nn(att[rows, :], wo[own_cols, :]) + nn(att_other[rows, :], wo[other_cols, :]))
        res_ref[rows, :] = residual
        r = lax.rsqrt(jnp.mean(residual * residual, axis=-1, keepdims=True) + EPS)
        n2 = (residual * r * gain_two[...]).astype(BF)
        normed2[rows, :] = n2
        gate = nn(n2, wg[...])
        up = nn(n2, wu[...])
        sig = 1.0 / (1.0 + jnp.exp(-gate))
        act = gate * sig
        hid = (act * up).astype(BF)
        hidden[rows, :] = hid
        d_hidden = nt(dy, wd[...])
        dg = (d_hidden * up * (sig * (1.0 + gate * (1.0 - sig)))).astype(BF)
        du = (d_hidden * act).astype(BF)
        d_gate[rows, :] = dg
        d_up[rows, :] = du
        dn_own[rows, :] = (nt(dg, wg[...]) + nt(du, wu[...])).astype(BF)
        send_dn(t).start()
        down = nn(hid, wd[...])

        @pl.when(is_own)
        def _():
            out_keep[local, :] = residual + down

        @pl.when(jnp.logical_not(is_own))
        def _():
            out_send[local, :] = down.astype(BF)
            send_out(t % half_blocks).start()

        return carry

    lax.fori_loop(0, blocks, feed, 0)

    wide = ff // 8
    pieces = width // LANES

    def gate_up(name, source, first):
        row = chunks[name][0]

        def slot(j, carry):
            owner = owner_of(first, j // 2, j % 2)
            cut = pl.ds(pl.multiple_of(owner * wide, wide), wide)
            grad = tn(source[:, cut], normed2[...]).astype(BF)
            for piece in range(pieces):
                pack[4 * first + j, pl.ds(row + piece * wide, wide), :] = grad[:, piece * LANES : (piece + 1) * LANES]
            return carry

        lax.fori_loop(0, 4, slot, 0)

    gate_up("gate", d_gate, 1)
    start("gate", 0)
    gate_up("gate", d_gate, 0)
    gate_up("up", d_up, 1)
    start("up", 0)
    gate_up("up", d_up, 0)

    def spread(name, piece, grad, count):
        row, rows = chunks[name][:2]
        for o in range(16):
            slot, far = slot_of(o)
            at = pl.multiple_of(row + far * (rows // 2) + piece * low, 16)
            pack[slot, pl.ds(at, low), :] = grad[o * low : (o + 1) * low, :]

    def down_piece(piece, carry):
        lanes = pl.ds(pl.multiple_of(piece * LANES, LANES), LANES)
        spread("down", piece, tn(dys[...], hidden[:, lanes]).astype(BF), 8)
        return carry

    lax.fori_loop(0, ff // LANES, down_piece, 0)
    start("down", 0)
    advance("gate", 0)


    d_branch, d_att = normed2, hidden
    gains[...] = jnp.zeros_like(gains)

    def norm_two(t, carry):
        rows = rows_of(t)
        local = rows_of(t % half_blocks)
        is_own = t // half_blocks == core
        send_dn(t).wait_recv()
        dy = dys[rows, :].astype(F32)
        residual = res_ref[rows, :]
        dn = dn_own[rows, :].astype(F32) + dn_other[rows, :].astype(F32)
        r = lax.rsqrt(jnp.mean(residual * residual, axis=-1, keepdims=True) + EPS)
        scaled = residual * r
        e = gain_two[...] * dn
        grad = dy + r * (e - scaled * (r * jnp.mean(e * residual, axis=-1, keepdims=True)))
        small = grad.astype(BF)
        d_branch[rows, :] = small
        d_att[rows, 0:cols] = nt(small, wo[own_cols, :]).astype(BF)

        @pl.when(is_own)
        def _():
            gains[0:1, :] += jnp.sum(dn * scaled, axis=0, keepdims=True)
            send_out(t % half_blocks).wait_recv()
            out_got[local, :] = (out_keep[local, :] + out_got[local, :].astype(F32)).astype(BF)
            write_out(t % half_blocks).start()
            out_keep[local, :] = grad

        return carry

    lax.fori_loop(0, blocks, norm_two, 0)
    d_res = out_keep

    def out_piece(piece, carry):
        lanes = pl.ds(pl.multiple_of(piece * LANES, LANES), LANES)
        spread("out", piece, tn(d_branch[...], att[:, lanes]).astype(BF), 3)
        return carry

    lax.fori_loop(0, cols // LANES, out_piece, 0)
    start("out", 0)

    res_ref[:, cols:] = jnp.zeros((length, cols), F32)
    dv_ref[...] = jnp.zeros_like(dv_ref)

    def attention_back(block, first_head, last_head):
        first = window(block)
        keys = (block + 1) * TB - first
        rows = pl.ds(block * TB, TB)
        span = pl.ds(first, keys)

        def head(h, carry):
            at = pl.multiple_of((h // 2) * LANES, LANES)
            lanes = pl.ds(at, LANES)
            k_lanes = pl.ds(pl.multiple_of(cols + at, LANES), LANES)
            mine = (lane // HD) == (h % 2)
            q = q_ref[rows, lanes]
            qm = jnp.where(mine, q, jnp.zeros_like(q))
            do = d_att[rows, lanes]
            dom = jnp.where(mine, do, jnp.zeros_like(do))
            lse = jnp.sum(jnp.where(lane == h, lse_ref[rows, :], 0.0), axis=-1, keepdims=True)
            k = k_ref[span, lanes]
            probs = jnp.exp(nt(qm, k) + (bias_ref[:, :keys] - lse))
            d_probs = nt(dom, v_ref[span, lanes])
            delta = jnp.sum(probs * d_probs, axis=-1, keepdims=True)
            ds = (probs * (d_probs - delta)).astype(BF)
            res_ref[rows, lanes] = jnp.where(mine, nn(ds, k), res_ref[rows, lanes])
            res_ref[span, k_lanes] += tn(ds, qm)
            dv_ref[span, lanes] += tn(probs.astype(BF), dom)
            return carry

        lax.fori_loop(first_head, last_head, head, 0)

    heads = cols // HD
    progress = {
        (0, 0): [("up", 0)],
        (1, 0): [("gate", 1)],
        (1, 1): [("down", 0)],
        (2, 0): [("up", 1), ("gate", 2)],
        (2, 1): [("out", 0), ("down", 1)],
        (3, 0): [("up", 2), ("out", 1)],
        (3, 1): [("down", 2), ("gate", 3)],
    }
    for block in range(blocks):
        set_bias(block)
        for part in range(2):
            attention_back(block, part * heads // 2, (part + 1) * heads // 2)
            for name, step in progress.get((block, part), ()):
                advance(name, step)

    def lower(t, carry):
        rows = rows_of(t)
        for sub in range(TB // 64):
            cosine, sine, low_half = angle_block(tables, t * (TB // 64) + sub)
            at = pl.ds(pl.multiple_of(t * TB + sub * 64, 64), 64)
            for tile in range(cols // LANES):
                lanes = slice(tile * LANES, (tile + 1) * LANES)
                k_lanes = slice(cols + tile * LANES, cols + (tile + 1) * LANES)
                d_gate[at, lanes] = (rotate(res_ref[at, lanes], cosine, -sine, low_half) * SCALE).astype(BF)
                d_gate[at, k_lanes] = rotate(res_ref[at, k_lanes], cosine, -sine, low_half).astype(BF)
        d_up[rows, 0:cols] = dv_ref[rows, :].astype(BF)
        return carry

    lax.fori_loop(0, blocks, lower, 0)

    def qkv(name, source, lanes_at):
        row = chunks[name][0]

        def piece_of(piece, carry):
            lanes = pl.ds(pl.multiple_of(piece * LANES, LANES), LANES)
            grad = tn(source[:, lanes_at : lanes_at + cols], normed1[:, lanes]).astype(BF)
            for o in range(8):
                at = pl.multiple_of(row + piece * low, 16)
                pack[slot_of(o)[0], pl.ds(at, low), :] = grad[o * low : (o + 1) * low, :]
            return carry

        lax.fori_loop(0, pieces, piece_of, 0)
        start(name, 0)

    qkv("value", d_up, 0)
    qkv("query", d_gate, 0)
    qkv("key", d_gate, cols)
    advance("up", 3)
    advance("out", 2)

    def finish(j, carry):
        t = ((1 - core) * half_blocks + j) % blocks
        rows = rows_of(t)
        local = rows_of(t % half_blocks)
        is_own = t // half_blocks == core
        dn = nt(d_gate[rows, 0:cols], wq[...]) + nt(d_gate[rows, cols : 2 * cols], wk[...]) + nt(d_up[rows, 0:cols], wv[...])
        x = xs[rows, :].astype(F32)
        r = lax.rsqrt(jnp.mean(x * x, axis=-1, keepdims=True) + EPS)
        gains[1:2, :] += jnp.sum(dn * (x * r), axis=0, keepdims=True)

        @pl.when(is_own)
        def _():
            dn_keep[local, :] = dn

        @pl.when(jnp.logical_not(is_own))
        def _():
            send_out(t % half_blocks).wait_send()
            out_send[local, :] = dn.astype(BF)
            send_dn1(t % half_blocks).start()

        return carry

    lax.fori_loop(0, blocks, finish, 0)
    turned = jnp.transpose(gains[...])
    turned_low = turned.astype(BF)
    rest = turned - turned_low.astype(F32)
    both = jnp.where(lane < LANES // 2, turned, pltpu.roll(rest, LANES // 2, 1)).astype(BF)
    spread("gains", 0, both, 1)
    start("gains", 0)
    advance("value", 0)

    def input_part(t, carry):
        local = rows_of(t)
        send_dn1(t).wait_recv()
        dn = dn_keep[local, :] + dn_got[local, :].astype(F32)
        x = xs[rows_of(core * half_blocks + t), :].astype(F32)
        r = lax.rsqrt(jnp.mean(x * x, axis=-1, keepdims=True) + EPS)
        e = gain_one[...] * dn
        grad = d_res[local, :] + r * e - x * (r * r * r) * jnp.mean(e * x, axis=-1, keepdims=True)
        dn_got[local, :] = grad.astype(BF)
        write_grad(t).start()
        return carry

    lax.fori_loop(0, half_blocks, input_part, 0)
    advance("query", 0)
    advance("value", 1)
    advance("down", 3)
    advance("out", 3)
    early = chunks["query"][5]
    send_final(0, 0, early).start()
    advance("key", 0)
    advance("query", 1)
    advance("value", 2)
    advance("gains", 0)
    advance("key", 1)
    advance("query", 2)
    advance("gains", 1)
    advance("key", 2)
    advance("gains", 2)
    advance("value", 3)
    advance("query", 3)
    advance("key", 3)
    advance("gains", 3)
    rows_final = final.shape[1]
    send_final(1, early, rows_final - early).start()
    mine_out = load(0, final.at[core], final_out.at[0])
    mine_out.start()
    send_final(0, 0, early).wait_recv()
    early_out = load(1, final_got.at[pl.ds(0, early)], final_out.at[1, pl.ds(0, early)])
    early_out.start()
    for name in names:
        drain(name)
    send_x.wait_send()
    send_ids.wait_send()
    send_dy.wait_send()
    for t in range(blocks):
        send_att(t).wait_send()
        send_dn(t).wait_send()
    for t in range(half_blocks):
        write_out(t).wait()
        write_grad(t).wait()
        send_dn1(t).wait_send()
    send_final(0, 0, early).wait_send()
    send_final(1, early, rows_final - early).wait()
    late = pl.ds(early, rows_final - early)
    late_out = load(2, final_got.at[late], final_out.at[1, late])
    late_out.start()
    mine_out.wait()
    early_out.wait()
    late_out.wait()


def fused_shards(
    tokens, segment_ids, norm1_gain, w_query, w_key, w_value, w_out, norm2_gain, w_gate, w_up, w_down, out_grad,
):
    seqs, half_tokens, width = tokens.shape
    length = 2 * half_tokens
    cols = w_query.shape[1] // 2
    ff = w_gate.shape[1] // 2
    chunks, rows, rows_final = layout_of(width, cols, ff)
    core = lax.axis_index("seq")
    chip = lax.axis_index("dp")
    tables = tuple(jnp.asarray(t) for t in small_tables(length))
    any_space = pl.BlockSpec(memory_space=pl.ANY)
    vmem = pl.BlockSpec(memory_space=pltpu.VMEM)

    def low(*dims):
        return pltpu.VMEM(dims, BF)

    def full(*dims):
        return pltpu.VMEM(dims, F32)

    scratch = [
        low(length, width), low(length, width), pltpu.VMEM((1, length), jnp.int32), full(length, LANES),
        low(width, cols), low(width, cols), low(width, cols), low(width, width), low(width, ff), low(width, ff), low(ff, width),
        low(length, width), low(length, cols), low(length, cols), low(length, cols), low(length, cols), low(length, cols),
        full(length, LANES), full(TB, 3 * TB),
        full(length, width), low(length, width), low(length, ff), low(length, ff), low(length, ff), low(length, width),
        low(length, width), full(half_tokens, width), low(half_tokens, width), low(half_tokens, width), full(length, cols),
        full(half_tokens, width), low(half_tokens, width),
        full(LANES, width), low(8, rows, LANES), low(4, rows, LANES), low(2, rows, LANES), low(1, rows, LANES), low(rows, LANES),
        full(rows, LANES), full(2, rows_final, LANES), full(rows_final, LANES),
        pltpu.SemaphoreType.DMA((10,)), pltpu.SemaphoreType.DMA((17,)), pltpu.SemaphoreType.DMA((17,)),
        pltpu.SemaphoreType.DMA((4 * len(chunks),)), pltpu.SemaphoreType.DMA((4 * len(chunks),)),
    ]
    block_out, input_grad, final = pl.pallas_call(
        block_kernel,
        out_shape=(shape(half_tokens, width), shape(half_tokens, width), shape(2, rows_final, LANES, dtype=F32)),
        in_specs=[any_space] * 10 + [vmem] * 6,
        out_specs=[any_space] * 3,
        scratch_shapes=scratch,
        compiler_params=pltpu.CompilerParams(
            vmem_limit_bytes=67043328, collective_id=0, has_side_effects=True,
        ),
        name="block",
    )(
        tokens.reshape(half_tokens, width), segment_ids.reshape(1, half_tokens), out_grad.reshape(half_tokens, width),
        w_query, w_key, w_value, w_out, w_gate, w_up, w_down,
        norm1_gain.astype(F32).reshape(1, width), norm2_gain.astype(F32).reshape(1, width), *tables,
    )
    mine, got = final[0], final[1]
    holds = (chip >> 3) == core

    def part(name):
        _, _, kind, pieces, each, at = chunks[name]
        half = each // 2
        cut = slice(at, at + pieces * half)
        a, b = mine[cut].reshape(pieces, half, LANES), got[cut].reshape(pieces, half, LANES)
        if kind == "B":
            taken = jnp.where(holds, a, b)
        else:
            taken = jnp.where(core == 0, jnp.concatenate([a, b]), jnp.concatenate([b, a]))
        return jnp.transpose(taken, (0, 2, 1)).reshape(-1, half)

    gains = part("gains")
    gains = gains[:LANES] + gains[LANES:]
    summed = (
        gains[1] + gains[1 + LANES // 2],
        part("query"),
        part("key"),
        part("value"),
        part("out"),
        gains[0] + gains[LANES // 2],
        part("gate"),
        part("up"),
        part("down"),
    )
    return (block_out.reshape(seqs, half_tokens, width), input_grad.reshape(seqs, half_tokens, width), *summed)


def solution(mesh):
    placed = (P("dp", "seq", None), P("dp", "seq"), *([P()] * 9), P("dp", "seq", None))
    column = P(None, AX)
    chips = mesh.shape["dp"]
    body = fused_shards if chips == 16 else functools.partial(shards, chips=chips)
    return jax.shard_map(
        body,
        mesh=mesh,
        in_specs=placed,
        out_specs=(
            P("dp", "seq", None), P("dp", "seq", None), P(AX), column, column, column, column, P(AX), column, column, column,
        ),
        check_vma=False,
    )
```

```python
import functools

import jax
import jax.numpy as jnp
import numpy as np
from jax import lax
from jax.experimental import pallas as pl
from jax.experimental.pallas import tpu as pltpu
from jax.sharding import PartitionSpec as P

HD = 64
EPS = 1e-06
SCALE = 0.125
NEG = -1e30
BASE = 10000.0
AX = ("dp", "seq")
BF = jnp.bfloat16
F32 = jnp.float32
TB = 256
LANES = 128


def nn(a, b):
    return lax.dot_general(a, b, (((1,), (0,)), ((), ())), preferred_element_type=F32)


def nt(a, b):
    return lax.dot_general(a, b, (((1,), (1,)), ((), ())), preferred_element_type=F32)


def tn(a, b):
    return lax.dot_general(a, b, (((0,), (0,)), ((), ())), preferred_element_type=F32)


def small_tables(length):
    freqs = BASE ** (-np.arange(HD // 2, dtype=np.float64) * (2.0 / HD))
    lane_freqs = np.tile(freqs, 4)[None, :]
    fine = np.arange(64, dtype=np.float64)[:, None] * lane_freqs
    coarse = 64.0 * np.arange(length // 64, dtype=np.float64)[:, None] * lane_freqs
    return tuple(
        np.asarray(t, np.float32) for t in (np.cos(fine), np.sin(fine), np.cos(coarse), np.sin(coarse))
    )


def angle_block(tables, sub):
    cos_f, sin_f, cos_c, sin_c = tables
    ca = cos_c[pl.ds(sub, 1), :]
    sa = sin_c[pl.ds(sub, 1), :]
    cb = cos_f[...]
    sb = sin_f[...]
    low_half = (lax.broadcasted_iota(jnp.int32, (64, LANES), 1) % HD) < HD // 2
    cosine = ca * cb - sa * sb
    sine = sa * cb + ca * sb
    return cosine, jnp.where(low_half, -sine, sine), low_half


def rotate(v, cosine, sine, low_half):
    partner = jnp.where(low_half, pltpu.roll(v, LANES - HD // 2, 1), pltpu.roll(v, HD // 2, 1))
    return v * cosine + partner * sine


def window(block):
    return max(0, (block - 2) * TB)


def bias_of(seg_col, seg_row, block):
    first = window(block)
    keys = (block + 1) * TB - first
    rows = seg_col[pl.ds(block * TB, TB), :]
    cols = seg_row[:, pl.ds(first, keys)]
    q_at = block * TB + lax.broadcasted_iota(jnp.int32, (TB, keys), 0)
    k_at = first + lax.broadcasted_iota(jnp.int32, (TB, keys), 1)
    return jnp.where((rows == cols) & (k_at <= q_at), 0.0, NEG).astype(F32)


def forward_attention(
    core, own_ref, other_ref, gain_ref, wq_ref, wk_ref, wv_ref, cos_f, sin_f, cos_c, sin_c, seg_col, seg_row,
    normed_ref, q_ref, k_ref, v_ref, att_ref, lse_ref, bias_ref,
):
    s = core[0]
    half_tokens, width = own_ref.shape
    length = 2 * half_tokens
    cols = wq_ref.shape[1]
    tables = (cos_f, sin_f, cos_c, sin_c)

    def project(t, carry):
        rows = pl.ds(pl.multiple_of(t * TB, TB), TB)
        part = t // (half_tokens // TB)
        local = pl.ds(pl.multiple_of((t % (half_tokens // TB)) * TB, TB), TB)
        x = jnp.where(part == s, own_ref[local, :], other_ref[local, :]).astype(F32)
        r = lax.rsqrt(jnp.mean(x * x, axis=-1, keepdims=True) + EPS)
        normed = (x * r * gain_ref[...]).astype(BF)
        normed_ref[rows, :] = normed
        v_ref[rows, :] = nn(normed, wv_ref[...]).astype(BF)
        q = nn(normed, wq_ref[...]).astype(BF).astype(F32)
        k = nn(normed, wk_ref[...]).astype(BF).astype(F32)
        for sub in range(TB // 64):
            cosine, sine, low_half = angle_block(tables, t * (TB // 64) + sub)
            at = pl.ds(pl.multiple_of(t * TB + sub * 64, 64), 64)
            for tile in range(cols // LANES):
                lanes = slice(tile * LANES, (tile + 1) * LANES)
                part_rows = slice(sub * 64, (sub + 1) * 64)
                q_ref[at, lanes] = (rotate(q[part_rows, lanes], cosine, sine, low_half).astype(BF) * BF(SCALE)).astype(BF)
                k_ref[at, lanes] = rotate(k[part_rows, lanes], cosine, sine, low_half).astype(BF)
        return carry

    lax.fori_loop(0, length // TB, project, 0)

    for block in range(length // TB):
        first = window(block)
        keys = (block + 1) * TB - first
        bias_ref[:, :keys] = bias_of(seg_col, seg_row, block)
        rows = pl.ds(block * TB, TB)
        span = pl.ds(first, keys)

        def head(h, carry):
            lanes = pl.ds(pl.multiple_of((h // 2) * LANES, LANES), LANES)
            lane = lax.broadcasted_iota(jnp.int32, (1, LANES), 1)
            mine = (lane // HD) == (h % 2)
            q = q_ref[rows, lanes]
            qm = jnp.where(mine, q, jnp.zeros_like(q))
            scores = nt(qm, k_ref[span, lanes]) + bias_ref[:, :keys]
            peak = jnp.max(scores, axis=-1, keepdims=True)
            weights = jnp.exp(scores - peak)
            total = jnp.sum(weights, axis=-1, keepdims=True)
            probs = (weights * (1.0 / total)).astype(BF)
            result = nn(probs, v_ref[span, lanes]).astype(BF)
            att_ref[rows, lanes] = jnp.where(mine, result, att_ref[rows, lanes])
            lse_ref[rows, :] = jnp.where(lane == h, peak + jnp.log(total), lse_ref[rows, :])
            return carry

        lax.fori_loop(0, cols // HD, head, 0)


def feed_forward(
    core, slots_a, slots_b, own_ref, other_ref, att_own, att_other, gain_ref, wo_ref, wg_ref, wu_ref, wd_ref,
    dy_own, dy_other,
    res_ref, out_keep, out_send, dn_ref, pack_ref, normed, hidden, d_gate, d_up, dy_all,
):
    s = core[0]
    half_tokens, width = own_ref.shape
    length = 2 * half_tokens
    cols = att_own.shape[1]
    own_rows = pl.ds(pl.multiple_of(s * cols, cols), cols)
    other_rows = pl.ds(pl.multiple_of((1 - s) * cols, cols), cols)

    def block(t, carry):
        rows = pl.ds(pl.multiple_of(t * TB, TB), TB)
        part = t // (half_tokens // TB)
        local = pl.ds(pl.multiple_of((t % (half_tokens // TB)) * TB, TB), TB)
        is_own = part == s
        x = jnp.where(is_own, own_ref[local, :], other_ref[local, :]).astype(F32)
        dy = jnp.where(is_own, dy_own[local, :], dy_other[local, :])
        dy_all[rows, :] = dy
        residual = x + (nn(att_own[rows, :], wo_ref[own_rows, :]) + nn(att_other[rows, :], wo_ref[other_rows, :]))
        res_ref[rows, :] = residual
        r = lax.rsqrt(jnp.mean(residual * residual, axis=-1, keepdims=True) + EPS)
        n2 = (residual * r * gain_ref[...]).astype(BF)
        normed[rows, :] = n2
        gate = nn(n2, wg_ref[...])
        up = nn(n2, wu_ref[...])
        sig = 1.0 / (1.0 + jnp.exp(-gate))
        act = gate * sig
        hid = (act * up).astype(BF)
        hidden[rows, :] = hid
        down = nn(hid, wd_ref[...])

        @pl.when(is_own)
        def _():
            out_keep[local, :] = residual + down

        @pl.when(jnp.logical_not(is_own))
        def _():
            out_send[local, :] = down.astype(BF)

        d_hidden = nt(dy, wd_ref[...])
        dg = (d_hidden * up * (sig * (1.0 + gate * (1.0 - sig)))).astype(BF)
        du = (d_hidden * act).astype(BF)
        d_gate[rows, :] = dg
        d_up[rows, :] = du
        dn_ref[rows, :] = (nt(dg, wg_ref[...]) + nt(du, wu_ref[...])).astype(BF)
        return carry

    lax.fori_loop(0, length // TB, block, 0)

    wide = wg_ref.shape[1] // 8
    pieces = width // LANES

    def gate_up(o, carry):
        cut = pl.ds(pl.multiple_of(o * wide, wide), wide)
        slot = slots_b[o]
        for which, source in ((0, d_gate), (1, d_up)):
            grad = tn(source[:, cut], normed[...]).astype(BF)
            for piece in range(pieces):
                pack_ref[slot, pl.ds((which * pieces + piece) * wide, wide), :] = grad[:, piece * LANES : (piece + 1) * LANES]
        return carry

    lax.fori_loop(0, 8, gate_up, 0)
    low = width // 16
    base = 2 * pieces * wide
    deep = hidden.shape[1] // LANES
    for piece in range(deep):
        grad = tn(dy_all[...], hidden[:, piece * LANES : (piece + 1) * LANES]).astype(BF)
        for o in range(16):
            slot = slots_a[o]
            at = pl.multiple_of(base + (slot % 2) * (deep * low) + piece * low, 16)
            pack_ref[slot // 2, pl.ds(at, low), :] = grad[o * low : (o + 1) * low, :]


def backward_attention(
    core, slots_a, slots_b, own_ref, other_ref, gain_one, gain_two, wq_ref, wk_ref, wv_ref, wo_ref, dy_own, dy_other,
    res_ref, dn_own, dn_other, att_ref, normed_ref, q_ref, k_ref, v_ref, lse_ref, cos_f, sin_f, cos_c, sin_c, seg_col, seg_row,
    d_res, dn_keep, dn_send, pack_ref, d_branch, d_att, dq, dk, dv, dq_low, dk_low, dv_low, gains, bias_ref,
):
    s = core[0]
    half_tokens, width = own_ref.shape
    length = 2 * half_tokens
    cols = att_ref.shape[1]
    tables = (cos_f, sin_f, cos_c, sin_c)
    gains[...] = jnp.zeros_like(gains)

    def norm_two(t, carry):
        rows = pl.ds(pl.multiple_of(t * TB, TB), TB)
        part = t // (half_tokens // TB)
        local = pl.ds(pl.multiple_of((t % (half_tokens // TB)) * TB, TB), TB)
        is_own = part == s
        dy = jnp.where(is_own, dy_own[local, :], dy_other[local, :]).astype(F32)
        residual = res_ref[rows, :]
        dn = dn_own[rows, :].astype(F32) + dn_other[rows, :].astype(F32)
        r = lax.rsqrt(jnp.mean(residual * residual, axis=-1, keepdims=True) + EPS)
        scaled = residual * r
        e = gain_two[...] * dn
        gains[0:1, :] += jnp.sum(dn * scaled, axis=0, keepdims=True)
        grad = dy + r * (e - scaled * (r * jnp.mean(e * residual, axis=-1, keepdims=True)))
        low = grad.astype(BF)
        d_branch[rows, :] = low

        @pl.when(is_own)
        def _():
            d_res[local, :] = grad

        d_att[rows, :] = nt(low, wo_ref[...]).astype(BF)
        return carry

    lax.fori_loop(0, length // TB, norm_two, 0)

    dk[...] = jnp.zeros_like(dk)
    dv[...] = jnp.zeros_like(dv)
    for block in range(length // TB):
        first = window(block)
        keys = (block + 1) * TB - first
        bias_ref[:, :keys] = bias_of(seg_col, seg_row, block)
        rows = pl.ds(block * TB, TB)
        span = pl.ds(first, keys)

        def head(h, carry):
            lanes = pl.ds(pl.multiple_of((h // 2) * LANES, LANES), LANES)
            lane = lax.broadcasted_iota(jnp.int32, (1, LANES), 1)
            mine = (lane // HD) == (h % 2)
            q = q_ref[rows, lanes]
            qm = jnp.where(mine, q, jnp.zeros_like(q))
            do = d_att[rows, lanes]
            dom = jnp.where(mine, do, jnp.zeros_like(do))
            lse = jnp.sum(jnp.where(lane == h, lse_ref[rows, :], 0.0), axis=-1, keepdims=True)
            k = k_ref[span, lanes]
            probs = jnp.exp(nt(qm, k) + (bias_ref[:, :keys] - lse))
            d_probs = nt(dom, v_ref[span, lanes])
            delta = jnp.sum(probs * d_probs, axis=-1, keepdims=True)
            ds = (probs * (d_probs - delta)).astype(BF)
            part = nn(ds, k)
            dq[rows, lanes] = jnp.where(mine, part, dq[rows, lanes])
            dk[span, lanes] += tn(ds, qm)
            dv[span, lanes] += tn(probs.astype(BF), dom)
            return carry

        lax.fori_loop(0, cols // HD, head, 0)

    def finish(t, carry):
        rows = pl.ds(pl.multiple_of(t * TB, TB), TB)
        part = t // (half_tokens // TB)
        local = pl.ds(pl.multiple_of((t % (half_tokens // TB)) * TB, TB), TB)
        is_own = part == s
        for sub in range(TB // 64):
            cosine, sine, low_half = angle_block(tables, t * (TB // 64) + sub)
            at = pl.ds(pl.multiple_of(t * TB + sub * 64, 64), 64)
            for tile in range(cols // LANES):
                lanes = slice(tile * LANES, (tile + 1) * LANES)
                dq_low[at, lanes] = (rotate(dq[at, lanes], cosine, -sine, low_half) * SCALE).astype(BF)
                dk_low[at, lanes] = rotate(dk[at, lanes], cosine, -sine, low_half).astype(BF)
        dv_low[rows, :] = dv[rows, :].astype(BF)
        dn = nt(dq_low[rows, :], wq_ref[...]) + nt(dk_low[rows, :], wk_ref[...]) + nt(dv_low[rows, :], wv_ref[...])
        x = jnp.where(is_own, own_ref[local, :], other_ref[local, :]).astype(F32)
        r = lax.rsqrt(jnp.mean(x * x, axis=-1, keepdims=True) + EPS)
        gains[1:2, :] += jnp.sum(dn * (x * r), axis=0, keepdims=True)

        @pl.when(is_own)
        def _():
            dn_keep[local, :] = dn

        @pl.when(jnp.logical_not(is_own))
        def _():
            dn_send[local, :] = dn.astype(BF)

        return carry

    lax.fori_loop(0, length // TB, finish, 0)

    low = width // 16
    pieces = width // LANES
    for which, source in ((0, dq_low), (1, dk_low), (2, dv_low)):
        for piece in range(pieces):
            grad = tn(source[...], normed_ref[:, piece * LANES : (piece + 1) * LANES]).astype(BF)
            for o in range(8):
                at = (which * pieces + piece) * low
                pack_ref[slots_b[o], pl.ds(at, low), :] = grad[o * low : (o + 1) * low, :]
    turned = jnp.transpose(gains[...])
    turned_low = turned.astype(BF)
    rest = (turned - turned_low.astype(F32)).astype(BF)
    lane = lax.broadcasted_iota(jnp.int32, (1, LANES), 1)
    both = jnp.where(lane < LANES // 2, turned_low, pltpu.roll(rest.astype(F32), LANES // 2, 1).astype(BF))
    at_b = 3 * pieces * low
    size_a = (cols // LANES + 1) * low
    base = at_b + low
    for piece in range(cols // LANES):
        grad = tn(d_branch[...], att_ref[:, piece * LANES : (piece + 1) * LANES]).astype(BF)
        for o in range(16):
            slot = slots_a[o]
            at = pl.multiple_of(base + (slot % 2) * size_a + piece * low, 16)
            pack_ref[slot // 2, pl.ds(at, low), :] = grad[o * low : (o + 1) * low, :]
    for o in range(16):
        slot = slots_a[o]
        at = pl.multiple_of(base + (slot % 2) * size_a + (cols // LANES) * low, 16)
        pack_ref[slot // 2, pl.ds(at, low), :] = both[o * low : (o + 1) * low, :]

        @pl.when(s == o // 8)
        def _():
            pack_ref[slots_b[o % 8], pl.ds(at_b, low), :] = both[o * low : (o + 1) * low, :]


BIG = pltpu.CompilerParams(vmem_limit_bytes=60 * 1024 * 1024)


def shape(*dims, dtype=BF):
    return jax.ShapeDtypeStruct(dims, dtype)


def flat(dp, core):
    return 2 * dp + core


def swap_cores(chips):
    return [(flat(d, c), flat(d, 1 - c)) for d in range(chips) for c in range(2)]


ORDER = ((0, 1, 2, 3), (1, 0, 2, 3))


def swap_chips(step):
    return [(flat(d, c), flat(d ^ (1 << ORDER[c][step]), c)) for d in range(16) for c in range(2)]


def to_owner_half():
    return [(flat(d, c), flat(d ^ 8, c)) for d in range(16) for c in range(2) if d // 8 != c]


def slot_tables(chip, core, chips):
    if chips != 16:
        return jnp.arange(16, dtype=jnp.int32), jnp.arange(8, dtype=jnp.int32)
    owner = jnp.arange(16, dtype=jnp.int32)
    away = owner ^ chip
    x, y, z0, z1 = away & 1, (away >> 1) & 1, (away >> 2) & 1, (away >> 3) & 1
    first = jnp.where(core == 0, x, y)
    second = jnp.where(core == 0, y, x)
    slots_a = first * 8 + second * 4 + z0 * 2 + z1
    near = slots_a // 2
    return slots_a, jnp.where(core == 0, near[:8], near[8:])


def halve(pack):
    for step in range(3):
        half = pack.shape[0] // 2
        pack3 = pack.reshape(2, half, *pack.shape[1:])
        got = lax.ppermute(pack3[1], AX, swap_chips(step))
        total = pack3[0].astype(F32) + got.astype(F32)
        pack = total.astype(BF) if step < 2 else total
    return pack[0]


def last_step(total, size_b):
    kind_b = total[:size_b]
    kind_a = total[size_b:].reshape(2, -1, LANES)
    got_a = lax.ppermute(kind_a[1].astype(BF), AX, swap_chips(3))
    got_b = lax.ppermute(kind_b.astype(BF), AX, to_owner_half())
    return kind_a[0] + got_a.astype(F32), kind_b + got_b.astype(F32)


def shards(
    tokens, segment_ids, norm1_gain, w_query, w_key, w_value, w_out, norm2_gain, w_gate, w_up, w_down, out_grad,
    *, chips,
):
    seqs, half_tokens, width = tokens.shape
    length = 2 * half_tokens
    cols = w_query.shape[1] // 2
    ff = w_gate.shape[1] // 2
    core = lax.axis_index("seq")
    chip = lax.axis_index("dp")
    core_id = core.reshape(1).astype(jnp.int32)
    pairs = swap_cores(chips)
    own = tokens.reshape(half_tokens, width)
    dy_own = out_grad.reshape(half_tokens, width)
    ids = segment_ids.reshape(1, half_tokens)
    other = lax.ppermute(own, AX, pairs)
    ids_other = lax.ppermute(ids, AX, pairs)
    dy_other = lax.ppermute(dy_own, AX, pairs)
    seg_row = jnp.where(core == 0, jnp.concatenate([ids, ids_other], 1), jnp.concatenate([ids_other, ids], 1))
    seg_col = seg_row.reshape(length, 1)
    gain_one = norm1_gain.astype(F32).reshape(1, width)
    gain_two = norm2_gain.astype(F32).reshape(1, width)
    tables = tuple(jnp.asarray(t) for t in small_tables(length))
    slots_a, slots_b = slot_tables(chip, core, chips)
    half_w = pl.BlockSpec((width, cols), lambda g, c: (0, c[0]))
    half_wide = pl.BlockSpec((width, ff), lambda g, c, a, b: (0, c[0]))
    whole = lambda a: pl.BlockSpec(a.shape, lambda g, *_: (0,) * len(a.shape))

    def out_block(s):
        return pl.BlockSpec(s.shape, lambda g, *_: (0,) * len(s.shape))

    outs = (
        shape(length, width), shape(length, cols), shape(length, cols), shape(length, cols), shape(length, cols),
        shape(length, LANES, dtype=F32),
    )
    normed1, q, k, v, att, lse = pl.pallas_call(
        forward_attention,
        out_shape=outs,
        grid_spec=pltpu.PrefetchScalarGridSpec(
            num_scalar_prefetch=1,
            grid=(1,),
            in_specs=[whole(own), whole(other), whole(gain_one), half_w, half_w, half_w]
            + [whole(t) for t in tables]
            + [whole(seg_col), whole(seg_row)],
            out_specs=[out_block(o) for o in outs],
            scratch_shapes=[pltpu.VMEM((TB, 3 * TB), F32)],
        ),
        compiler_params=BIG,
        name="attention_forward",
    )(core_id, own, other, gain_one, w_query, w_key, w_value, *tables, seg_col, seg_row)
    att_other = lax.ppermute(att, AX, pairs)

    rows_one = 2 * (width // LANES) * (ff // 8) + 2 * (ff // LANES) * (width // 16)
    outs = (
        shape(length, width, dtype=F32), shape(half_tokens, width, dtype=F32), shape(half_tokens, width),
        shape(length, width), shape(8, rows_one, LANES),
    )
    residual, out_keep, out_send, dn, pack_one = pl.pallas_call(
        feed_forward,
        out_shape=outs,
        grid_spec=pltpu.PrefetchScalarGridSpec(
            num_scalar_prefetch=3,
            grid=(1,),
            in_specs=[whole(own), whole(other), whole(att), whole(att), whole(gain_two), whole(w_out), half_wide, half_wide,
                      pl.BlockSpec((ff, width), lambda g, c, a, b: (c[0], 0)), whole(own), whole(own)],
            out_specs=[out_block(o) for o in outs],
            scratch_shapes=[
                pltpu.VMEM((length, width), BF), pltpu.VMEM((length, ff), BF), pltpu.VMEM((length, ff), BF),
                pltpu.VMEM((length, ff), BF), pltpu.VMEM((length, width), BF),
            ],
        ),
        compiler_params=BIG,
        name="feed_forward",
    )(core_id, slots_a, slots_b, own, other, att, att_other, gain_two, w_out, w_gate, w_up, w_down, dy_own, dy_other)
    out_other = lax.ppermute(out_send, AX, pairs)
    block_out = (out_keep + out_other.astype(F32)).astype(BF)
    dn_other = lax.ppermute(dn, AX, pairs)

    low = width // 16
    size_b2 = 3 * (width // LANES) * low + low
    size_a2 = (cols // LANES + 1) * low
    outs = (
        shape(half_tokens, width, dtype=F32), shape(half_tokens, width, dtype=F32), shape(half_tokens, width),
        shape(8, size_b2 + 2 * size_a2, LANES),
    )
    half_w3 = pl.BlockSpec((width, cols), lambda g, c, a, b: (0, c[0]))
    inputs = (own, other, gain_one, gain_two, w_query, w_key, w_value, w_out, dy_own, dy_other, residual, dn, dn_other,
              att, normed1, q, k, v, lse, *tables, seg_col, seg_row)
    specs = [whole(a) for a in inputs]
    specs[4] = specs[5] = specs[6] = half_w3
    specs[7] = pl.BlockSpec((cols, width), lambda g, c, a, b: (c[0], 0))
    d_res, dn_keep, dn_send, pack_two = pl.pallas_call(
        backward_attention,
        out_shape=outs,
        grid_spec=pltpu.PrefetchScalarGridSpec(
            num_scalar_prefetch=3,
            grid=(1,),
            in_specs=specs,
            out_specs=[out_block(o) for o in outs],
            scratch_shapes=[
                pltpu.VMEM((length, width), BF), pltpu.VMEM((length, cols), BF),
                pltpu.VMEM((length, cols), F32), pltpu.VMEM((length, cols), F32), pltpu.VMEM((length, cols), F32),
                pltpu.VMEM((length, cols), BF), pltpu.VMEM((length, cols), BF), pltpu.VMEM((length, cols), BF),
                pltpu.VMEM((LANES, width), F32), pltpu.VMEM((TB, 3 * TB), F32),
            ],
        ),
        compiler_params=BIG,
        name="attention_backward",
    )(core_id, slots_a, slots_b, *inputs)
    dn1 = dn_keep + lax.ppermute(dn_send, AX, pairs).astype(F32)
    x = own.astype(F32)
    r = lax.rsqrt(jnp.mean(x * x, axis=-1, keepdims=True) + EPS)
    e = gain_one * dn1
    input_grad = (d_res + r * e - x * (r * r * r) * jnp.mean(e * x, axis=-1, keepdims=True)).astype(BF)

    pieces = width // LANES
    wide = ff // 8
    size_b1 = 2 * pieces * wide
    size_a1 = (ff // LANES) * low

    if chips == 16:
        one_a, one_b = last_step(halve(pack_one), size_b1)
        two_a, two_b = last_step(halve(pack_two), size_b2)
        holds = (chip >> 3) == core

        def share(a):
            parts = a.reshape(a.shape[0], 2, a.shape[1] // 2, LANES)
            mine = jnp.where(core == 0, parts[:, 0], parts[:, 1])
            theirs = jnp.where(core == 0, parts[:, 1], parts[:, 0])
            return mine, lax.ppermute(theirs, AX, pairs)

        def both(a):
            mine, got = share(a)
            return jnp.where(core == 0, mine, got), jnp.where(core == 0, got, mine)

        def one(a):
            mine, got = share(a)
            return jnp.where(holds, mine, got)

        down_lo, down_hi = both(one_a.reshape(ff // LANES, low, LANES))
        kind_a = two_a.reshape(cols // LANES + 1, low, LANES)
        out_lo, out_hi = both(kind_a)
        gates = one(one_b.reshape(2 * pieces, wide, LANES))
        rest = one(two_b.reshape(3 * pieces + 1, low, LANES))

        def turn(a):
            return jnp.transpose(a, (0, 2, 1)).reshape(-1, a.shape[1])

        tiles = cols // LANES
        gain1 = out_lo[tiles] + out_hi[tiles]
        gain1 = gain1[:, 1] + gain1[:, 1 + LANES // 2]
        gain2 = rest[3 * pieces]
        gain2 = gain2[:, 0] + gain2[:, LANES // 2]
        summed = (
            gain1,
            turn(rest[:pieces]),
            turn(rest[pieces : 2 * pieces]),
            turn(rest[2 * pieces : 3 * pieces]),
            turn(jnp.concatenate([out_lo[:tiles], out_hi[:tiles]])),
            gain2,
            turn(gates[:pieces]),
            turn(gates[pieces:]),
            turn(jnp.concatenate([down_lo, down_hi])),
        )
    else:
        def plain_b(rows, count, size, at):
            part = rows[:, at : at + count * size].reshape(8, count, size, LANES)
            part = jnp.transpose(part, (1, 3, 0, 2)).reshape(count * LANES, 8 * size).astype(F32)
            zero = jnp.zeros_like(part)
            return jnp.where(core == 0, jnp.concatenate([part, zero], 1), jnp.concatenate([zero, part], 1))

        def plain_a(rows, count, at, each):
            part = rows[:, at:].reshape(8, 2, each, low, LANES)[:, :, :count].reshape(16, count, low, LANES)
            part = jnp.transpose(part, (1, 3, 0, 2)).reshape(count * LANES, 16 * low).astype(F32)
            zero = jnp.zeros_like(part)
            return jnp.where(core == 0, jnp.concatenate([part, zero], 0), jnp.concatenate([zero, part], 0))

        def scatter(a):
            return lax.psum_scatter(a, AX, scatter_dimension=1, tiled=True)

        tiles = cols // LANES
        gain_a = pack_two[:, size_b2:].reshape(16, tiles + 1, low, LANES)[:, tiles].astype(F32)
        gain_a = gain_a[:, :, : LANES // 2] + gain_a[:, :, LANES // 2 :]
        gain_a = gain_a.reshape(width, LANES // 2)
        gain1 = gain_a[:, 1].reshape(1, width)
        gain2 = jnp.where(core == 0, gain_a[:, 0], 0.0).reshape(1, width)
        n = pieces * low
        summed = (
            scatter(gain1).reshape(-1),
            scatter(plain_b(pack_two, pieces, low, 0)),
            scatter(plain_b(pack_two, pieces, low, n)),
            scatter(plain_b(pack_two, pieces, low, 2 * n)),
            scatter(plain_a(pack_two, tiles, size_b2, tiles + 1)),
            scatter(gain2).reshape(-1),
            scatter(plain_b(pack_one, pieces, wide, 0)),
            scatter(plain_b(pack_one, pieces, wide, pieces * wide)),
            scatter(plain_a(pack_one, ff // LANES, size_b1, ff // LANES)),
        )
    return (block_out.reshape(seqs, half_tokens, width), input_grad.reshape(seqs, half_tokens, width), *summed)


MESH = pl.DeviceIdType.MESH


def bit(value, place):
    return (value // (1 << place)) % 2


def other_bit(a, b):
    return a + b - 2 * a * b


def layout_of(width, cols, ff):
    low, wide = width // 16, ff // 8
    table, row, final = {}, 0, 0
    for name, kind, pieces, each in (
        ("gate", "B", width // LANES, wide), ("up", "B", width // LANES, wide), ("down", "A", ff // LANES, low),
        ("out", "A", cols // LANES, low), ("query", "B", width // LANES, low), ("key", "B", width // LANES, low),
        ("value", "B", width // LANES, low), ("gains", "A", 1, low),
    ):
        rows = pieces * each * (2 if kind == "A" else 1)
        table[name] = (row, rows, kind, pieces, each, final)
        row, final = row + rows, final + pieces * each // 2
    return table, row, final


def block_kernel(
    x_hbm, ids_hbm, dy_hbm, wq_hbm, wk_hbm, wv_hbm, wo_hbm, wg_hbm, wu_hbm, wd_hbm, gain_one, gain_two,
    cos_f, sin_f, cos_c, sin_c,
    block_out, input_grad, final_out,
    xs, dys, ids, wq, wk, wv, wo, wg, wu, wd, normed1, q_ref, k_ref, v_ref, att, att_other, lse_ref, bias_ref,
    res_ref, normed2, hidden, d_gate, d_up, dn_own, dn_other, out_keep, out_send, out_got, dv_ref, dn_keep, dn_got,
    gains, pack, got1, got2, got3, got4, acc, final, final_got,
    load_sem, pair_send, pair_recv, hop_send, hop_recv,
):
    core = lax.axis_index("seq")
    chip = lax.axis_index("dp")
    half_tokens, width = x_hbm.shape
    length = 2 * half_tokens
    cols = wq.shape[1]
    ff = wg.shape[1]
    blocks = length // TB
    half_blocks = half_tokens // TB
    tables = (cos_f, sin_f, cos_c, sin_c)
    chunks, _, _ = layout_of(width, cols, ff)
    names = list(chunks)
    low = width // 16

    bx, by, bz, bw = (bit(chip, i) for i in range(4))
    step_x, step_y = 1 - 2 * bx, 2 * (1 - 2 * by)
    partners = (
        chip + (1 - core) * step_x + core * step_y,
        chip + core * step_x + (1 - core) * step_y,
        chip + 4 * (1 - 2 * bz),
        chip + 8 * (1 - 2 * bw),
    )
    holds = bw == core

    def slot_of(owner):
        kx, ky, kz = other_bit(bx, owner & 1), other_bit(by, (owner >> 1) & 1), other_bit(bz, (owner >> 2) & 1)
        first = (1 - core) * kx + core * ky
        second = core * kx + (1 - core) * ky
        return first * 4 + second * 2 + kz, other_bit(bw, (owner >> 3) & 1)

    def owner_of(first, second, third):
        kx = (1 - core) * first + core * second
        ky = core * first + (1 - core) * second
        return other_bit(bx, kx) + 2 * other_bit(by, ky) + 4 * other_bit(bz, third)

    barrier = pltpu.get_barrier_semaphore()
    everyone = [{"dp": chip, "seq": 1 - core}] + [{"dp": p, "seq": core} for p in partners]
    for device in everyone:
        pl.semaphore_signal(barrier, inc=1, device_id=device, device_id_type=MESH)

    own_rows = pl.ds(pl.multiple_of(core * half_tokens, half_tokens), half_tokens)
    own_cols = pl.ds(pl.multiple_of(core * cols, cols), cols)
    own_ff = pl.ds(pl.multiple_of(core * ff, ff), ff)

    def load(i, src, dst):
        return pltpu.make_async_copy(src, dst, load_sem.at[i])

    loads = [
        load(0, x_hbm, xs.at[own_rows]),
        load(1, wv_hbm.at[:, own_cols], wv),
        load(2, wq_hbm.at[:, own_cols], wq),
        load(3, wk_hbm.at[:, own_cols], wk),
        load(4, ids_hbm, ids.at[:, own_rows]),
        load(5, wo_hbm, wo),
        load(6, wg_hbm.at[:, own_ff], wg),
        load(7, wu_hbm.at[:, own_ff], wu),
        load(8, wd_hbm.at[own_ff, :], wd),
        load(9, dy_hbm, dys.at[own_rows]),
    ]
    for copy in loads:
        copy.start()

    def to_pair(i, src, dst):
        return pltpu.make_async_remote_copy(
            src_ref=src, dst_ref=dst, send_sem=pair_send.at[i], recv_sem=pair_recv.at[i],
            device_id={"dp": chip, "seq": 1 - core}, device_id_type=MESH,
        )

    send_x = to_pair(0, x_hbm, xs.at[own_rows])
    send_ids = to_pair(1, ids_hbm, ids.at[:, own_rows])
    send_dy = to_pair(2, dy_hbm, dys.at[own_rows])

    def rows_of(t):
        return pl.ds(pl.multiple_of(t * TB, TB), TB)

    def send_att(t):
        return to_pair(3 + t, att.at[rows_of(t)], att_other.at[rows_of(t)])

    def send_dn(t):
        return to_pair(7 + t, dn_own.at[rows_of(t)], dn_other.at[rows_of(t)])

    def send_out(t):
        return to_pair(11 + t, out_send.at[rows_of(t)], out_got.at[rows_of(t)])

    def send_dn1(t):
        return to_pair(13 + t, out_send.at[rows_of(t)], dn_got.at[rows_of(t)])

    def write_out(t):
        return pltpu.make_async_copy(out_got.at[rows_of(t)], block_out.at[rows_of(t)], load_sem.at[3 + t])

    def write_grad(t):
        return pltpu.make_async_copy(dn_got.at[rows_of(t)], input_grad.at[rows_of(t)], load_sem.at[5 + t])

    def send_final(i, first, count):
        rows = pl.ds(first, count)
        return to_pair(15 + i, final.at[1 - core, rows], final_got.at[rows])


    def hop(name, step):
        row, count, kind = chunks[name][:3]
        at = 4 * names.index(name) + step
        rows = pl.ds(row, count)
        if step < 3:
            n = 4 >> step
            src, dst = pack.at[pl.ds(n, n), rows], (got1, got2, got3)[step].at[:, rows]
        elif kind == "B":
            src, dst = pack.at[0, rows], got4.at[rows]
        else:
            src, dst = pack.at[0, pl.ds(row + count // 2, count // 2)], got4.at[pl.ds(row, count // 2)]
        return pltpu.make_async_remote_copy(
            src_ref=src, dst_ref=dst, send_sem=hop_send.at[at], recv_sem=hop_recv.at[at],
            device_id={"dp": partners[step], "seq": core}, device_id_type=MESH,
        )

    def start(name, step):
        if step == 3 and chunks[name][2] == "B":
            @pl.when(jnp.logical_not(holds))
            def _():
                hop(name, step).start()
        else:
            hop(name, step).start()

    def advance(name, step):
        row, count, kind, pieces, each, at = chunks[name]
        if step < 3:
            hop(name, step).wait_recv()
            n = 4 >> step
            size = 384 if count % 384 == 0 else (288 if count % 288 == 0 else count)
            source = (got1, got2, got3)[step]
            per = count // size

            def add(i, carry):
                slab = i // per
                rows = pl.ds(pl.multiple_of(row + (i % per) * size, 16), size)
                total = pack[slab, rows, :].astype(F32) + source[slab, rows, :].astype(F32)
                pack[slab, rows, :] = total.astype(BF)
                if step == 2:
                    acc[rows, :] = total
                return carry

            lax.fori_loop(0, n * per, add, 0)
            start(name, step + 1)
            return
        half = each // 2
        if kind == "B":
            @pl.when(holds)
            def _():
                hop(name, step).wait_recv()
                for p in range(pieces):
                    for c in range(2):
                        rows = pl.ds(row + p * each + c * half, half)
                        final[c, pl.ds(at + p * half, half), :] = acc[rows, :] + got4[rows, :].astype(F32)

            @pl.when(jnp.logical_not(holds))
            def _():
                hop(name, step).wait_send()
                for p in range(pieces):
                    for c in range(2):
                        final[c, pl.ds(at + p * half, half), :] = acc[pl.ds(row + p * each + c * half, half), :]
        else:
            hop(name, step).wait_recv()
            for p in range(pieces):
                for c in range(2):
                    rows = pl.ds(row + p * each + c * half, half)
                    final[c, pl.ds(at + p * half, half), :] = acc[rows, :] + got4[rows, :].astype(F32)

    def drain(name):
        for step in range(3):
            hop(name, step).wait_send()
        if chunks[name][2] == "A":
            hop(name, 3).wait_send()


    pl.semaphore_wait(barrier, len(everyone))
    send_x.start()
    send_ids.start()
    send_dy.start()
    for copy in loads[:4]:
        copy.wait()

    def project(j, carry):
        t = (core * half_blocks + j) % blocks

        @pl.when(j == half_blocks)
        def _():
            send_x.wait_recv()

        rows = rows_of(t)
        x = xs[rows, :].astype(F32)
        r = lax.rsqrt(jnp.mean(x * x, axis=-1, keepdims=True) + EPS)
        normed = (x * r * gain_one[...]).astype(BF)
        normed1[rows, :] = normed
        v_ref[rows, :] = nn(normed, wv[...]).astype(BF)
        q = nn(normed, wq[...]).astype(BF).astype(F32)
        k = nn(normed, wk[...]).astype(BF).astype(F32)
        for sub in range(TB // 64):
            cosine, sine, low_half = angle_block(tables, t * (TB // 64) + sub)
            at = pl.ds(pl.multiple_of(t * TB + sub * 64, 64), 64)
            for tile in range(cols // LANES):
                lanes = slice(tile * LANES, (tile + 1) * LANES)
                part = slice(sub * 64, (sub + 1) * 64)
                q_ref[at, lanes] = (rotate(q[part, lanes], cosine, sine, low_half).astype(BF) * BF(SCALE)).astype(BF)
                k_ref[at, lanes] = rotate(k[part, lanes], cosine, sine, low_half).astype(BF)
        return carry

    lax.fori_loop(0, blocks, project, 0)
    loads[4].wait()
    send_ids.wait_recv()
    lse_ref[...] = jnp.transpose(jnp.broadcast_to(ids[...].astype(F32), (LANES, length)))

    def set_bias(block):
        first = window(block)
        keys = (block + 1) * TB - first
        rows = lse_ref[pl.ds(block * TB, TB), LANES - 1 :]
        columns = ids[:, pl.ds(first, keys)].astype(F32)
        q_at = block * TB + lax.broadcasted_iota(jnp.int32, (TB, keys), 0)
        k_at = first + lax.broadcasted_iota(jnp.int32, (TB, keys), 1)
        bias_ref[:, :keys] = jnp.where((rows == columns) & (k_at <= q_at), 0.0, NEG).astype(F32)

    lane = lax.broadcasted_iota(jnp.int32, (1, LANES), 1)
    first_head = lane < HD
    for block in range(blocks):
        first = window(block)
        keys = (block + 1) * TB - first
        set_bias(block)
        rows = pl.ds(block * TB, TB)
        span = pl.ds(first, keys)

        def pair(j, carry, rows=rows, span=span, keys=keys):
            lanes = pl.ds(pl.multiple_of(j * LANES, LANES), LANES)
            q, k, v = q_ref[rows, lanes], k_ref[span, lanes], v_ref[span, lanes]
            results, sums = [], []
            for mine in (first_head, jnp.logical_not(first_head)):
                scores = nt(jnp.where(mine, q, jnp.zeros_like(q)), k) + bias_ref[:, :keys]
                peak = jnp.max(scores, axis=-1, keepdims=True)
                weights = jnp.exp(scores - peak)
                total = jnp.sum(weights, axis=-1, keepdims=True)
                results.append(nn(weights.astype(BF), v) * (1.0 / total))
                sums.append(peak + jnp.log(total))
            att[rows, lanes] = jnp.where(first_head, *results).astype(BF)
            old = jnp.where(lane == 2 * j + 1, sums[1], lse_ref[rows, :])
            lse_ref[rows, :] = jnp.where(lane == 2 * j, sums[0], old)
            return carry

        lax.fori_loop(0, cols // LANES, pair, 0)
        send_att(block).start()


    for copy in loads[5:]:
        copy.wait()
    send_dy.wait_recv()
    other_cols = pl.ds(pl.multiple_of((1 - core) * cols, cols), cols)

    def feed(t, carry):
        rows = rows_of(t)
        local = rows_of(t % half_blocks)
        is_own = t // half_blocks == core
        send_att(t).wait_recv()
        x = xs[rows, :].astype(F32)
        dy = dys[rows, :]
        residual = x + (nn(att[rows, :], wo[own_cols, :]) + nn(att_other[rows, :], wo[other_cols, :]))
        res_ref[rows, :] = residual
        r = lax.rsqrt(jnp.mean(residual * residual, axis=-1, keepdims=True) + EPS)
        n2 = (residual * r * gain_two[...]).astype(BF)
        normed2[rows, :] = n2
        gate = nn(n2, wg[...])
        up = nn(n2, wu[...])
        sig = 1.0 / (1.0 + jnp.exp(-gate))
        act = gate * sig
        hid = (act * up).astype(BF)
        hidden[rows, :] = hid
        d_hidden = nt(dy, wd[...])
        dg = (d_hidden * up * (sig * (1.0 + gate * (1.0 - sig)))).astype(BF)
        du = (d_hidden * act).astype(BF)
        d_gate[rows, :] = dg
        d_up[rows, :] = du
        dn_own[rows, :] = (nt(dg, wg[...]) + nt(du, wu[...])).astype(BF)
        send_dn(t).start()
        down = nn(hid, wd[...])

        @pl.when(is_own)
        def _():
            out_keep[local, :] = residual + down

        @pl.when(jnp.logical_not(is_own))
        def _():
            out_send[local, :] = down.astype(BF)
            send_out(t % half_blocks).start()

        return carry

    lax.fori_loop(0, blocks, feed, 0)

    wide = ff // 8
    pieces = width // LANES

    def gate_up(name, source, first):
        row = chunks[name][0]

        cuts = []
        for j in range(4):
            owner = owner_of(first, j // 2, j % 2)
            cuts.append(source[:, pl.ds(pl.multiple_of(owner * wide, wide), wide)])
        grad = tn(jnp.concatenate(cuts, axis=1), normed2[...]).astype(BF)
        for j in range(4):
            for piece in range(pieces):
                part = grad[j * wide : (j + 1) * wide, piece * LANES : (piece + 1) * LANES]
                pack[4 * first + j, pl.ds(row + piece * wide, wide), :] = part

    gate_up("gate", d_gate, 1)
    start("gate", 0)
    gate_up("gate", d_gate, 0)
    gate_up("up", d_up, 1)
    start("up", 0)
    gate_up("up", d_up, 0)

    def spread(name, piece, grad):
        row, rows = chunks[name][:2]
        for o in range(16):
            slot, far = slot_of(o)
            at = pl.multiple_of(row + far * (rows // 2) + piece * low, 16)
            pack[slot, pl.ds(at, low), :] = grad[o * low : (o + 1) * low, :]

    def down_part(part, carry):
        at = part * (ff // 2)
        grad = tn(dys[...], hidden[:, pl.ds(pl.multiple_of(at, LANES), ff // 2)]).astype(BF)
        for piece in range(ff // 2 // LANES):
            spread("down", part * (ff // 2 // LANES) + piece, grad[:, piece * LANES : (piece + 1) * LANES])
        return carry

    lax.fori_loop(0, 2, down_part, 0)
    start("down", 0)
    advance("gate", 0)


    d_branch, d_att = normed2, hidden
    gains[...] = jnp.zeros_like(gains)

    def norm_two(t, carry):
        rows = rows_of(t)
        local = rows_of(t % half_blocks)
        is_own = t // half_blocks == core
        send_dn(t).wait_recv()
        dy = dys[rows, :].astype(F32)
        residual = res_ref[rows, :]
        dn = dn_own[rows, :].astype(F32) + dn_other[rows, :].astype(F32)
        r = lax.rsqrt(jnp.mean(residual * residual, axis=-1, keepdims=True) + EPS)
        scaled = residual * r
        e = gain_two[...] * dn
        grad = dy + r * (e - scaled * (r * jnp.mean(e * residual, axis=-1, keepdims=True)))
        small = grad.astype(BF)
        d_branch[rows, :] = small
        d_att[rows, 0:cols] = nt(small, wo[own_cols, :]).astype(BF)

        @pl.when(is_own)
        def _():
            gains[0:1, :] += jnp.sum(dn * scaled, axis=0, keepdims=True)
            send_out(t % half_blocks).wait_recv()
            out_got[local, :] = (out_keep[local, :] + out_got[local, :].astype(F32)).astype(BF)
            write_out(t % half_blocks).start()
            out_keep[local, :] = grad

        return carry

    lax.fori_loop(0, blocks, norm_two, 0)
    d_res = out_keep

    out_grad = tn(d_branch[...], att[...]).astype(BF)
    for piece in range(cols // LANES):
        spread("out", piece, out_grad[:, piece * LANES : (piece + 1) * LANES])
    start("out", 0)

    res_ref[:, cols:] = jnp.zeros((length, cols), F32)
    dv_ref[...] = jnp.zeros_like(dv_ref)

    def attention_back(block, first_pair, last_pair):
        first = window(block)
        keys = (block + 1) * TB - first
        rows = pl.ds(block * TB, TB)
        span = pl.ds(first, keys)

        def pair(j, carry):
            at = pl.multiple_of(j * LANES, LANES)
            lanes = pl.ds(at, LANES)
            k_lanes = pl.ds(pl.multiple_of(cols + at, LANES), LANES)
            q, do, k, v = q_ref[rows, lanes], d_att[rows, lanes], k_ref[span, lanes], v_ref[span, lanes]
            products = do.astype(F32) * att[rows, lanes].astype(F32)
            q_parts, do_parts, probs_parts, ds_parts, dq_parts = [], [], [], [], []
            for h, mine in enumerate((first_head, jnp.logical_not(first_head))):
                q_parts.append(jnp.where(mine, q, jnp.zeros_like(q)))
                do_parts.append(jnp.where(mine, do, jnp.zeros_like(do)))
                lse = jnp.sum(jnp.where(lane == 2 * j + h, lse_ref[rows, :], 0.0), axis=-1, keepdims=True)
                delta = jnp.sum(jnp.where(mine, products, 0.0), axis=-1, keepdims=True)
                probs = jnp.exp(nt(q_parts[h], k) + (bias_ref[:, :keys] - lse))
                ds = (probs * (nt(do_parts[h], v) - delta)).astype(BF)
                probs_parts.append(probs.astype(BF))
                ds_parts.append(ds)
                dq_parts.append(nn(ds, k))
            res_ref[rows, lanes] = jnp.where(first_head, *dq_parts)
            res_ref[span, k_lanes] += tn(jnp.concatenate(ds_parts), jnp.concatenate(q_parts))
            dv_ref[span, lanes] += tn(jnp.concatenate(probs_parts), jnp.concatenate(do_parts))
            return carry

        lax.fori_loop(first_pair, last_pair, pair, 0)

    tiles = cols // LANES
    progress = {
        (0, 0): [("up", 0)],
        (1, 0): [("gate", 1)],
        (1, 1): [("down", 0)],
        (2, 0): [("up", 1), ("gate", 2)],
        (2, 1): [("out", 0), ("down", 1)],
        (3, 0): [("up", 2), ("out", 1)],
        (3, 1): [("down", 2), ("gate", 3)],
    }
    for block in range(blocks):
        set_bias(block)
        for part in range(2):
            attention_back(block, *((0, tiles - 1), (tiles - 1, tiles))[part])
            for name, step in progress.get((block, part), ()):
                advance(name, step)

    def lower(t, carry):
        rows = rows_of(t)
        for sub in range(TB // 64):
            cosine, sine, low_half = angle_block(tables, t * (TB // 64) + sub)
            at = pl.ds(pl.multiple_of(t * TB + sub * 64, 64), 64)
            for tile in range(cols // LANES):
                lanes = slice(tile * LANES, (tile + 1) * LANES)
                k_lanes = slice(cols + tile * LANES, cols + (tile + 1) * LANES)
                d_gate[at, lanes] = (rotate(res_ref[at, lanes], cosine, -sine, low_half) * SCALE).astype(BF)
                d_gate[at, k_lanes] = rotate(res_ref[at, k_lanes], cosine, -sine, low_half).astype(BF)
        d_up[rows, 0:cols] = dv_ref[rows, :].astype(BF)
        return carry

    lax.fori_loop(0, blocks, lower, 0)

    def qkv(name, source, lanes_at):
        row = chunks[name][0]

        grad = tn(source[:, lanes_at : lanes_at + cols], normed1[...]).astype(BF)
        for o in range(8):
            slot = slot_of(o)[0]
            for piece in range(pieces):
                part = grad[o * low : (o + 1) * low, piece * LANES : (piece + 1) * LANES]
                pack[slot, pl.ds(row + piece * low, low), :] = part
        start(name, 0)

    qkv("value", d_up, 0)
    qkv("query", d_gate, 0)
    qkv("key", d_gate, cols)
    advance("up", 3)
    advance("out", 2)

    def finish(j, carry):
        t = ((1 - core) * half_blocks + j) % blocks
        rows = rows_of(t)
        local = rows_of(t % half_blocks)
        is_own = t // half_blocks == core
        dn = nt(d_gate[rows, 0:cols], wq[...]) + nt(d_gate[rows, cols : 2 * cols], wk[...]) + nt(d_up[rows, 0:cols], wv[...])
        x = xs[rows, :].astype(F32)
        r = lax.rsqrt(jnp.mean(x * x, axis=-1, keepdims=True) + EPS)
        gains[1:2, :] += jnp.sum(dn * (x * r), axis=0, keepdims=True)

        @pl.when(is_own)
        def _():
            dn_keep[local, :] = dn

        @pl.when(jnp.logical_not(is_own))
        def _():
            send_out(t % half_blocks).wait_send()
            out_send[local, :] = dn.astype(BF)
            send_dn1(t % half_blocks).start()

        return carry

    lax.fori_loop(0, blocks, finish, 0)
    turned = jnp.transpose(gains[...])
    turned_low = turned.astype(BF)
    rest = turned - turned_low.astype(F32)
    both = jnp.where(lane < LANES // 2, turned, pltpu.roll(rest, LANES // 2, 1)).astype(BF)
    spread("gains", 0, both)
    start("gains", 0)
    advance("value", 0)

    def input_part(t, carry):
        local = rows_of(t)
        send_dn1(t).wait_recv()
        dn = dn_keep[local, :] + dn_got[local, :].astype(F32)
        x = xs[rows_of(core * half_blocks + t), :].astype(F32)
        r = lax.rsqrt(jnp.mean(x * x, axis=-1, keepdims=True) + EPS)
        e = gain_one[...] * dn
        grad = d_res[local, :] + r * e - x * (r * r * r) * jnp.mean(e * x, axis=-1, keepdims=True)
        dn_got[local, :] = grad.astype(BF)
        write_grad(t).start()
        return carry

    lax.fori_loop(0, half_blocks, input_part, 0)
    advance("query", 0)
    advance("value", 1)
    advance("down", 3)
    advance("out", 3)
    early = chunks["query"][5]
    send_final(0, 0, early).start()
    advance("key", 0)
    advance("query", 1)
    advance("value", 2)
    advance("gains", 0)
    advance("key", 1)
    advance("query", 2)
    advance("gains", 1)
    advance("key", 2)
    advance("gains", 2)
    advance("value", 3)
    advance("query", 3)
    advance("key", 3)
    advance("gains", 3)
    rows_final = final.shape[1]
    send_final(1, early, rows_final - early).start()
    mine_out = load(0, final.at[core], final_out.at[0])
    mine_out.start()
    send_final(0, 0, early).wait_recv()
    early_out = load(1, final_got.at[pl.ds(0, early)], final_out.at[1, pl.ds(0, early)])
    early_out.start()
    for name in names:
        drain(name)
    send_x.wait_send()
    send_ids.wait_send()
    send_dy.wait_send()
    for t in range(blocks):
        send_att(t).wait_send()
        send_dn(t).wait_send()
    for t in range(half_blocks):
        write_out(t).wait()
        write_grad(t).wait()
        send_dn1(t).wait_send()
    send_final(0, 0, early).wait_send()
    send_final(1, early, rows_final - early).wait()
    late = pl.ds(early, rows_final - early)
    late_out = load(2, final_got.at[late], final_out.at[1, late])
    late_out.start()
    mine_out.wait()
    early_out.wait()
    late_out.wait()


def fused_shards(
    tokens, segment_ids, norm1_gain, w_query, w_key, w_value, w_out, norm2_gain, w_gate, w_up, w_down, out_grad,
):
    seqs, half_tokens, width = tokens.shape
    length = 2 * half_tokens
    cols = w_query.shape[1] // 2
    ff = w_gate.shape[1] // 2
    chunks, rows, rows_final = layout_of(width, cols, ff)
    core = lax.axis_index("seq")
    chip = lax.axis_index("dp")
    tables = tuple(jnp.asarray(t) for t in small_tables(length))
    any_space = pl.BlockSpec(memory_space=pl.ANY)
    vmem = pl.BlockSpec(memory_space=pltpu.VMEM)

    def low(*dims):
        return pltpu.VMEM(dims, BF)

    def full(*dims):
        return pltpu.VMEM(dims, F32)

    scratch = [
        low(length, width), low(length, width), pltpu.VMEM((1, length), jnp.int32),
        low(width, cols), low(width, cols), low(width, cols), low(width, width), low(width, ff), low(width, ff), low(ff, width),
        low(length, width), low(length, cols), low(length, cols), low(length, cols), low(length, cols), low(length, cols),
        full(length, LANES), full(TB, 3 * TB),
        full(length, width), low(length, width), low(length, ff), low(length, ff), low(length, ff), low(length, width),
        low(length, width), full(half_tokens, width), low(half_tokens, width), low(half_tokens, width), full(length, cols),
        full(half_tokens, width), low(half_tokens, width),
        full(LANES, width), low(8, rows, LANES), low(4, rows, LANES), low(2, rows, LANES), low(1, rows, LANES), low(rows, LANES),
        full(rows, LANES), full(2, rows_final, LANES), full(rows_final, LANES),
        pltpu.SemaphoreType.DMA((10,)), pltpu.SemaphoreType.DMA((17,)), pltpu.SemaphoreType.DMA((17,)),
        pltpu.SemaphoreType.DMA((4 * len(chunks),)), pltpu.SemaphoreType.DMA((4 * len(chunks),)),
    ]
    block_out, input_grad, final = pl.pallas_call(
        block_kernel,
        out_shape=(shape(half_tokens, width), shape(half_tokens, width), shape(2, rows_final, LANES, dtype=F32)),
        in_specs=[any_space] * 10 + [vmem] * 6,
        out_specs=[any_space] * 3,
        scratch_shapes=scratch,
        compiler_params=pltpu.CompilerParams(
            vmem_limit_bytes=67043328, collective_id=0, has_side_effects=True,
        ),
        name="block",
    )(
        tokens.reshape(half_tokens, width), segment_ids.reshape(1, half_tokens), out_grad.reshape(half_tokens, width),
        w_query, w_key, w_value, w_out, w_gate, w_up, w_down,
        norm1_gain.astype(F32).reshape(1, width), norm2_gain.astype(F32).reshape(1, width), *tables,
    )
    mine, got = final[0], final[1]
    holds = (chip >> 3) == core

    def part(name):
        _, _, kind, pieces, each, at = chunks[name]
        half = each // 2
        cut = slice(at, at + pieces * half)
        a, b = mine[cut].reshape(pieces, half, LANES), got[cut].reshape(pieces, half, LANES)
        if kind == "B":
            taken = jnp.where(holds, a, b)
        else:
            taken = jnp.where(core == 0, jnp.concatenate([a, b]), jnp.concatenate([b, a]))
        return jnp.transpose(taken, (0, 2, 1)).reshape(-1, half)

    gains = part("gains")
    gains = gains[:LANES] + gains[LANES:]
    summed = (
        gains[1] + gains[1 + LANES // 2],
        part("query"),
        part("key"),
        part("value"),
        part("out"),
        gains[0] + gains[LANES // 2],
        part("gate"),
        part("up"),
        part("down"),
    )
    return (block_out.reshape(seqs, half_tokens, width), input_grad.reshape(seqs, half_tokens, width), *summed)


def solution(mesh):
    placed = (P("dp", "seq", None), P("dp", "seq"), *([P()] * 9), P("dp", "seq", None))
    column = P(None, AX)
    chips = mesh.shape["dp"]
    body = fused_shards if chips == 16 else functools.partial(shards, chips=chips)
    return jax.shard_map(
        body,
        mesh=mesh,
        in_specs=placed,
        out_specs=(
            P("dp", "seq", None), P("dp", "seq", None), P(AX), column, column, column, column, P(AX), column, column, column,
        ),
        check_vma=False,
    )
```

```python
import functools

import jax
import jax.numpy as jnp
import numpy as np
from jax import lax
from jax.experimental import pallas as pl
from jax.experimental.pallas import tpu as pltpu
from jax.sharding import PartitionSpec as P

HD = 64
EPS = 1e-06
SCALE = 0.125
NEG = -1e30
BASE = 10000.0
AX = ("dp", "seq")
BF = jnp.bfloat16
F32 = jnp.float32
TB = 256
LANES = 128


def nn(a, b):
    return lax.dot_general(a, b, (((1,), (0,)), ((), ())), preferred_element_type=F32)


def nt(a, b):
    return lax.dot_general(a, b, (((1,), (1,)), ((), ())), preferred_element_type=F32)


def tn(a, b):
    return lax.dot_general(a, b, (((0,), (0,)), ((), ())), preferred_element_type=F32)


def small_tables(length):
    freqs = BASE ** (-np.arange(HD // 2, dtype=np.float64) * (2.0 / HD))
    lane_freqs = np.tile(freqs, 4)[None, :]
    fine = np.arange(64, dtype=np.float64)[:, None] * lane_freqs
    coarse = 64.0 * np.arange(length // 64, dtype=np.float64)[:, None] * lane_freqs
    return tuple(
        np.asarray(t, np.float32) for t in (np.cos(fine), np.sin(fine), np.cos(coarse), np.sin(coarse))
    )


def angle_block(tables, sub):
    cos_f, sin_f, cos_c, sin_c = tables
    ca = cos_c[pl.ds(sub, 1), :]
    sa = sin_c[pl.ds(sub, 1), :]
    cb = cos_f[...]
    sb = sin_f[...]
    low_half = (lax.broadcasted_iota(jnp.int32, (64, LANES), 1) % HD) < HD // 2
    cosine = ca * cb - sa * sb
    sine = sa * cb + ca * sb
    return cosine, jnp.where(low_half, -sine, sine), low_half


def rotate(v, cosine, sine, low_half):
    partner = jnp.where(low_half, pltpu.roll(v, LANES - HD // 2, 1), pltpu.roll(v, HD // 2, 1))
    return v * cosine + partner * sine


def window(block):
    return max(0, (block - 2) * TB)


def bias_of(seg_col, seg_row, block):
    first = window(block)
    keys = (block + 1) * TB - first
    rows = seg_col[pl.ds(block * TB, TB), :]
    cols = seg_row[:, pl.ds(first, keys)]
    q_at = block * TB + lax.broadcasted_iota(jnp.int32, (TB, keys), 0)
    k_at = first + lax.broadcasted_iota(jnp.int32, (TB, keys), 1)
    return jnp.where((rows == cols) & (k_at <= q_at), 0.0, NEG).astype(F32)


def forward_attention(
    core, own_ref, other_ref, gain_ref, wq_ref, wk_ref, wv_ref, cos_f, sin_f, cos_c, sin_c, seg_col, seg_row,
    normed_ref, q_ref, k_ref, v_ref, att_ref, lse_ref, bias_ref,
):
    s = core[0]
    half_tokens, width = own_ref.shape
    length = 2 * half_tokens
    cols = wq_ref.shape[1]
    tables = (cos_f, sin_f, cos_c, sin_c)

    def project(t, carry):
        rows = pl.ds(pl.multiple_of(t * TB, TB), TB)
        part = t // (half_tokens // TB)
        local = pl.ds(pl.multiple_of((t % (half_tokens // TB)) * TB, TB), TB)
        x = jnp.where(part == s, own_ref[local, :], other_ref[local, :]).astype(F32)
        r = lax.rsqrt(jnp.mean(x * x, axis=-1, keepdims=True) + EPS)
        normed = (x * r * gain_ref[...]).astype(BF)
        normed_ref[rows, :] = normed
        v_ref[rows, :] = nn(normed, wv_ref[...]).astype(BF)
        q = nn(normed, wq_ref[...]).astype(BF).astype(F32)
        k = nn(normed, wk_ref[...]).astype(BF).astype(F32)
        for sub in range(TB // 64):
            cosine, sine, low_half = angle_block(tables, t * (TB // 64) + sub)
            at = pl.ds(pl.multiple_of(t * TB + sub * 64, 64), 64)
            for tile in range(cols // LANES):
                lanes = slice(tile * LANES, (tile + 1) * LANES)
                part_rows = slice(sub * 64, (sub + 1) * 64)
                q_ref[at, lanes] = (rotate(q[part_rows, lanes], cosine, sine, low_half).astype(BF) * BF(SCALE)).astype(BF)
                k_ref[at, lanes] = rotate(k[part_rows, lanes], cosine, sine, low_half).astype(BF)
        return carry

    lax.fori_loop(0, length // TB, project, 0)

    for block in range(length // TB):
        first = window(block)
        keys = (block + 1) * TB - first
        bias_ref[:, :keys] = bias_of(seg_col, seg_row, block)
        rows = pl.ds(block * TB, TB)
        span = pl.ds(first, keys)

        def head(h, carry):
            lanes = pl.ds(pl.multiple_of((h // 2) * LANES, LANES), LANES)
            lane = lax.broadcasted_iota(jnp.int32, (1, LANES), 1)
            mine = (lane // HD) == (h % 2)
            q = q_ref[rows, lanes]
            qm = jnp.where(mine, q, jnp.zeros_like(q))
            scores = nt(qm, k_ref[span, lanes]) + bias_ref[:, :keys]
            peak = jnp.max(scores, axis=-1, keepdims=True)
            weights = jnp.exp(scores - peak)
            total = jnp.sum(weights, axis=-1, keepdims=True)
            probs = (weights * (1.0 / total)).astype(BF)
            result = nn(probs, v_ref[span, lanes]).astype(BF)
            att_ref[rows, lanes] = jnp.where(mine, result, att_ref[rows, lanes])
            lse_ref[rows, :] = jnp.where(lane == h, peak + jnp.log(total), lse_ref[rows, :])
            return carry

        lax.fori_loop(0, cols // HD, head, 0)


def feed_forward(
    core, slots_a, slots_b, own_ref, other_ref, att_own, att_other, gain_ref, wo_ref, wg_ref, wu_ref, wd_ref,
    dy_own, dy_other,
    res_ref, out_keep, out_send, dn_ref, pack_ref, normed, hidden, d_gate, d_up, dy_all,
):
    s = core[0]
    half_tokens, width = own_ref.shape
    length = 2 * half_tokens
    cols = att_own.shape[1]
    own_rows = pl.ds(pl.multiple_of(s * cols, cols), cols)
    other_rows = pl.ds(pl.multiple_of((1 - s) * cols, cols), cols)

    def block(t, carry):
        rows = pl.ds(pl.multiple_of(t * TB, TB), TB)
        part = t // (half_tokens // TB)
        local = pl.ds(pl.multiple_of((t % (half_tokens // TB)) * TB, TB), TB)
        is_own = part == s
        x = jnp.where(is_own, own_ref[local, :], other_ref[local, :]).astype(F32)
        dy = jnp.where(is_own, dy_own[local, :], dy_other[local, :])
        dy_all[rows, :] = dy
        residual = x + (nn(att_own[rows, :], wo_ref[own_rows, :]) + nn(att_other[rows, :], wo_ref[other_rows, :]))
        res_ref[rows, :] = residual
        r = lax.rsqrt(jnp.mean(residual * residual, axis=-1, keepdims=True) + EPS)
        n2 = (residual * r * gain_ref[...]).astype(BF)
        normed[rows, :] = n2
        gate = nn(n2, wg_ref[...])
        up = nn(n2, wu_ref[...])
        sig = 1.0 / (1.0 + jnp.exp(-gate))
        act = gate * sig
        hid = (act * up).astype(BF)
        hidden[rows, :] = hid
        down = nn(hid, wd_ref[...])

        @pl.when(is_own)
        def _():
            out_keep[local, :] = residual + down

        @pl.when(jnp.logical_not(is_own))
        def _():
            out_send[local, :] = down.astype(BF)

        d_hidden = nt(dy, wd_ref[...])
        dg = (d_hidden * up * (sig * (1.0 + gate * (1.0 - sig)))).astype(BF)
        du = (d_hidden * act).astype(BF)
        d_gate[rows, :] = dg
        d_up[rows, :] = du
        dn_ref[rows, :] = (nt(dg, wg_ref[...]) + nt(du, wu_ref[...])).astype(BF)
        return carry

    lax.fori_loop(0, length // TB, block, 0)

    wide = wg_ref.shape[1] // 8
    pieces = width // LANES

    def gate_up(o, carry):
        cut = pl.ds(pl.multiple_of(o * wide, wide), wide)
        slot = slots_b[o]
        for which, source in ((0, d_gate), (1, d_up)):
            grad = tn(source[:, cut], normed[...]).astype(BF)
            for piece in range(pieces):
                pack_ref[slot, pl.ds((which * pieces + piece) * wide, wide), :] = grad[:, piece * LANES : (piece + 1) * LANES]
        return carry

    lax.fori_loop(0, 8, gate_up, 0)
    low = width // 16
    base = 2 * pieces * wide
    deep = hidden.shape[1] // LANES
    for piece in range(deep):
        grad = tn(dy_all[...], hidden[:, piece * LANES : (piece + 1) * LANES]).astype(BF)
        for o in range(16):
            slot = slots_a[o]
            at = pl.multiple_of(base + (slot % 2) * (deep * low) + piece * low, 16)
            pack_ref[slot // 2, pl.ds(at, low), :] = grad[o * low : (o + 1) * low, :]


def backward_attention(
    core, slots_a, slots_b, own_ref, other_ref, gain_one, gain_two, wq_ref, wk_ref, wv_ref, wo_ref, dy_own, dy_other,
    res_ref, dn_own, dn_other, att_ref, normed_ref, q_ref, k_ref, v_ref, lse_ref, cos_f, sin_f, cos_c, sin_c, seg_col, seg_row,
    d_res, dn_keep, dn_send, pack_ref, d_branch, d_att, dq, dk, dv, dq_low, dk_low, dv_low, gains, bias_ref,
):
    s = core[0]
    half_tokens, width = own_ref.shape
    length = 2 * half_tokens
    cols = att_ref.shape[1]
    tables = (cos_f, sin_f, cos_c, sin_c)
    gains[...] = jnp.zeros_like(gains)

    def norm_two(t, carry):
        rows = pl.ds(pl.multiple_of(t * TB, TB), TB)
        part = t // (half_tokens // TB)
        local = pl.ds(pl.multiple_of((t % (half_tokens // TB)) * TB, TB), TB)
        is_own = part == s
        dy = jnp.where(is_own, dy_own[local, :], dy_other[local, :]).astype(F32)
        residual = res_ref[rows, :]
        dn = dn_own[rows, :].astype(F32) + dn_other[rows, :].astype(F32)
        r = lax.rsqrt(jnp.mean(residual * residual, axis=-1, keepdims=True) + EPS)
        scaled = residual * r
        e = gain_two[...] * dn
        gains[0:1, :] += jnp.sum(dn * scaled, axis=0, keepdims=True)
        grad = dy + r * (e - scaled * (r * jnp.mean(e * residual, axis=-1, keepdims=True)))
        low = grad.astype(BF)
        d_branch[rows, :] = low

        @pl.when(is_own)
        def _():
            d_res[local, :] = grad

        d_att[rows, :] = nt(low, wo_ref[...]).astype(BF)
        return carry

    lax.fori_loop(0, length // TB, norm_two, 0)

    dk[...] = jnp.zeros_like(dk)
    dv[...] = jnp.zeros_like(dv)
    for block in range(length // TB):
        first = window(block)
        keys = (block + 1) * TB - first
        bias_ref[:, :keys] = bias_of(seg_col, seg_row, block)
        rows = pl.ds(block * TB, TB)
        span = pl.ds(first, keys)

        def head(h, carry):
            lanes = pl.ds(pl.multiple_of((h // 2) * LANES, LANES), LANES)
            lane = lax.broadcasted_iota(jnp.int32, (1, LANES), 1)
            mine = (lane // HD) == (h % 2)
            q = q_ref[rows, lanes]
            qm = jnp.where(mine, q, jnp.zeros_like(q))
            do = d_att[rows, lanes]
            dom = jnp.where(mine, do, jnp.zeros_like(do))
            lse = jnp.sum(jnp.where(lane == h, lse_ref[rows, :], 0.0), axis=-1, keepdims=True)
            k = k_ref[span, lanes]
            probs = jnp.exp(nt(qm, k) + (bias_ref[:, :keys] - lse))
            d_probs = nt(dom, v_ref[span, lanes])
            delta = jnp.sum(probs * d_probs, axis=-1, keepdims=True)
            ds = (probs * (d_probs - delta)).astype(BF)
            part = nn(ds, k)
            dq[rows, lanes] = jnp.where(mine, part, dq[rows, lanes])
            dk[span, lanes] += tn(ds, qm)
            dv[span, lanes] += tn(probs.astype(BF), dom)
            return carry

        lax.fori_loop(0, cols // HD, head, 0)

    def finish(t, carry):
        rows = pl.ds(pl.multiple_of(t * TB, TB), TB)
        part = t // (half_tokens // TB)
        local = pl.ds(pl.multiple_of((t % (half_tokens // TB)) * TB, TB), TB)
        is_own = part == s
        for sub in range(TB // 64):
            cosine, sine, low_half = angle_block(tables, t * (TB // 64) + sub)
            at = pl.ds(pl.multiple_of(t * TB + sub * 64, 64), 64)
            for tile in range(cols // LANES):
                lanes = slice(tile * LANES, (tile + 1) * LANES)
                dq_low[at, lanes] = (rotate(dq[at, lanes], cosine, -sine, low_half) * SCALE).astype(BF)
                dk_low[at, lanes] = rotate(dk[at, lanes], cosine, -sine, low_half).astype(BF)
        dv_low[rows, :] = dv[rows, :].astype(BF)
        dn = nt(dq_low[rows, :], wq_ref[...]) + nt(dk_low[rows, :], wk_ref[...]) + nt(dv_low[rows, :], wv_ref[...])
        x = jnp.where(is_own, own_ref[local, :], other_ref[local, :]).astype(F32)
        r = lax.rsqrt(jnp.mean(x * x, axis=-1, keepdims=True) + EPS)
        gains[1:2, :] += jnp.sum(dn * (x * r), axis=0, keepdims=True)

        @pl.when(is_own)
        def _():
            dn_keep[local, :] = dn

        @pl.when(jnp.logical_not(is_own))
        def _():
            dn_send[local, :] = dn.astype(BF)

        return carry

    lax.fori_loop(0, length // TB, finish, 0)

    low = width // 16
    pieces = width // LANES
    for which, source in ((0, dq_low), (1, dk_low), (2, dv_low)):
        for piece in range(pieces):
            grad = tn(source[...], normed_ref[:, piece * LANES : (piece + 1) * LANES]).astype(BF)
            for o in range(8):
                at = (which * pieces + piece) * low
                pack_ref[slots_b[o], pl.ds(at, low), :] = grad[o * low : (o + 1) * low, :]
    turned = jnp.transpose(gains[...])
    turned_low = turned.astype(BF)
    rest = (turned - turned_low.astype(F32)).astype(BF)
    lane = lax.broadcasted_iota(jnp.int32, (1, LANES), 1)
    both = jnp.where(lane < LANES // 2, turned_low, pltpu.roll(rest.astype(F32), LANES // 2, 1).astype(BF))
    at_b = 3 * pieces * low
    size_a = (cols // LANES + 1) * low
    base = at_b + low
    for piece in range(cols // LANES):
        grad = tn(d_branch[...], att_ref[:, piece * LANES : (piece + 1) * LANES]).astype(BF)
        for o in range(16):
            slot = slots_a[o]
            at = pl.multiple_of(base + (slot % 2) * size_a + piece * low, 16)
            pack_ref[slot // 2, pl.ds(at, low), :] = grad[o * low : (o + 1) * low, :]
    for o in range(16):
        slot = slots_a[o]
        at = pl.multiple_of(base + (slot % 2) * size_a + (cols // LANES) * low, 16)
        pack_ref[slot // 2, pl.ds(at, low), :] = both[o * low : (o + 1) * low, :]

        @pl.when(s == o // 8)
        def _():
            pack_ref[slots_b[o % 8], pl.ds(at_b, low), :] = both[o * low : (o + 1) * low, :]


BIG = pltpu.CompilerParams(vmem_limit_bytes=60 * 1024 * 1024)


def shape(*dims, dtype=BF):
    return jax.ShapeDtypeStruct(dims, dtype)


def flat(dp, core):
    return 2 * dp + core


def swap_cores(chips):
    return [(flat(d, c), flat(d, 1 - c)) for d in range(chips) for c in range(2)]


ORDER = ((0, 1, 2, 3), (1, 0, 2, 3))


def swap_chips(step):
    return [(flat(d, c), flat(d ^ (1 << ORDER[c][step]), c)) for d in range(16) for c in range(2)]


def to_owner_half():
    return [(flat(d, c), flat(d ^ 8, c)) for d in range(16) for c in range(2) if d // 8 != c]


def slot_tables(chip, core, chips):
    if chips != 16:
        return jnp.arange(16, dtype=jnp.int32), jnp.arange(8, dtype=jnp.int32)
    owner = jnp.arange(16, dtype=jnp.int32)
    away = owner ^ chip
    x, y, z0, z1 = away & 1, (away >> 1) & 1, (away >> 2) & 1, (away >> 3) & 1
    first = jnp.where(core == 0, x, y)
    second = jnp.where(core == 0, y, x)
    slots_a = first * 8 + second * 4 + z0 * 2 + z1
    near = slots_a // 2
    return slots_a, jnp.where(core == 0, near[:8], near[8:])


def halve(pack):
    for step in range(3):
        half = pack.shape[0] // 2
        pack3 = pack.reshape(2, half, *pack.shape[1:])
        got = lax.ppermute(pack3[1], AX, swap_chips(step))
        total = pack3[0].astype(F32) + got.astype(F32)
        pack = total.astype(BF) if step < 2 else total
    return pack[0]


def last_step(total, size_b):
    kind_b = total[:size_b]
    kind_a = total[size_b:].reshape(2, -1, LANES)
    got_a = lax.ppermute(kind_a[1].astype(BF), AX, swap_chips(3))
    got_b = lax.ppermute(kind_b.astype(BF), AX, to_owner_half())
    return kind_a[0] + got_a.astype(F32), kind_b + got_b.astype(F32)


def shards(
    tokens, segment_ids, norm1_gain, w_query, w_key, w_value, w_out, norm2_gain, w_gate, w_up, w_down, out_grad,
    *, chips,
):
    seqs, half_tokens, width = tokens.shape
    length = 2 * half_tokens
    cols = w_query.shape[1] // 2
    ff = w_gate.shape[1] // 2
    core = lax.axis_index("seq")
    chip = lax.axis_index("dp")
    core_id = core.reshape(1).astype(jnp.int32)
    pairs = swap_cores(chips)
    own = tokens.reshape(half_tokens, width)
    dy_own = out_grad.reshape(half_tokens, width)
    ids = segment_ids.reshape(1, half_tokens)
    other = lax.ppermute(own, AX, pairs)
    ids_other = lax.ppermute(ids, AX, pairs)
    dy_other = lax.ppermute(dy_own, AX, pairs)
    seg_row = jnp.where(core == 0, jnp.concatenate([ids, ids_other], 1), jnp.concatenate([ids_other, ids], 1))
    seg_col = seg_row.reshape(length, 1)
    gain_one = norm1_gain.astype(F32).reshape(1, width)
    gain_two = norm2_gain.astype(F32).reshape(1, width)
    tables = tuple(jnp.asarray(t) for t in small_tables(length))
    slots_a, slots_b = slot_tables(chip, core, chips)
    half_w = pl.BlockSpec((width, cols), lambda g, c: (0, c[0]))
    half_wide = pl.BlockSpec((width, ff), lambda g, c, a, b: (0, c[0]))
    whole = lambda a: pl.BlockSpec(a.shape, lambda g, *_: (0,) * len(a.shape))

    def out_block(s):
        return pl.BlockSpec(s.shape, lambda g, *_: (0,) * len(s.shape))

    outs = (
        shape(length, width), shape(length, cols), shape(length, cols), shape(length, cols), shape(length, cols),
        shape(length, LANES, dtype=F32),
    )
    normed1, q, k, v, att, lse = pl.pallas_call(
        forward_attention,
        out_shape=outs,
        grid_spec=pltpu.PrefetchScalarGridSpec(
            num_scalar_prefetch=1,
            grid=(1,),
            in_specs=[whole(own), whole(other), whole(gain_one), half_w, half_w, half_w]
            + [whole(t) for t in tables]
            + [whole(seg_col), whole(seg_row)],
            out_specs=[out_block(o) for o in outs],
            scratch_shapes=[pltpu.VMEM((TB, 3 * TB), F32)],
        ),
        compiler_params=BIG,
        name="attention_forward",
    )(core_id, own, other, gain_one, w_query, w_key, w_value, *tables, seg_col, seg_row)
    att_other = lax.ppermute(att, AX, pairs)

    rows_one = 2 * (width // LANES) * (ff // 8) + 2 * (ff // LANES) * (width // 16)
    outs = (
        shape(length, width, dtype=F32), shape(half_tokens, width, dtype=F32), shape(half_tokens, width),
        shape(length, width), shape(8, rows_one, LANES),
    )
    residual, out_keep, out_send, dn, pack_one = pl.pallas_call(
        feed_forward,
        out_shape=outs,
        grid_spec=pltpu.PrefetchScalarGridSpec(
            num_scalar_prefetch=3,
            grid=(1,),
            in_specs=[whole(own), whole(other), whole(att), whole(att), whole(gain_two), whole(w_out), half_wide, half_wide,
                      pl.BlockSpec((ff, width), lambda g, c, a, b: (c[0], 0)), whole(own), whole(own)],
            out_specs=[out_block(o) for o in outs],
            scratch_shapes=[
                pltpu.VMEM((length, width), BF), pltpu.VMEM((length, ff), BF), pltpu.VMEM((length, ff), BF),
                pltpu.VMEM((length, ff), BF), pltpu.VMEM((length, width), BF),
            ],
        ),
        compiler_params=BIG,
        name="feed_forward",
    )(core_id, slots_a, slots_b, own, other, att, att_other, gain_two, w_out, w_gate, w_up, w_down, dy_own, dy_other)
    out_other = lax.ppermute(out_send, AX, pairs)
    block_out = (out_keep + out_other.astype(F32)).astype(BF)
    dn_other = lax.ppermute(dn, AX, pairs)

    low = width // 16
    size_b2 = 3 * (width // LANES) * low + low
    size_a2 = (cols // LANES + 1) * low
    outs = (
        shape(half_tokens, width, dtype=F32), shape(half_tokens, width, dtype=F32), shape(half_tokens, width),
        shape(8, size_b2 + 2 * size_a2, LANES),
    )
    half_w3 = pl.BlockSpec((width, cols), lambda g, c, a, b: (0, c[0]))
    inputs = (own, other, gain_one, gain_two, w_query, w_key, w_value, w_out, dy_own, dy_other, residual, dn, dn_other,
              att, normed1, q, k, v, lse, *tables, seg_col, seg_row)
    specs = [whole(a) for a in inputs]
    specs[4] = specs[5] = specs[6] = half_w3
    specs[7] = pl.BlockSpec((cols, width), lambda g, c, a, b: (c[0], 0))
    d_res, dn_keep, dn_send, pack_two = pl.pallas_call(
        backward_attention,
        out_shape=outs,
        grid_spec=pltpu.PrefetchScalarGridSpec(
            num_scalar_prefetch=3,
            grid=(1,),
            in_specs=specs,
            out_specs=[out_block(o) for o in outs],
            scratch_shapes=[
                pltpu.VMEM((length, width), BF), pltpu.VMEM((length, cols), BF),
                pltpu.VMEM((length, cols), F32), pltpu.VMEM((length, cols), F32), pltpu.VMEM((length, cols), F32),
                pltpu.VMEM((length, cols), BF), pltpu.VMEM((length, cols), BF), pltpu.VMEM((length, cols), BF),
                pltpu.VMEM((LANES, width), F32), pltpu.VMEM((TB, 3 * TB), F32),
            ],
        ),
        compiler_params=BIG,
        name="attention_backward",
    )(core_id, slots_a, slots_b, *inputs)
    dn1 = dn_keep + lax.ppermute(dn_send, AX, pairs).astype(F32)
    x = own.astype(F32)
    r = lax.rsqrt(jnp.mean(x * x, axis=-1, keepdims=True) + EPS)
    e = gain_one * dn1
    input_grad = (d_res + r * e - x * (r * r * r) * jnp.mean(e * x, axis=-1, keepdims=True)).astype(BF)

    pieces = width // LANES
    wide = ff // 8
    size_b1 = 2 * pieces * wide
    size_a1 = (ff // LANES) * low

    if chips == 16:
        one_a, one_b = last_step(halve(pack_one), size_b1)
        two_a, two_b = last_step(halve(pack_two), size_b2)
        holds = (chip >> 3) == core

        def share(a):
            parts = a.reshape(a.shape[0], 2, a.shape[1] // 2, LANES)
            mine = jnp.where(core == 0, parts[:, 0], parts[:, 1])
            theirs = jnp.where(core == 0, parts[:, 1], parts[:, 0])
            return mine, lax.ppermute(theirs, AX, pairs)

        def both(a):
            mine, got = share(a)
            return jnp.where(core == 0, mine, got), jnp.where(core == 0, got, mine)

        def one(a):
            mine, got = share(a)
            return jnp.where(holds, mine, got)

        down_lo, down_hi = both(one_a.reshape(ff // LANES, low, LANES))
        kind_a = two_a.reshape(cols // LANES + 1, low, LANES)
        out_lo, out_hi = both(kind_a)
        gates = one(one_b.reshape(2 * pieces, wide, LANES))
        rest = one(two_b.reshape(3 * pieces + 1, low, LANES))

        def turn(a):
            return jnp.transpose(a, (0, 2, 1)).reshape(-1, a.shape[1])

        tiles = cols // LANES
        gain1 = out_lo[tiles] + out_hi[tiles]
        gain1 = gain1[:, 1] + gain1[:, 1 + LANES // 2]
        gain2 = rest[3 * pieces]
        gain2 = gain2[:, 0] + gain2[:, LANES // 2]
        summed = (
            gain1,
            turn(rest[:pieces]),
            turn(rest[pieces : 2 * pieces]),
            turn(rest[2 * pieces : 3 * pieces]),
            turn(jnp.concatenate([out_lo[:tiles], out_hi[:tiles]])),
            gain2,
            turn(gates[:pieces]),
            turn(gates[pieces:]),
            turn(jnp.concatenate([down_lo, down_hi])),
        )
    else:
        def plain_b(rows, count, size, at):
            part = rows[:, at : at + count * size].reshape(8, count, size, LANES)
            part = jnp.transpose(part, (1, 3, 0, 2)).reshape(count * LANES, 8 * size).astype(F32)
            zero = jnp.zeros_like(part)
            return jnp.where(core == 0, jnp.concatenate([part, zero], 1), jnp.concatenate([zero, part], 1))

        def plain_a(rows, count, at, each):
            part = rows[:, at:].reshape(8, 2, each, low, LANES)[:, :, :count].reshape(16, count, low, LANES)
            part = jnp.transpose(part, (1, 3, 0, 2)).reshape(count * LANES, 16 * low).astype(F32)
            zero = jnp.zeros_like(part)
            return jnp.where(core == 0, jnp.concatenate([part, zero], 0), jnp.concatenate([zero, part], 0))

        def scatter(a):
            return lax.psum_scatter(a, AX, scatter_dimension=1, tiled=True)

        tiles = cols // LANES
        gain_a = pack_two[:, size_b2:].reshape(16, tiles + 1, low, LANES)[:, tiles].astype(F32)
        gain_a = gain_a[:, :, : LANES // 2] + gain_a[:, :, LANES // 2 :]
        gain_a = gain_a.reshape(width, LANES // 2)
        gain1 = gain_a[:, 1].reshape(1, width)
        gain2 = jnp.where(core == 0, gain_a[:, 0], 0.0).reshape(1, width)
        n = pieces * low
        summed = (
            scatter(gain1).reshape(-1),
            scatter(plain_b(pack_two, pieces, low, 0)),
            scatter(plain_b(pack_two, pieces, low, n)),
            scatter(plain_b(pack_two, pieces, low, 2 * n)),
            scatter(plain_a(pack_two, tiles, size_b2, tiles + 1)),
            scatter(gain2).reshape(-1),
            scatter(plain_b(pack_one, pieces, wide, 0)),
            scatter(plain_b(pack_one, pieces, wide, pieces * wide)),
            scatter(plain_a(pack_one, ff // LANES, size_b1, ff // LANES)),
        )
    return (block_out.reshape(seqs, half_tokens, width), input_grad.reshape(seqs, half_tokens, width), *summed)


MESH = pl.DeviceIdType.MESH


PLAN = {
    "u0": (("down", 0),),
    "a21": (("down", 1), ("gate", 0),),
    "a30": (("out", 0),),
    "a32": (("up", 0),),
    "lower": (("gate", 1),),
    "value": (("out", 1),),
    "query": (("down", 2),),
    "f1": (("up", 1),),
    "f3": (("gate", 2), ("query", 0),),
    "inp": (("down", 3),),
    "end": (("up", 2), ("value", 0), ("key", 0), ("out", 2), ("gate", 3), ("gains", 0), ("query", 1), ("value", 1), ("key", 1), ("gains", 1), ("up", 3), ("query", 2), ("out", 3), ("value", 2), ("key", 2), ("gains", 2), ("query", 3), ("value", 3), ("key", 3), ("gains", 3),),
}
Z_FIRST = ("up", "value")


def bit(value, place):
    return (value // (1 << place)) % 2


def other_bit(a, b):
    return a + b - 2 * a * b


def layout_of(width, cols, ff):
    low, wide = width // 16, ff // 8
    table, row, final = {}, 0, 0
    for name, kind, pieces, each in (
        ("gate", "B", width // LANES, wide), ("up", "B", width // LANES, wide), ("down", "A", ff // LANES, low),
        ("out", "A", cols // LANES, low), ("query", "B", width // LANES, low), ("key", "B", width // LANES, low),
        ("value", "B", width // LANES, low), ("gains", "A", 1, low),
    ):
        rows = pieces * each * (2 if kind == "A" else 1)
        table[name] = (row, rows, kind, pieces, each, final)
        row, final = row + rows, final + pieces * each // 2
    return table, row, final


def block_kernel(
    x_hbm, ids_hbm, dy_hbm, wq_hbm, wk_hbm, wv_hbm, wo_hbm, wg_hbm, wu_hbm, wd_hbm, gain_one, gain_two,
    cos_f, sin_f, cos_c, sin_c,
    block_out, input_grad, final_out,
    xs, dys, ids, wq, wk, wv, wo, wg, wu, wd, normed1, q_ref, k_ref, v_ref, att, att_other, lse_ref, bias_ref,
    res_ref, normed2, hidden, d_gate, d_up, dn_own, dn_other, out_keep, out_send, out_got, dv_ref, dn_keep, dn_got,
    gains, pack, got1, got2, got3, got4, acc, final, final_got,
    load_sem, pair_send, pair_recv, hop_send, hop_recv,
):
    core = lax.axis_index("seq")
    chip = lax.axis_index("dp")
    half_tokens, width = x_hbm.shape
    length = 2 * half_tokens
    cols = wq.shape[1]
    ff = wg.shape[1]
    blocks = length // TB
    half_blocks = half_tokens // TB
    tables = (cos_f, sin_f, cos_c, sin_c)
    chunks, _, _ = layout_of(width, cols, ff)
    names = list(chunks)
    low = width // 16

    bx, by, bz, bw = (bit(chip, i) for i in range(4))
    step_x, step_y = 1 - 2 * bx, 2 * (1 - 2 * by)
    near = chip + (1 - core) * step_x + core * step_y
    aside = chip + core * step_x + (1 - core) * step_y
    above = chip + 4 * (1 - 2 * bz)
    across = chip + 8 * (1 - 2 * bw)
    partners = (near, aside, above, across)
    holds = bw == core

    def path_of(name):
        return (above, near, aside, across) if name in Z_FIRST else partners

    def slot_of(name, owner):
        kx, ky, kz = other_bit(bx, owner & 1), other_bit(by, (owner >> 1) & 1), other_bit(bz, (owner >> 2) & 1)
        first = (1 - core) * kx + core * ky
        second = core * kx + (1 - core) * ky
        slot = kz * 4 + first * 2 + second if name in Z_FIRST else first * 4 + second * 2 + kz
        return slot, other_bit(bw, (owner >> 3) & 1)

    def owner_of(name, first, second, third):
        if name in Z_FIRST:
            first, second, third = second, third, first
        kx = (1 - core) * first + core * second
        ky = core * first + (1 - core) * second
        return other_bit(bx, kx) + 2 * other_bit(by, ky) + 4 * other_bit(bz, third)

    barrier = pltpu.get_barrier_semaphore()
    everyone = [{"dp": chip, "seq": 1 - core}] + [{"dp": p, "seq": core} for p in partners]
    for device in everyone:
        pl.semaphore_signal(barrier, inc=1, device_id=device, device_id_type=MESH)

    own_rows = pl.ds(pl.multiple_of(core * half_tokens, half_tokens), half_tokens)
    own_cols = pl.ds(pl.multiple_of(core * cols, cols), cols)
    own_ff = pl.ds(pl.multiple_of(core * ff, ff), ff)

    def load(i, src, dst):
        return pltpu.make_async_copy(src, dst, load_sem.at[i])

    loads = [
        load(0, x_hbm, xs.at[own_rows]),
        load(1, wv_hbm.at[:, own_cols], wv),
        load(2, wq_hbm.at[:, own_cols], wq),
        load(3, wk_hbm.at[:, own_cols], wk),
        load(4, ids_hbm, ids.at[:, own_rows]),
        load(5, wo_hbm, wo),
        load(6, wg_hbm.at[:, own_ff], wg),
        load(7, wu_hbm.at[:, own_ff], wu),
        load(8, wd_hbm.at[own_ff, :], wd),
        load(9, dy_hbm, dys.at[own_rows]),
    ]
    for copy in loads:
        copy.start()

    def to_pair(i, src, dst):
        return pltpu.make_async_remote_copy(
            src_ref=src, dst_ref=dst, send_sem=pair_send.at[i], recv_sem=pair_recv.at[i],
            device_id={"dp": chip, "seq": 1 - core}, device_id_type=MESH,
        )

    send_x = to_pair(0, x_hbm, xs.at[own_rows])
    send_ids = to_pair(1, ids_hbm, ids.at[:, own_rows])
    send_dy = to_pair(2, dy_hbm, dys.at[own_rows])

    def rows_of(t):
        return pl.ds(pl.multiple_of(t * TB, TB), TB)

    def send_att(t):
        return to_pair(3 + t, att.at[rows_of(t)], att_other.at[rows_of(t)])

    def send_dn(t):
        return to_pair(7 + t, dn_own.at[rows_of(t)], dn_other.at[rows_of(t)])

    def send_out(t):
        return to_pair(11 + t, out_send.at[rows_of(t)], out_got.at[rows_of(t)])

    def send_dn1(t):
        return to_pair(13 + t, out_send.at[rows_of(t)], dn_got.at[rows_of(t)])

    def write_out(t):
        return pltpu.make_async_copy(out_got.at[rows_of(t)], block_out.at[rows_of(t)], load_sem.at[3 + t])

    def write_grad(t):
        return pltpu.make_async_copy(dn_got.at[rows_of(t)], input_grad.at[rows_of(t)], load_sem.at[5 + t])

    def send_final(i, first, count):
        rows = pl.ds(first, count)
        return to_pair(15 + i, final.at[1 - core, rows], final_got.at[rows])


    def hop(name, step):
        row, count, kind = chunks[name][:3]
        at = 4 * names.index(name) + step
        rows = pl.ds(row, count)
        if step < 3:
            n = 4 >> step
            src, dst = pack.at[pl.ds(n, n), rows], (got1, got2, got3)[step].at[:, rows]
        elif kind == "B":
            src, dst = pack.at[0, rows], got4.at[rows]
        else:
            src, dst = pack.at[0, pl.ds(row + count // 2, count // 2)], got4.at[pl.ds(row, count // 2)]
        return pltpu.make_async_remote_copy(
            src_ref=src, dst_ref=dst, send_sem=hop_send.at[at], recv_sem=hop_recv.at[at],
            device_id={"dp": path_of(name)[step], "seq": core}, device_id_type=MESH,
        )

    def start(name, step):
        if step == 3 and chunks[name][2] == "B":
            @pl.when(jnp.logical_not(holds))
            def _():
                hop(name, step).start()
        else:
            hop(name, step).start()

    def advance(name, step):
        row, count, kind, pieces, each, at = chunks[name]
        if step < 3:
            hop(name, step).wait_recv()
            n = 4 >> step
            size = 384 if count % 384 == 0 else (288 if count % 288 == 0 else count)
            source = (got1, got2, got3)[step]
            per = count // size

            def add(i, carry):
                slab = i // per
                rows = pl.ds(pl.multiple_of(row + (i % per) * size, 16), size)
                total = pack[slab, rows, :].astype(F32) + source[slab, rows, :].astype(F32)
                pack[slab, rows, :] = total.astype(BF)
                if step == 2:
                    acc[rows, :] = total
                return carry

            lax.fori_loop(0, n * per, add, 0)
            start(name, step + 1)
            return
        half = each // 2
        if kind == "B":
            @pl.when(holds)
            def _():
                hop(name, step).wait_recv()
                for p in range(pieces):
                    for c in range(2):
                        rows = pl.ds(row + p * each + c * half, half)
                        final[c, pl.ds(at + p * half, half), :] = acc[rows, :] + got4[rows, :].astype(F32)

            @pl.when(jnp.logical_not(holds))
            def _():
                hop(name, step).wait_send()
                for p in range(pieces):
                    for c in range(2):
                        final[c, pl.ds(at + p * half, half), :] = acc[pl.ds(row + p * each + c * half, half), :]
        else:
            hop(name, step).wait_recv()
            for p in range(pieces):
                for c in range(2):
                    rows = pl.ds(row + p * each + c * half, half)
                    final[c, pl.ds(at + p * half, half), :] = acc[rows, :] + got4[rows, :].astype(F32)

    def proceed(point, here=None):
        steps = PLAN.get(point, ())
        if not steps:
            return
        if here is None:
            for name, step in steps:
                advance(name, step)
            return

        @pl.when(here)
        def _():
            for name, step in steps:
                advance(name, step)

    def drain(name):
        for step in range(3):
            hop(name, step).wait_send()
        if chunks[name][2] == "A":
            hop(name, 3).wait_send()


    pl.semaphore_wait(barrier, len(everyone))
    send_x.start()
    send_ids.start()
    send_dy.start()
    for copy in loads[:4]:
        copy.wait()

    def project(j, carry):
        t = (core * half_blocks + j) % blocks

        @pl.when(j == half_blocks)
        def _():
            send_x.wait_recv()

        rows = rows_of(t)
        x = xs[rows, :].astype(F32)
        r = lax.rsqrt(jnp.mean(x * x, axis=-1, keepdims=True) + EPS)
        normed = (x * r * gain_one[...]).astype(BF)
        normed1[rows, :] = normed
        v_ref[rows, :] = nn(normed, wv[...]).astype(BF)
        q = nn(normed, wq[...]).astype(BF).astype(F32)
        k = nn(normed, wk[...]).astype(BF).astype(F32)
        for sub in range(TB // 64):
            cosine, sine, low_half = angle_block(tables, t * (TB // 64) + sub)
            at = pl.ds(pl.multiple_of(t * TB + sub * 64, 64), 64)
            for tile in range(cols // LANES):
                lanes = slice(tile * LANES, (tile + 1) * LANES)
                part = slice(sub * 64, (sub + 1) * 64)
                q_ref[at, lanes] = (rotate(q[part, lanes], cosine, sine, low_half).astype(BF) * BF(SCALE)).astype(BF)
                k_ref[at, lanes] = rotate(k[part, lanes], cosine, sine, low_half).astype(BF)
        return carry

    lax.fori_loop(0, blocks, project, 0)
    loads[4].wait()
    send_ids.wait_recv()
    lse_ref[...] = jnp.transpose(jnp.broadcast_to(ids[...].astype(F32), (LANES, length)))

    def set_bias(block):
        first = window(block)
        keys = (block + 1) * TB - first
        rows = lse_ref[pl.ds(block * TB, TB), LANES - 1 :]
        columns = ids[:, pl.ds(first, keys)].astype(F32)
        q_at = block * TB + lax.broadcasted_iota(jnp.int32, (TB, keys), 0)
        k_at = first + lax.broadcasted_iota(jnp.int32, (TB, keys), 1)
        bias_ref[:, :keys] = jnp.where((rows == columns) & (k_at <= q_at), 0.0, NEG).astype(F32)

    lane = lax.broadcasted_iota(jnp.int32, (1, LANES), 1)
    first_head = lane < HD
    for block in range(blocks):
        first = window(block)
        keys = (block + 1) * TB - first
        set_bias(block)
        rows = pl.ds(block * TB, TB)
        span = pl.ds(first, keys)

        def pair(j, carry, rows=rows, span=span, keys=keys):
            lanes = pl.ds(pl.multiple_of(j * LANES, LANES), LANES)
            q, k, v = q_ref[rows, lanes], k_ref[span, lanes], v_ref[span, lanes]
            results, sums = [], []
            for mine in (first_head, jnp.logical_not(first_head)):
                scores = nt(jnp.where(mine, q, jnp.zeros_like(q)), k) + bias_ref[:, :keys]
                peak = jnp.max(scores, axis=-1, keepdims=True)
                weights = jnp.exp(scores - peak)
                total = jnp.sum(weights, axis=-1, keepdims=True)
                results.append(nn(weights.astype(BF), v) * (1.0 / total))
                sums.append(peak + jnp.log(total))
            att[rows, lanes] = jnp.where(first_head, *results).astype(BF)
            old = jnp.where(lane == 2 * j + 1, sums[1], lse_ref[rows, :])
            lse_ref[rows, :] = jnp.where(lane == 2 * j, sums[0], old)
            return carry

        lax.fori_loop(0, cols // LANES, pair, 0)
        send_att(block).start()


    for copy in loads[5:]:
        copy.wait()
    send_dy.wait_recv()
    other_cols = pl.ds(pl.multiple_of((1 - core) * cols, cols), cols)

    def feed(t, carry):
        rows = rows_of(t)
        local = rows_of(t % half_blocks)
        send_att(t).wait_recv()
        x = xs[rows, :].astype(F32)
        residual = x + (nn(att[rows, :], wo[own_cols, :]) + nn(att_other[rows, :], wo[other_cols, :]))
        res_ref[rows, :] = residual
        r = lax.rsqrt(jnp.mean(residual * residual, axis=-1, keepdims=True) + EPS)
        n2 = (residual * r * gain_two[...]).astype(BF)
        normed2[rows, :] = n2
        gate = nn(n2, wg[...])
        up = nn(n2, wu[...])
        hidden[rows, :] = (gate * (1.0 / (1.0 + jnp.exp(-gate))) * up).astype(BF)
        d_gate[rows, :] = gate.astype(BF)
        d_up[rows, :] = up.astype(BF)
        return carry

    lax.fori_loop(0, blocks, feed, 0)

    def spread(name, piece, grad):
        row, rows = chunks[name][:2]
        for o in range(16):
            slot, far = slot_of(name, o)
            at = pl.multiple_of(row + far * (rows // 2) + piece * low, 16)
            pack[slot, pl.ds(at, low), :] = grad[o * low : (o + 1) * low, :]

    def down_part(part, carry):
        at = part * (ff // 2)
        grad = tn(dys[...], hidden[:, pl.ds(pl.multiple_of(at, LANES), ff // 2)]).astype(BF)
        for piece in range(ff // 2 // LANES):
            spread("down", part * (ff // 2 // LANES) + piece, grad[:, piece * LANES : (piece + 1) * LANES])
        return carry

    lax.fori_loop(0, 2, down_part, 0)
    start("down", 0)

    def feed_back(t, carry):
        rows = rows_of(t)
        local = rows_of(t % half_blocks)
        is_own = t // half_blocks == core
        gate = d_gate[rows, :].astype(F32)
        up = d_up[rows, :].astype(F32)
        sig = 1.0 / (1.0 + jnp.exp(-gate))
        d_hidden = nt(dys[rows, :], wd[...])
        dg = (d_hidden * up * (sig * (1.0 + gate * (1.0 - sig)))).astype(BF)
        du = (d_hidden * (gate * sig)).astype(BF)
        d_gate[rows, :] = dg
        d_up[rows, :] = du
        dn_own[rows, :] = (nt(dg, wg[...]) + nt(du, wu[...])).astype(BF)
        send_dn(t).start()
        down = nn(hidden[rows, :], wd[...])

        @pl.when(is_own)
        def _():
            out_keep[local, :] = res_ref[rows, :] + down

        @pl.when(jnp.logical_not(is_own))
        def _():
            out_send[local, :] = down.astype(BF)
            send_out(t % half_blocks).start()

        for n in range(blocks):
            proceed(f"fb{n}", t == n)
        return carry

    lax.fori_loop(0, blocks, feed_back, 0)

    wide = ff // 8
    pieces = width // LANES

    def gate_up(name, source, first):
        row = chunks[name][0]

        cuts = []
        for j in range(4):
            owner = owner_of(name, first, j // 2, j % 2)
            cuts.append(source[:, pl.ds(pl.multiple_of(owner * wide, wide), wide)])
        grad = tn(jnp.concatenate(cuts, axis=1), normed2[...]).astype(BF)
        for j in range(4):
            for piece in range(pieces):
                part = grad[j * wide : (j + 1) * wide, piece * LANES : (piece + 1) * LANES]
                pack[4 * first + j, pl.ds(row + piece * wide, wide), :] = part

    gate_up("gate", d_gate, 1)
    start("gate", 0)
    proceed("g1")
    gate_up("gate", d_gate, 0)
    proceed("g0")
    gate_up("up", d_up, 1)
    start("up", 0)
    proceed("u1")
    gate_up("up", d_up, 0)
    proceed("u0")


    d_branch, d_att = normed2, hidden
    gains[...] = jnp.zeros_like(gains)

    def norm_two(t, carry):
        rows = rows_of(t)
        local = rows_of(t % half_blocks)
        is_own = t // half_blocks == core
        send_dn(t).wait_recv()
        dy = dys[rows, :].astype(F32)
        residual = res_ref[rows, :]
        dn = dn_own[rows, :].astype(F32) + dn_other[rows, :].astype(F32)
        r = lax.rsqrt(jnp.mean(residual * residual, axis=-1, keepdims=True) + EPS)
        scaled = residual * r
        e = gain_two[...] * dn
        grad = dy + r * (e - scaled * (r * jnp.mean(e * residual, axis=-1, keepdims=True)))
        small = grad.astype(BF)
        d_branch[rows, :] = small
        d_att[rows, 0:cols] = nt(small, wo[own_cols, :]).astype(BF)

        @pl.when(is_own)
        def _():
            gains[0:1, :] += jnp.sum(dn * scaled, axis=0, keepdims=True)
            send_out(t % half_blocks).wait_recv()
            out_got[local, :] = (out_keep[local, :] + out_got[local, :].astype(F32)).astype(BF)
            write_out(t % half_blocks).start()
            out_keep[local, :] = grad

        for n in range(blocks):
            proceed(f"n{n}", t == n)
        return carry

    lax.fori_loop(0, blocks, norm_two, 0)
    d_res = out_keep

    out_grad = tn(d_branch[...], att[...]).astype(BF)
    for piece in range(cols // LANES):
        spread("out", piece, out_grad[:, piece * LANES : (piece + 1) * LANES])
    start("out", 0)
    proceed("out")

    res_ref[:, cols:] = jnp.zeros((length, cols), F32)
    dv_ref[...] = jnp.zeros_like(dv_ref)

    def attention_back(block):
        first = window(block)
        keys = (block + 1) * TB - first
        rows = pl.ds(block * TB, TB)
        span = pl.ds(first, keys)

        def pair(j, carry):
            at = pl.multiple_of(j * LANES, LANES)
            lanes = pl.ds(at, LANES)
            k_lanes = pl.ds(pl.multiple_of(cols + at, LANES), LANES)
            q, do, k, v = q_ref[rows, lanes], d_att[rows, lanes], k_ref[span, lanes], v_ref[span, lanes]
            products = do.astype(F32) * att[rows, lanes].astype(F32)
            q_parts, do_parts, probs_parts, ds_parts, dq_parts = [], [], [], [], []
            for h, mine in enumerate((first_head, jnp.logical_not(first_head))):
                q_parts.append(jnp.where(mine, q, jnp.zeros_like(q)))
                do_parts.append(jnp.where(mine, do, jnp.zeros_like(do)))
                lse = jnp.sum(jnp.where(lane == 2 * j + h, lse_ref[rows, :], 0.0), axis=-1, keepdims=True)
                delta = jnp.sum(jnp.where(mine, products, 0.0), axis=-1, keepdims=True)
                probs = jnp.exp(nt(q_parts[h], k) + (bias_ref[:, :keys] - lse))
                ds = (probs * (nt(do_parts[h], v) - delta)).astype(BF)
                probs_parts.append(probs.astype(BF))
                ds_parts.append(ds)
                dq_parts.append(nn(ds, k))
            res_ref[rows, lanes] = jnp.where(first_head, *dq_parts)
            res_ref[span, k_lanes] += tn(jnp.concatenate(ds_parts), jnp.concatenate(q_parts))
            dv_ref[span, lanes] += tn(jnp.concatenate(probs_parts), jnp.concatenate(do_parts))
            for n in range(cols // LANES):
                proceed(f"a{block}{n}", j == n)
            return carry

        lax.fori_loop(0, cols // LANES, pair, 0)

    for block in range(blocks):
        set_bias(block)
        attention_back(block)

    def lower(t, carry):
        rows = rows_of(t)
        for sub in range(TB // 64):
            cosine, sine, low_half = angle_block(tables, t * (TB // 64) + sub)
            at = pl.ds(pl.multiple_of(t * TB + sub * 64, 64), 64)
            for tile in range(cols // LANES):
                lanes = slice(tile * LANES, (tile + 1) * LANES)
                k_lanes = slice(cols + tile * LANES, cols + (tile + 1) * LANES)
                d_gate[at, lanes] = (rotate(res_ref[at, lanes], cosine, -sine, low_half) * SCALE).astype(BF)
                d_gate[at, k_lanes] = rotate(res_ref[at, k_lanes], cosine, -sine, low_half).astype(BF)
        d_up[rows, 0:cols] = dv_ref[rows, :].astype(BF)
        return carry

    lax.fori_loop(0, blocks, lower, 0)
    proceed("lower")

    def qkv(name, source, lanes_at):
        row = chunks[name][0]

        grad = tn(source[:, lanes_at : lanes_at + cols], normed1[...]).astype(BF)
        for o in range(8):
            slot = slot_of(name, o)[0]
            for piece in range(pieces):
                part = grad[o * low : (o + 1) * low, piece * LANES : (piece + 1) * LANES]
                pack[slot, pl.ds(row + piece * low, low), :] = part
        start(name, 0)
        proceed(name)

    qkv("value", d_up, 0)
    qkv("query", d_gate, 0)
    qkv("key", d_gate, cols)

    def finish(j, carry):
        t = ((1 - core) * half_blocks + j) % blocks
        rows = rows_of(t)
        local = rows_of(t % half_blocks)
        is_own = t // half_blocks == core
        dn = nt(d_gate[rows, 0:cols], wq[...]) + nt(d_gate[rows, cols : 2 * cols], wk[...]) + nt(d_up[rows, 0:cols], wv[...])
        x = xs[rows, :].astype(F32)
        r = lax.rsqrt(jnp.mean(x * x, axis=-1, keepdims=True) + EPS)
        gains[1:2, :] += jnp.sum(dn * (x * r), axis=0, keepdims=True)

        @pl.when(is_own)
        def _():
            dn_keep[local, :] = dn

        @pl.when(jnp.logical_not(is_own))
        def _():
            send_out(t % half_blocks).wait_send()
            out_send[local, :] = dn.astype(BF)
            send_dn1(t % half_blocks).start()

        for n in range(blocks):
            proceed(f"f{n}", j == n)
        return carry

    lax.fori_loop(0, blocks, finish, 0)
    turned = jnp.transpose(gains[...])
    turned_low = turned.astype(BF)
    rest = turned - turned_low.astype(F32)
    both = jnp.where(lane < LANES // 2, turned, pltpu.roll(rest, LANES // 2, 1)).astype(BF)
    spread("gains", 0, both)
    start("gains", 0)
    proceed("gains")

    def input_part(t, carry):
        local = rows_of(t)
        send_dn1(t).wait_recv()
        dn = dn_keep[local, :] + dn_got[local, :].astype(F32)
        x = xs[rows_of(core * half_blocks + t), :].astype(F32)
        r = lax.rsqrt(jnp.mean(x * x, axis=-1, keepdims=True) + EPS)
        e = gain_one[...] * dn
        grad = d_res[local, :] + r * e - x * (r * r * r) * jnp.mean(e * x, axis=-1, keepdims=True)
        dn_got[local, :] = grad.astype(BF)
        write_grad(t).start()
        return carry

    lax.fori_loop(0, half_blocks, input_part, 0)
    proceed("inp")
    early = chunks["query"][5]
    steps = PLAN["end"]
    last = max([i + 1 for i, (name, step) in enumerate(steps) if step == 3 and chunks[name][5] < early], default=0)
    for name, step in steps[:last]:
        advance(name, step)
    send_final(0, 0, early).start()
    for name, step in steps[last:]:
        advance(name, step)
    rows_final = final.shape[1]
    send_final(1, early, rows_final - early).start()
    mine_out = load(0, final.at[core], final_out.at[0])
    mine_out.start()
    send_final(0, 0, early).wait_recv()
    early_out = load(1, final_got.at[pl.ds(0, early)], final_out.at[1, pl.ds(0, early)])
    early_out.start()
    for name in names:
        drain(name)
    send_x.wait_send()
    send_ids.wait_send()
    send_dy.wait_send()
    for t in range(blocks):
        send_att(t).wait_send()
        send_dn(t).wait_send()
    for t in range(half_blocks):
        write_out(t).wait()
        write_grad(t).wait()
        send_dn1(t).wait_send()
    send_final(0, 0, early).wait_send()
    send_final(1, early, rows_final - early).wait()
    late = pl.ds(early, rows_final - early)
    late_out = load(2, final_got.at[late], final_out.at[1, late])
    late_out.start()
    mine_out.wait()
    early_out.wait()
    late_out.wait()


def fused_shards(
    tokens, segment_ids, norm1_gain, w_query, w_key, w_value, w_out, norm2_gain, w_gate, w_up, w_down, out_grad,
):
    seqs, half_tokens, width = tokens.shape
    length = 2 * half_tokens
    cols = w_query.shape[1] // 2
    ff = w_gate.shape[1] // 2
    chunks, rows, rows_final = layout_of(width, cols, ff)
    core = lax.axis_index("seq")
    chip = lax.axis_index("dp")
    tables = tuple(jnp.asarray(t) for t in small_tables(length))
    any_space = pl.BlockSpec(memory_space=pl.ANY)
    vmem = pl.BlockSpec(memory_space=pltpu.VMEM)

    def low(*dims):
        return pltpu.VMEM(dims, BF)

    def full(*dims):
        return pltpu.VMEM(dims, F32)

    scratch = [
        low(length, width), low(length, width), pltpu.VMEM((1, length), jnp.int32),
        low(width, cols), low(width, cols), low(width, cols), low(width, width), low(width, ff), low(width, ff), low(ff, width),
        low(length, width), low(length, cols), low(length, cols), low(length, cols), low(length, cols), low(length, cols),
        full(length, LANES), full(TB, 3 * TB),
        full(length, width), low(length, width), low(length, ff), low(length, ff), low(length, ff), low(length, width),
        low(length, width), full(half_tokens, width), low(half_tokens, width), low(half_tokens, width), full(length, cols),
        full(half_tokens, width), low(half_tokens, width),
        full(LANES, width), low(8, rows, LANES), low(4, rows, LANES), low(2, rows, LANES), low(1, rows, LANES), low(rows, LANES),
        full(rows, LANES), full(2, rows_final, LANES), full(rows_final, LANES),
        pltpu.SemaphoreType.DMA((10,)), pltpu.SemaphoreType.DMA((17,)), pltpu.SemaphoreType.DMA((17,)),
        pltpu.SemaphoreType.DMA((4 * len(chunks),)), pltpu.SemaphoreType.DMA((4 * len(chunks),)),
    ]
    block_out, input_grad, final = pl.pallas_call(
        block_kernel,
        out_shape=(shape(half_tokens, width), shape(half_tokens, width), shape(2, rows_final, LANES, dtype=F32)),
        in_specs=[any_space] * 10 + [vmem] * 6,
        out_specs=[any_space] * 3,
        scratch_shapes=scratch,
        compiler_params=pltpu.CompilerParams(
            vmem_limit_bytes=67043328, collective_id=0, has_side_effects=True,
        ),
        name="block",
    )(
        tokens.reshape(half_tokens, width), segment_ids.reshape(1, half_tokens), out_grad.reshape(half_tokens, width),
        w_query, w_key, w_value, w_out, w_gate, w_up, w_down,
        norm1_gain.astype(F32).reshape(1, width), norm2_gain.astype(F32).reshape(1, width), *tables,
    )
    mine, got = final[0], final[1]
    holds = (chip >> 3) == core

    def part(name):
        _, _, kind, pieces, each, at = chunks[name]
        half = each // 2
        cut = slice(at, at + pieces * half)
        a, b = mine[cut].reshape(pieces, half, LANES), got[cut].reshape(pieces, half, LANES)
        if kind == "B":
            taken = jnp.where(holds, a, b)
        else:
            taken = jnp.where(core == 0, jnp.concatenate([a, b]), jnp.concatenate([b, a]))
        return jnp.transpose(taken, (0, 2, 1)).reshape(-1, half)

    gains = part("gains")
    gains = gains[:LANES] + gains[LANES:]
    summed = (
        gains[1] + gains[1 + LANES // 2],
        part("query"),
        part("key"),
        part("value"),
        part("out"),
        gains[0] + gains[LANES // 2],
        part("gate"),
        part("up"),
        part("down"),
    )
    return (block_out.reshape(seqs, half_tokens, width), input_grad.reshape(seqs, half_tokens, width), *summed)


def solution(mesh):
    placed = (P("dp", "seq", None), P("dp", "seq"), *([P()] * 9), P("dp", "seq", None))
    column = P(None, AX)
    chips = mesh.shape["dp"]
    body = fused_shards if chips == 16 else functools.partial(shards, chips=chips)
    return jax.shard_map(
        body,
        mesh=mesh,
        in_specs=placed,
        out_specs=(
            P("dp", "seq", None), P("dp", "seq", None), P(AX), column, column, column, column, P(AX), column, column, column,
        ),
        check_vma=False,
    )
```

```python
import functools

import jax
import jax.numpy as jnp
import numpy as np
from jax import lax
from jax.experimental import pallas as pl
from jax.experimental.pallas import tpu as pltpu
from jax.sharding import PartitionSpec as P

HD = 64
EPS = 1e-06
SCALE = 0.125
NEG = -1e30
BASE = 10000.0
AX = ("dp", "seq")
BF = jnp.bfloat16
F32 = jnp.float32
TB = 256
LANES = 128


def nn(a, b):
    return lax.dot_general(a, b, (((1,), (0,)), ((), ())), preferred_element_type=F32)


def nt(a, b):
    return lax.dot_general(a, b, (((1,), (1,)), ((), ())), preferred_element_type=F32)


def tn(a, b):
    return lax.dot_general(a, b, (((0,), (0,)), ((), ())), preferred_element_type=F32)


def small_tables(length):
    freqs = BASE ** (-np.arange(HD // 2, dtype=np.float64) * (2.0 / HD))
    lane_freqs = np.tile(freqs, 4)[None, :]
    fine = np.arange(64, dtype=np.float64)[:, None] * lane_freqs
    coarse = 64.0 * np.arange(length // 64, dtype=np.float64)[:, None] * lane_freqs
    return tuple(
        np.asarray(t, np.float32) for t in (np.cos(fine), np.sin(fine), np.cos(coarse), np.sin(coarse))
    )


def angle_block(tables, sub):
    cos_f, sin_f, cos_c, sin_c = tables
    ca = cos_c[pl.ds(sub, 1), :]
    sa = sin_c[pl.ds(sub, 1), :]
    cb = cos_f[...]
    sb = sin_f[...]
    low_half = (lax.broadcasted_iota(jnp.int32, (64, LANES), 1) % HD) < HD // 2
    cosine = ca * cb - sa * sb
    sine = sa * cb + ca * sb
    return cosine, jnp.where(low_half, -sine, sine), low_half


def rotate(v, cosine, sine, low_half):
    partner = jnp.where(low_half, pltpu.roll(v, LANES - HD // 2, 1), pltpu.roll(v, HD // 2, 1))
    return v * cosine + partner * sine


def window(block):
    return max(0, (block - 2) * TB)


def bias_of(seg_col, seg_row, block):
    first = window(block)
    keys = (block + 1) * TB - first
    rows = seg_col[pl.ds(block * TB, TB), :]
    cols = seg_row[:, pl.ds(first, keys)]
    q_at = block * TB + lax.broadcasted_iota(jnp.int32, (TB, keys), 0)
    k_at = first + lax.broadcasted_iota(jnp.int32, (TB, keys), 1)
    return jnp.where((rows == cols) & (k_at <= q_at), 0.0, NEG).astype(F32)


def forward_attention(
    core, own_ref, other_ref, gain_ref, wq_ref, wk_ref, wv_ref, cos_f, sin_f, cos_c, sin_c, seg_col, seg_row,
    normed_ref, q_ref, k_ref, v_ref, att_ref, lse_ref, bias_ref,
):
    s = core[0]
    half_tokens, width = own_ref.shape
    length = 2 * half_tokens
    cols = wq_ref.shape[1]
    tables = (cos_f, sin_f, cos_c, sin_c)

    def project(t, carry):
        rows = pl.ds(pl.multiple_of(t * TB, TB), TB)
        part = t // (half_tokens // TB)
        local = pl.ds(pl.multiple_of((t % (half_tokens // TB)) * TB, TB), TB)
        x = jnp.where(part == s, own_ref[local, :], other_ref[local, :]).astype(F32)
        r = lax.rsqrt(jnp.mean(x * x, axis=-1, keepdims=True) + EPS)
        normed = (x * r * gain_ref[...]).astype(BF)
        normed_ref[rows, :] = normed
        v_ref[rows, :] = nn(normed, wv_ref[...]).astype(BF)
        q = nn(normed, wq_ref[...]).astype(BF).astype(F32)
        k = nn(normed, wk_ref[...]).astype(BF).astype(F32)
        for sub in range(TB // 64):
            cosine, sine, low_half = angle_block(tables, t * (TB // 64) + sub)
            at = pl.ds(pl.multiple_of(t * TB + sub * 64, 64), 64)
            for tile in range(cols // LANES):
                lanes = slice(tile * LANES, (tile + 1) * LANES)
                part_rows = slice(sub * 64, (sub + 1) * 64)
                q_ref[at, lanes] = (rotate(q[part_rows, lanes], cosine, sine, low_half).astype(BF) * BF(SCALE)).astype(BF)
                k_ref[at, lanes] = rotate(k[part_rows, lanes], cosine, sine, low_half).astype(BF)
        return carry

    lax.fori_loop(0, length // TB, project, 0)

    for block in range(length // TB):
        first = window(block)
        keys = (block + 1) * TB - first
        bias_ref[:, :keys] = bias_of(seg_col, seg_row, block)
        rows = pl.ds(block * TB, TB)
        span = pl.ds(first, keys)

        def head(h, carry):
            lanes = pl.ds(pl.multiple_of((h // 2) * LANES, LANES), LANES)
            lane = lax.broadcasted_iota(jnp.int32, (1, LANES), 1)
            mine = (lane // HD) == (h % 2)
            q = q_ref[rows, lanes]
            qm = jnp.where(mine, q, jnp.zeros_like(q))
            scores = nt(qm, k_ref[span, lanes]) + bias_ref[:, :keys]
            peak = jnp.max(scores, axis=-1, keepdims=True)
            weights = jnp.exp(scores - peak)
            total = jnp.sum(weights, axis=-1, keepdims=True)
            probs = (weights * (1.0 / total)).astype(BF)
            result = nn(probs, v_ref[span, lanes]).astype(BF)
            att_ref[rows, lanes] = jnp.where(mine, result, att_ref[rows, lanes])
            lse_ref[rows, :] = jnp.where(lane == h, peak + jnp.log(total), lse_ref[rows, :])
            return carry

        lax.fori_loop(0, cols // HD, head, 0)


def feed_forward(
    core, slots_a, slots_b, own_ref, other_ref, att_own, att_other, gain_ref, wo_ref, wg_ref, wu_ref, wd_ref,
    dy_own, dy_other,
    res_ref, out_keep, out_send, dn_ref, pack_ref, normed, hidden, d_gate, d_up, dy_all,
):
    s = core[0]
    half_tokens, width = own_ref.shape
    length = 2 * half_tokens
    cols = att_own.shape[1]
    own_rows = pl.ds(pl.multiple_of(s * cols, cols), cols)
    other_rows = pl.ds(pl.multiple_of((1 - s) * cols, cols), cols)

    def block(t, carry):
        rows = pl.ds(pl.multiple_of(t * TB, TB), TB)
        part = t // (half_tokens // TB)
        local = pl.ds(pl.multiple_of((t % (half_tokens // TB)) * TB, TB), TB)
        is_own = part == s
        x = jnp.where(is_own, own_ref[local, :], other_ref[local, :]).astype(F32)
        dy = jnp.where(is_own, dy_own[local, :], dy_other[local, :])
        dy_all[rows, :] = dy
        residual = x + (nn(att_own[rows, :], wo_ref[own_rows, :]) + nn(att_other[rows, :], wo_ref[other_rows, :]))
        res_ref[rows, :] = residual
        r = lax.rsqrt(jnp.mean(residual * residual, axis=-1, keepdims=True) + EPS)
        n2 = (residual * r * gain_ref[...]).astype(BF)
        normed[rows, :] = n2
        gate = nn(n2, wg_ref[...])
        up = nn(n2, wu_ref[...])
        sig = 1.0 / (1.0 + jnp.exp(-gate))
        act = gate * sig
        hid = (act * up).astype(BF)
        hidden[rows, :] = hid
        down = nn(hid, wd_ref[...])

        @pl.when(is_own)
        def _():
            out_keep[local, :] = residual + down

        @pl.when(jnp.logical_not(is_own))
        def _():
            out_send[local, :] = down.astype(BF)

        d_hidden = nt(dy, wd_ref[...])
        dg = (d_hidden * up * (sig * (1.0 + gate * (1.0 - sig)))).astype(BF)
        du = (d_hidden * act).astype(BF)
        d_gate[rows, :] = dg
        d_up[rows, :] = du
        dn_ref[rows, :] = (nt(dg, wg_ref[...]) + nt(du, wu_ref[...])).astype(BF)
        return carry

    lax.fori_loop(0, length // TB, block, 0)

    wide = wg_ref.shape[1] // 8
    pieces = width // LANES

    def gate_up(o, carry):
        cut = pl.ds(pl.multiple_of(o * wide, wide), wide)
        slot = slots_b[o]
        for which, source in ((0, d_gate), (1, d_up)):
            grad = tn(source[:, cut], normed[...]).astype(BF)
            for piece in range(pieces):
                pack_ref[slot, pl.ds((which * pieces + piece) * wide, wide), :] = grad[:, piece * LANES : (piece + 1) * LANES]
        return carry

    lax.fori_loop(0, 8, gate_up, 0)
    low = width // 16
    base = 2 * pieces * wide
    deep = hidden.shape[1] // LANES
    for piece in range(deep):
        grad = tn(dy_all[...], hidden[:, piece * LANES : (piece + 1) * LANES]).astype(BF)
        for o in range(16):
            slot = slots_a[o]
            at = pl.multiple_of(base + (slot % 2) * (deep * low) + piece * low, 16)
            pack_ref[slot // 2, pl.ds(at, low), :] = grad[o * low : (o + 1) * low, :]


def backward_attention(
    core, slots_a, slots_b, own_ref, other_ref, gain_one, gain_two, wq_ref, wk_ref, wv_ref, wo_ref, dy_own, dy_other,
    res_ref, dn_own, dn_other, att_ref, normed_ref, q_ref, k_ref, v_ref, lse_ref, cos_f, sin_f, cos_c, sin_c, seg_col, seg_row,
    d_res, dn_keep, dn_send, pack_ref, d_branch, d_att, dq, dk, dv, dq_low, dk_low, dv_low, gains, bias_ref,
):
    s = core[0]
    half_tokens, width = own_ref.shape
    length = 2 * half_tokens
    cols = att_ref.shape[1]
    tables = (cos_f, sin_f, cos_c, sin_c)
    gains[...] = jnp.zeros_like(gains)

    def norm_two(t, carry):
        rows = pl.ds(pl.multiple_of(t * TB, TB), TB)
        part = t // (half_tokens // TB)
        local = pl.ds(pl.multiple_of((t % (half_tokens // TB)) * TB, TB), TB)
        is_own = part == s
        dy = jnp.where(is_own, dy_own[local, :], dy_other[local, :]).astype(F32)
        residual = res_ref[rows, :]
        dn = dn_own[rows, :].astype(F32) + dn_other[rows, :].astype(F32)
        r = lax.rsqrt(jnp.mean(residual * residual, axis=-1, keepdims=True) + EPS)
        scaled = residual * r
        e = gain_two[...] * dn
        gains[0:1, :] += jnp.sum(dn * scaled, axis=0, keepdims=True)
        grad = dy + r * (e - scaled * (r * jnp.mean(e * residual, axis=-1, keepdims=True)))
        low = grad.astype(BF)
        d_branch[rows, :] = low

        @pl.when(is_own)
        def _():
            d_res[local, :] = grad

        d_att[rows, :] = nt(low, wo_ref[...]).astype(BF)
        return carry

    lax.fori_loop(0, length // TB, norm_two, 0)

    dk[...] = jnp.zeros_like(dk)
    dv[...] = jnp.zeros_like(dv)
    for block in range(length // TB):
        first = window(block)
        keys = (block + 1) * TB - first
        bias_ref[:, :keys] = bias_of(seg_col, seg_row, block)
        rows = pl.ds(block * TB, TB)
        span = pl.ds(first, keys)

        def head(h, carry):
            lanes = pl.ds(pl.multiple_of((h // 2) * LANES, LANES), LANES)
            lane = lax.broadcasted_iota(jnp.int32, (1, LANES), 1)
            mine = (lane // HD) == (h % 2)
            q = q_ref[rows, lanes]
            qm = jnp.where(mine, q, jnp.zeros_like(q))
            do = d_att[rows, lanes]
            dom = jnp.where(mine, do, jnp.zeros_like(do))
            lse = jnp.sum(jnp.where(lane == h, lse_ref[rows, :], 0.0), axis=-1, keepdims=True)
            k = k_ref[span, lanes]
            probs = jnp.exp(nt(qm, k) + (bias_ref[:, :keys] - lse))
            d_probs = nt(dom, v_ref[span, lanes])
            delta = jnp.sum(probs * d_probs, axis=-1, keepdims=True)
            ds = (probs * (d_probs - delta)).astype(BF)
            part = nn(ds, k)
            dq[rows, lanes] = jnp.where(mine, part, dq[rows, lanes])
            dk[span, lanes] += tn(ds, qm)
            dv[span, lanes] += tn(probs.astype(BF), dom)
            return carry

        lax.fori_loop(0, cols // HD, head, 0)

    def finish(t, carry):
        rows = pl.ds(pl.multiple_of(t * TB, TB), TB)
        part = t // (half_tokens // TB)
        local = pl.ds(pl.multiple_of((t % (half_tokens // TB)) * TB, TB), TB)
        is_own = part == s
        for sub in range(TB // 64):
            cosine, sine, low_half = angle_block(tables, t * (TB // 64) + sub)
            at = pl.ds(pl.multiple_of(t * TB + sub * 64, 64), 64)
            for tile in range(cols // LANES):
                lanes = slice(tile * LANES, (tile + 1) * LANES)
                dq_low[at, lanes] = (rotate(dq[at, lanes], cosine, -sine, low_half) * SCALE).astype(BF)
                dk_low[at, lanes] = rotate(dk[at, lanes], cosine, -sine, low_half).astype(BF)
        dv_low[rows, :] = dv[rows, :].astype(BF)
        dn = nt(dq_low[rows, :], wq_ref[...]) + nt(dk_low[rows, :], wk_ref[...]) + nt(dv_low[rows, :], wv_ref[...])
        x = jnp.where(is_own, own_ref[local, :], other_ref[local, :]).astype(F32)
        r = lax.rsqrt(jnp.mean(x * x, axis=-1, keepdims=True) + EPS)
        gains[1:2, :] += jnp.sum(dn * (x * r), axis=0, keepdims=True)

        @pl.when(is_own)
        def _():
            dn_keep[local, :] = dn

        @pl.when(jnp.logical_not(is_own))
        def _():
            dn_send[local, :] = dn.astype(BF)

        return carry

    lax.fori_loop(0, length // TB, finish, 0)

    low = width // 16
    pieces = width // LANES
    for which, source in ((0, dq_low), (1, dk_low), (2, dv_low)):
        for piece in range(pieces):
            grad = tn(source[...], normed_ref[:, piece * LANES : (piece + 1) * LANES]).astype(BF)
            for o in range(8):
                at = (which * pieces + piece) * low
                pack_ref[slots_b[o], pl.ds(at, low), :] = grad[o * low : (o + 1) * low, :]
    turned = jnp.transpose(gains[...])
    turned_low = turned.astype(BF)
    rest = (turned - turned_low.astype(F32)).astype(BF)
    lane = lax.broadcasted_iota(jnp.int32, (1, LANES), 1)
    both = jnp.where(lane < LANES // 2, turned_low, pltpu.roll(rest.astype(F32), LANES // 2, 1).astype(BF))
    at_b = 3 * pieces * low
    size_a = (cols // LANES + 1) * low
    base = at_b + low
    for piece in range(cols // LANES):
        grad = tn(d_branch[...], att_ref[:, piece * LANES : (piece + 1) * LANES]).astype(BF)
        for o in range(16):
            slot = slots_a[o]
            at = pl.multiple_of(base + (slot % 2) * size_a + piece * low, 16)
            pack_ref[slot // 2, pl.ds(at, low), :] = grad[o * low : (o + 1) * low, :]
    for o in range(16):
        slot = slots_a[o]
        at = pl.multiple_of(base + (slot % 2) * size_a + (cols // LANES) * low, 16)
        pack_ref[slot // 2, pl.ds(at, low), :] = both[o * low : (o + 1) * low, :]

        @pl.when(s == o // 8)
        def _():
            pack_ref[slots_b[o % 8], pl.ds(at_b, low), :] = both[o * low : (o + 1) * low, :]


BIG = pltpu.CompilerParams(vmem_limit_bytes=60 * 1024 * 1024)


def shape(*dims, dtype=BF):
    return jax.ShapeDtypeStruct(dims, dtype)


def flat(dp, core):
    return 2 * dp + core


def swap_cores(chips):
    return [(flat(d, c), flat(d, 1 - c)) for d in range(chips) for c in range(2)]


ORDER = ((0, 1, 2, 3), (1, 0, 2, 3))


def swap_chips(step):
    return [(flat(d, c), flat(d ^ (1 << ORDER[c][step]), c)) for d in range(16) for c in range(2)]


def to_owner_half():
    return [(flat(d, c), flat(d ^ 8, c)) for d in range(16) for c in range(2) if d // 8 != c]


def slot_tables(chip, core, chips):
    if chips != 16:
        return jnp.arange(16, dtype=jnp.int32), jnp.arange(8, dtype=jnp.int32)
    owner = jnp.arange(16, dtype=jnp.int32)
    away = owner ^ chip
    x, y, z0, z1 = away & 1, (away >> 1) & 1, (away >> 2) & 1, (away >> 3) & 1
    first = jnp.where(core == 0, x, y)
    second = jnp.where(core == 0, y, x)
    slots_a = first * 8 + second * 4 + z0 * 2 + z1
    near = slots_a // 2
    return slots_a, jnp.where(core == 0, near[:8], near[8:])


def halve(pack):
    for step in range(3):
        half = pack.shape[0] // 2
        pack3 = pack.reshape(2, half, *pack.shape[1:])
        got = lax.ppermute(pack3[1], AX, swap_chips(step))
        total = pack3[0].astype(F32) + got.astype(F32)
        pack = total.astype(BF) if step < 2 else total
    return pack[0]


def last_step(total, size_b):
    kind_b = total[:size_b]
    kind_a = total[size_b:].reshape(2, -1, LANES)
    got_a = lax.ppermute(kind_a[1].astype(BF), AX, swap_chips(3))
    got_b = lax.ppermute(kind_b.astype(BF), AX, to_owner_half())
    return kind_a[0] + got_a.astype(F32), kind_b + got_b.astype(F32)


def shards(
    tokens, segment_ids, norm1_gain, w_query, w_key, w_value, w_out, norm2_gain, w_gate, w_up, w_down, out_grad,
    *, chips,
):
    seqs, half_tokens, width = tokens.shape
    length = 2 * half_tokens
    cols = w_query.shape[1] // 2
    ff = w_gate.shape[1] // 2
    core = lax.axis_index("seq")
    chip = lax.axis_index("dp")
    core_id = core.reshape(1).astype(jnp.int32)
    pairs = swap_cores(chips)
    own = tokens.reshape(half_tokens, width)
    dy_own = out_grad.reshape(half_tokens, width)
    ids = segment_ids.reshape(1, half_tokens)
    other = lax.ppermute(own, AX, pairs)
    ids_other = lax.ppermute(ids, AX, pairs)
    dy_other = lax.ppermute(dy_own, AX, pairs)
    seg_row = jnp.where(core == 0, jnp.concatenate([ids, ids_other], 1), jnp.concatenate([ids_other, ids], 1))
    seg_col = seg_row.reshape(length, 1)
    gain_one = norm1_gain.astype(F32).reshape(1, width)
    gain_two = norm2_gain.astype(F32).reshape(1, width)
    tables = tuple(jnp.asarray(t) for t in small_tables(length))
    slots_a, slots_b = slot_tables(chip, core, chips)
    half_w = pl.BlockSpec((width, cols), lambda g, c: (0, c[0]))
    half_wide = pl.BlockSpec((width, ff), lambda g, c, a, b: (0, c[0]))
    whole = lambda a: pl.BlockSpec(a.shape, lambda g, *_: (0,) * len(a.shape))

    def out_block(s):
        return pl.BlockSpec(s.shape, lambda g, *_: (0,) * len(s.shape))

    outs = (
        shape(length, width), shape(length, cols), shape(length, cols), shape(length, cols), shape(length, cols),
        shape(length, LANES, dtype=F32),
    )
    normed1, q, k, v, att, lse = pl.pallas_call(
        forward_attention,
        out_shape=outs,
        grid_spec=pltpu.PrefetchScalarGridSpec(
            num_scalar_prefetch=1,
            grid=(1,),
            in_specs=[whole(own), whole(other), whole(gain_one), half_w, half_w, half_w]
            + [whole(t) for t in tables]
            + [whole(seg_col), whole(seg_row)],
            out_specs=[out_block(o) for o in outs],
            scratch_shapes=[pltpu.VMEM((TB, 3 * TB), F32)],
        ),
        compiler_params=BIG,
        name="attention_forward",
    )(core_id, own, other, gain_one, w_query, w_key, w_value, *tables, seg_col, seg_row)
    att_other = lax.ppermute(att, AX, pairs)

    rows_one = 2 * (width // LANES) * (ff // 8) + 2 * (ff // LANES) * (width // 16)
    outs = (
        shape(length, width, dtype=F32), shape(half_tokens, width, dtype=F32), shape(half_tokens, width),
        shape(length, width), shape(8, rows_one, LANES),
    )
    residual, out_keep, out_send, dn, pack_one = pl.pallas_call(
        feed_forward,
        out_shape=outs,
        grid_spec=pltpu.PrefetchScalarGridSpec(
            num_scalar_prefetch=3,
            grid=(1,),
            in_specs=[whole(own), whole(other), whole(att), whole(att), whole(gain_two), whole(w_out), half_wide, half_wide,
                      pl.BlockSpec((ff, width), lambda g, c, a, b: (c[0], 0)), whole(own), whole(own)],
            out_specs=[out_block(o) for o in outs],
            scratch_shapes=[
                pltpu.VMEM((length, width), BF), pltpu.VMEM((length, ff), BF), pltpu.VMEM((length, ff), BF),
                pltpu.VMEM((length, ff), BF), pltpu.VMEM((length, width), BF),
            ],
        ),
        compiler_params=BIG,
        name="feed_forward",
    )(core_id, slots_a, slots_b, own, other, att, att_other, gain_two, w_out, w_gate, w_up, w_down, dy_own, dy_other)
    out_other = lax.ppermute(out_send, AX, pairs)
    block_out = (out_keep + out_other.astype(F32)).astype(BF)
    dn_other = lax.ppermute(dn, AX, pairs)

    low = width // 16
    size_b2 = 3 * (width // LANES) * low + low
    size_a2 = (cols // LANES + 1) * low
    outs = (
        shape(half_tokens, width, dtype=F32), shape(half_tokens, width, dtype=F32), shape(half_tokens, width),
        shape(8, size_b2 + 2 * size_a2, LANES),
    )
    half_w3 = pl.BlockSpec((width, cols), lambda g, c, a, b: (0, c[0]))
    inputs = (own, other, gain_one, gain_two, w_query, w_key, w_value, w_out, dy_own, dy_other, residual, dn, dn_other,
              att, normed1, q, k, v, lse, *tables, seg_col, seg_row)
    specs = [whole(a) for a in inputs]
    specs[4] = specs[5] = specs[6] = half_w3
    specs[7] = pl.BlockSpec((cols, width), lambda g, c, a, b: (c[0], 0))
    d_res, dn_keep, dn_send, pack_two = pl.pallas_call(
        backward_attention,
        out_shape=outs,
        grid_spec=pltpu.PrefetchScalarGridSpec(
            num_scalar_prefetch=3,
            grid=(1,),
            in_specs=specs,
            out_specs=[out_block(o) for o in outs],
            scratch_shapes=[
                pltpu.VMEM((length, width), BF), pltpu.VMEM((length, cols), BF),
                pltpu.VMEM((length, cols), F32), pltpu.VMEM((length, cols), F32), pltpu.VMEM((length, cols), F32),
                pltpu.VMEM((length, cols), BF), pltpu.VMEM((length, cols), BF), pltpu.VMEM((length, cols), BF),
                pltpu.VMEM((LANES, width), F32), pltpu.VMEM((TB, 3 * TB), F32),
            ],
        ),
        compiler_params=BIG,
        name="attention_backward",
    )(core_id, slots_a, slots_b, *inputs)
    dn1 = dn_keep + lax.ppermute(dn_send, AX, pairs).astype(F32)
    x = own.astype(F32)
    r = lax.rsqrt(jnp.mean(x * x, axis=-1, keepdims=True) + EPS)
    e = gain_one * dn1
    input_grad = (d_res + r * e - x * (r * r * r) * jnp.mean(e * x, axis=-1, keepdims=True)).astype(BF)

    pieces = width // LANES
    wide = ff // 8
    size_b1 = 2 * pieces * wide
    size_a1 = (ff // LANES) * low

    if chips == 16:
        one_a, one_b = last_step(halve(pack_one), size_b1)
        two_a, two_b = last_step(halve(pack_two), size_b2)
        holds = (chip >> 3) == core

        def share(a):
            parts = a.reshape(a.shape[0], 2, a.shape[1] // 2, LANES)
            mine = jnp.where(core == 0, parts[:, 0], parts[:, 1])
            theirs = jnp.where(core == 0, parts[:, 1], parts[:, 0])
            return mine, lax.ppermute(theirs, AX, pairs)

        def both(a):
            mine, got = share(a)
            return jnp.where(core == 0, mine, got), jnp.where(core == 0, got, mine)

        def one(a):
            mine, got = share(a)
            return jnp.where(holds, mine, got)

        down_lo, down_hi = both(one_a.reshape(ff // LANES, low, LANES))
        kind_a = two_a.reshape(cols // LANES + 1, low, LANES)
        out_lo, out_hi = both(kind_a)
        gates = one(one_b.reshape(2 * pieces, wide, LANES))
        rest = one(two_b.reshape(3 * pieces + 1, low, LANES))

        def turn(a):
            return jnp.transpose(a, (0, 2, 1)).reshape(-1, a.shape[1])

        tiles = cols // LANES
        gain1 = out_lo[tiles] + out_hi[tiles]
        gain1 = gain1[:, 1] + gain1[:, 1 + LANES // 2]
        gain2 = rest[3 * pieces]
        gain2 = gain2[:, 0] + gain2[:, LANES // 2]
        summed = (
            gain1,
            turn(rest[:pieces]),
            turn(rest[pieces : 2 * pieces]),
            turn(rest[2 * pieces : 3 * pieces]),
            turn(jnp.concatenate([out_lo[:tiles], out_hi[:tiles]])),
            gain2,
            turn(gates[:pieces]),
            turn(gates[pieces:]),
            turn(jnp.concatenate([down_lo, down_hi])),
        )
    else:
        def plain_b(rows, count, size, at):
            part = rows[:, at : at + count * size].reshape(8, count, size, LANES)
            part = jnp.transpose(part, (1, 3, 0, 2)).reshape(count * LANES, 8 * size).astype(F32)
            zero = jnp.zeros_like(part)
            return jnp.where(core == 0, jnp.concatenate([part, zero], 1), jnp.concatenate([zero, part], 1))

        def plain_a(rows, count, at, each):
            part = rows[:, at:].reshape(8, 2, each, low, LANES)[:, :, :count].reshape(16, count, low, LANES)
            part = jnp.transpose(part, (1, 3, 0, 2)).reshape(count * LANES, 16 * low).astype(F32)
            zero = jnp.zeros_like(part)
            return jnp.where(core == 0, jnp.concatenate([part, zero], 0), jnp.concatenate([zero, part], 0))

        def scatter(a):
            return lax.psum_scatter(a, AX, scatter_dimension=1, tiled=True)

        tiles = cols // LANES
        gain_a = pack_two[:, size_b2:].reshape(16, tiles + 1, low, LANES)[:, tiles].astype(F32)
        gain_a = gain_a[:, :, : LANES // 2] + gain_a[:, :, LANES // 2 :]
        gain_a = gain_a.reshape(width, LANES // 2)
        gain1 = gain_a[:, 1].reshape(1, width)
        gain2 = jnp.where(core == 0, gain_a[:, 0], 0.0).reshape(1, width)
        n = pieces * low
        summed = (
            scatter(gain1).reshape(-1),
            scatter(plain_b(pack_two, pieces, low, 0)),
            scatter(plain_b(pack_two, pieces, low, n)),
            scatter(plain_b(pack_two, pieces, low, 2 * n)),
            scatter(plain_a(pack_two, tiles, size_b2, tiles + 1)),
            scatter(gain2).reshape(-1),
            scatter(plain_b(pack_one, pieces, wide, 0)),
            scatter(plain_b(pack_one, pieces, wide, pieces * wide)),
            scatter(plain_a(pack_one, ff // LANES, size_b1, ff // LANES)),
        )
    return (block_out.reshape(seqs, half_tokens, width), input_grad.reshape(seqs, half_tokens, width), *summed)


MESH = pl.DeviceIdType.MESH


PLAN = {
    "n0": (("down", 0),),
    "a22": (("down", 1),),
    "a30": (("up", 0),),
    "a31": (("gate", 0), ("out", 0),),
    "lower": (("down", 2),),
    "d1": (("up", 1),),
    "f1": (("down", 3), ("gate", 1), ("out", 1),),
    "f3": (("value", 0), ("query", 0),),
    "end": (("up", 2), ("gate", 2), ("out", 2), ("key", 0), ("query", 1), ("value", 1), ("gains", 0), ("key", 1), ("up", 3), ("value", 2), ("query", 2), ("gains", 1), ("gate", 3), ("key", 2), ("out", 3), ("gains", 2), ("value", 3), ("query", 3), ("key", 3), ("gains", 3),),
}
Z_FIRST = ("gate", "value",)


def bit(value, place):
    return (value // (1 << place)) % 2


def other_bit(a, b):
    return a + b - 2 * a * b


def layout_of(width, cols, ff):
    low, wide = width // 16, ff // 8
    table, row, final = {}, 0, 0
    for name, kind, pieces, each in (
        ("gate", "B", width // LANES, wide), ("up", "B", width // LANES, wide), ("down", "A", ff // LANES, low),
        ("out", "A", cols // LANES, low), ("query", "B", width // LANES, low), ("key", "B", width // LANES, low),
        ("value", "B", width // LANES, low), ("gains", "A", 1, low),
    ):
        rows = pieces * each * (2 if kind == "A" else 1)
        table[name] = (row, rows, kind, pieces, each, final)
        row, final = row + rows, final + pieces * each // 2
    return table, row, final


def block_kernel(
    x_hbm, ids_hbm, dy_hbm, wq_hbm, wk_hbm, wv_hbm, wo_hbm, wg_hbm, wu_hbm, wd_hbm, gain_one_low, gain_two_low,
    cos_f, sin_f, cos_c, sin_c,
    block_out, input_grad, final_out,
    xs, dys, ids, wq, wk, wv, wo, wg, wu, wd, normed1, q_ref, k_ref, v_ref, att, att_other, lse_ref, bias_ref,
    gain_one, gain_two, res_ref, normed2, hidden, d_gate, d_up, dn_own, dn_other, d_res, out_send, out_got, dv_ref, dn_keep, dn_got,
    gains, pack, got1, got2, got3, got4, acc, final, final_got,
    load_sem, pair_send, pair_recv, hop_send, hop_recv,
):
    core = lax.axis_index("seq")
    chip = lax.axis_index("dp")
    half_tokens, width = x_hbm.shape
    length = 2 * half_tokens
    cols = wq.shape[1]
    ff = wg.shape[1]
    blocks = length // TB
    half_blocks = half_tokens // TB
    tables = (cos_f, sin_f, cos_c, sin_c)
    chunks, _, _ = layout_of(width, cols, ff)
    names = list(chunks)
    low = width // 16

    bx, by, bz, bw = (bit(chip, i) for i in range(4))
    step_x, step_y = 1 - 2 * bx, 2 * (1 - 2 * by)
    near = chip + (1 - core) * step_x + core * step_y
    aside = chip + core * step_x + (1 - core) * step_y
    above = chip + 4 * (1 - 2 * bz)
    across = chip + 8 * (1 - 2 * bw)
    partners = (near, aside, above, across)
    holds = bw == core

    def path_of(name):
        return (above, near, aside, across) if name in Z_FIRST else partners

    def slot_of(name, owner):
        kx, ky, kz = other_bit(bx, owner & 1), other_bit(by, (owner >> 1) & 1), other_bit(bz, (owner >> 2) & 1)
        first = (1 - core) * kx + core * ky
        second = core * kx + (1 - core) * ky
        slot = kz * 4 + first * 2 + second if name in Z_FIRST else first * 4 + second * 2 + kz
        return slot, other_bit(bw, (owner >> 3) & 1)

    def owner_of(name, first, second, third):
        if name in Z_FIRST:
            first, second, third = second, third, first
        kx = (1 - core) * first + core * second
        ky = core * first + (1 - core) * second
        return other_bit(bx, kx) + 2 * other_bit(by, ky) + 4 * other_bit(bz, third)

    barrier = pltpu.get_barrier_semaphore()
    everyone = [{"dp": chip, "seq": 1 - core}] + [{"dp": p, "seq": core} for p in partners]
    for device in everyone:
        pl.semaphore_signal(barrier, inc=1, device_id=device, device_id_type=MESH)

    own_rows = pl.ds(pl.multiple_of(core * half_tokens, half_tokens), half_tokens)
    own_cols = pl.ds(pl.multiple_of(core * cols, cols), cols)
    own_ff = pl.ds(pl.multiple_of(core * ff, ff), ff)

    def load(i, src, dst):
        return pltpu.make_async_copy(src, dst, load_sem.at[i])

    loads = [
        load(0, x_hbm, xs.at[own_rows]),
        load(1, wv_hbm.at[:, own_cols], wv),
        load(2, wq_hbm.at[:, own_cols], wq),
        load(3, wk_hbm.at[:, own_cols], wk),
        load(4, ids_hbm, ids.at[:, own_rows]),
        load(5, wo_hbm, wo),
        load(6, wg_hbm.at[:, own_ff], wg),
        load(7, wu_hbm.at[:, own_ff], wu),
        load(8, wd_hbm.at[own_ff, :], wd),
        load(9, dy_hbm, dys.at[own_rows]),
    ]
    for copy in loads[:5]:
        copy.start()

    def to_pair(i, src, dst):
        return pltpu.make_async_remote_copy(
            src_ref=src, dst_ref=dst, send_sem=pair_send.at[i], recv_sem=pair_recv.at[i],
            device_id={"dp": chip, "seq": 1 - core}, device_id_type=MESH,
        )

    send_x = to_pair(0, x_hbm, xs.at[own_rows])
    send_ids = to_pair(1, ids_hbm, ids.at[:, own_rows])
    send_dy = to_pair(2, dy_hbm, dys.at[own_rows])

    def rows_of(t):
        return pl.ds(pl.multiple_of(t * TB, TB), TB)

    def send_att(t):
        return to_pair(3 + t, att.at[rows_of(t)], att_other.at[rows_of(t)])

    def send_dn(t):
        return to_pair(7 + t, dn_own.at[rows_of(t)], dn_other.at[rows_of(t)])

    def send_out(t):
        return to_pair(11 + t, out_send.at[rows_of(t)], out_got.at[rows_of(t)])

    def send_dn1(t):
        return to_pair(13 + t, out_send.at[rows_of(t)], dn_got.at[rows_of(t)])

    def write_out(t):
        return pltpu.make_async_copy(out_got.at[rows_of(t)], block_out.at[rows_of(t)], load_sem.at[3 + t])

    def write_grad(t):
        return pltpu.make_async_copy(dn_got.at[rows_of(t)], input_grad.at[rows_of(t)], load_sem.at[5 + t])

    def send_final(i, first, count):
        rows = pl.ds(first, count)
        return to_pair(15 + i, final.at[1 - core, rows], final_got.at[rows])


    def hop(name, step):
        row, count, kind = chunks[name][:3]
        at = 4 * names.index(name) + step
        rows = pl.ds(row, count)
        if step < 3:
            n = 4 >> step
            src, dst = pack.at[pl.ds(n, n), rows], (got1, got2, got3)[step].at[:, rows]
        elif kind == "B":
            src, dst = pack.at[0, rows], got4.at[rows]
        else:
            src, dst = pack.at[0, pl.ds(row + count // 2, count // 2)], got4.at[pl.ds(row, count // 2)]
        return pltpu.make_async_remote_copy(
            src_ref=src, dst_ref=dst, send_sem=hop_send.at[at], recv_sem=hop_recv.at[at],
            device_id={"dp": path_of(name)[step], "seq": core}, device_id_type=MESH,
        )

    def start(name, step):
        if step == 3 and chunks[name][2] == "B":
            @pl.when(jnp.logical_not(holds))
            def _():
                hop(name, step).start()
        else:
            hop(name, step).start()

    def advance(name, step):
        row, count, kind, pieces, each, at = chunks[name]
        if step < 3:
            hop(name, step).wait_recv()
            n = 4 >> step
            size = 384 if count % 384 == 0 else (288 if count % 288 == 0 else count)
            source = (got1, got2, got3)[step]
            per = count // size

            def add(i, carry):
                slab = i // per
                rows = pl.ds(pl.multiple_of(row + (i % per) * size, 16), size)
                total = pack[slab, rows, :].astype(F32) + source[slab, rows, :].astype(F32)
                pack[slab, rows, :] = total.astype(BF)
                if step == 2:
                    acc[rows, :] = total
                return carry

            lax.fori_loop(0, n * per, add, 0)
            start(name, step + 1)
            return
        half = each // 2
        if kind == "B":
            @pl.when(holds)
            def _():
                hop(name, step).wait_recv()
                for p in range(pieces):
                    for c in range(2):
                        rows = pl.ds(row + p * each + c * half, half)
                        final[c, pl.ds(at + p * half, half), :] = acc[rows, :] + got4[rows, :].astype(F32)

            @pl.when(jnp.logical_not(holds))
            def _():
                hop(name, step).wait_send()
                for p in range(pieces):
                    for c in range(2):
                        final[c, pl.ds(at + p * half, half), :] = acc[pl.ds(row + p * each + c * half, half), :]
        else:
            hop(name, step).wait_recv()
            for p in range(pieces):
                for c in range(2):
                    rows = pl.ds(row + p * each + c * half, half)
                    final[c, pl.ds(at + p * half, half), :] = acc[rows, :] + got4[rows, :].astype(F32)

    def proceed(point, here=None):
        steps = PLAN.get(point, ())
        if not steps:
            return
        if here is None:
            for name, step in steps:
                advance(name, step)
            return

        @pl.when(here)
        def _():
            for name, step in steps:
                advance(name, step)

    def drain(name):
        for step in range(3):
            hop(name, step).wait_send()
        if chunks[name][2] == "A":
            hop(name, 3).wait_send()


    gain_one[...] = gain_one_low[...].astype(F32).reshape(1, width)
    gain_two[...] = gain_two_low[...].astype(F32).reshape(1, width)
    pl.semaphore_wait(barrier, len(everyone))
    send_x.start()
    send_ids.start()
    for copy in loads[:4]:
        copy.wait()
    for copy in loads[5:]:
        copy.start()
    send_dy.start()

    def project(j, carry):
        t = (core * half_blocks + j) % blocks

        @pl.when(j == half_blocks)
        def _():
            send_x.wait_recv()

        rows = rows_of(t)
        x = xs[rows, :].astype(F32)
        r = lax.rsqrt(jnp.mean(x * x, axis=-1, keepdims=True) + EPS)
        normed = (x * r * gain_one[...]).astype(BF)
        normed1[rows, :] = normed
        v_ref[rows, :] = nn(normed, wv[...]).astype(BF)
        q = nn(normed, wq[...]).astype(BF).astype(F32)
        k = nn(normed, wk[...]).astype(BF).astype(F32)
        for sub in range(TB // 64):
            cosine, sine, low_half = angle_block(tables, t * (TB // 64) + sub)
            at = pl.ds(pl.multiple_of(t * TB + sub * 64, 64), 64)
            for tile in range(cols // LANES):
                lanes = slice(tile * LANES, (tile + 1) * LANES)
                part = slice(sub * 64, (sub + 1) * 64)
                q_ref[at, lanes] = (rotate(q[part, lanes], cosine, sine, low_half).astype(BF) * BF(SCALE)).astype(BF)
                k_ref[at, lanes] = rotate(k[part, lanes], cosine, sine, low_half).astype(BF)
        return carry

    lax.fori_loop(0, blocks, project, 0)
    loads[4].wait()
    send_ids.wait_recv()
    lse_ref[...] = jnp.transpose(jnp.broadcast_to(ids[...].astype(F32), (LANES, length)))

    def set_bias(block):
        first = window(block)
        keys = (block + 1) * TB - first
        rows = lse_ref[pl.ds(block * TB, TB), LANES - 1 :]
        columns = ids[:, pl.ds(first, keys)].astype(F32)
        q_at = block * TB + lax.broadcasted_iota(jnp.int32, (TB, keys), 0)
        k_at = first + lax.broadcasted_iota(jnp.int32, (TB, keys), 1)
        bias_ref[:, :keys] = jnp.where((rows == columns) & (k_at <= q_at), 0.0, NEG).astype(F32)

    lane = lax.broadcasted_iota(jnp.int32, (1, LANES), 1)
    first_head = lane < HD
    for block in range(blocks):
        first = window(block)
        keys = (block + 1) * TB - first
        set_bias(block)
        rows = pl.ds(block * TB, TB)
        span = pl.ds(first, keys)

        def pair(j, carry, rows=rows, span=span, keys=keys):
            lanes = pl.ds(pl.multiple_of(j * LANES, LANES), LANES)
            q, k, v = q_ref[rows, lanes], k_ref[span, lanes], v_ref[span, lanes]
            results, sums = [], []
            for mine in (first_head, jnp.logical_not(first_head)):
                scores = nt(jnp.where(mine, q, jnp.zeros_like(q)), k) + bias_ref[:, :keys]
                peak = jnp.max(scores, axis=-1, keepdims=True)
                weights = jnp.exp(scores - peak)
                total = jnp.sum(weights, axis=-1, keepdims=True)
                results.append(nn(weights.astype(BF), v) * (1.0 / total))
                sums.append(peak + jnp.log(total))
            att[rows, lanes] = jnp.where(first_head, *results).astype(BF)
            old = jnp.where(lane == 2 * j + 1, sums[1], lse_ref[rows, :])
            lse_ref[rows, :] = jnp.where(lane == 2 * j, sums[0], old)
            return carry

        lax.fori_loop(0, cols // LANES, pair, 0)
        send_att(block).start()


    for copy in loads[5:]:
        copy.wait()
    send_dy.wait_recv()
    other_cols = pl.ds(pl.multiple_of((1 - core) * cols, cols), cols)

    def feed(t, carry):
        rows = rows_of(t)
        local = rows_of(t % half_blocks)
        send_att(t).wait_recv()
        x = xs[rows, :].astype(F32)
        residual = x + (nn(att[rows, :], wo[own_cols, :]) + nn(att_other[rows, :], wo[other_cols, :]))
        res_ref[rows, :] = residual

        @pl.when(t // half_blocks == core)
        def _():
            dn_keep[local, :] = residual

        r = lax.rsqrt(jnp.mean(residual * residual, axis=-1, keepdims=True) + EPS)
        n2 = (residual * r * gain_two[...]).astype(BF)
        normed2[rows, :] = n2
        gate = nn(n2, wg[...])
        up = nn(n2, wu[...])
        hidden[rows, :] = (gate * (1.0 / (1.0 + jnp.exp(-gate))) * up).astype(BF)
        d_gate[rows, :] = gate.astype(BF)
        d_up[rows, :] = up.astype(BF)
        return carry

    lax.fori_loop(0, blocks, feed, 0)

    def spread(name, piece, grad):
        row, rows = chunks[name][:2]
        for o in range(16):
            slot, far = slot_of(name, o)
            at = pl.multiple_of(row + far * (rows // 2) + piece * low, 16)
            pack[slot, pl.ds(at, low), :] = grad[o * low : (o + 1) * low, :]

    def down_part(part, carry):
        at = part * (ff // 2)
        grad = tn(dys[...], hidden[:, pl.ds(pl.multiple_of(at, LANES), ff // 2)]).astype(BF)
        for piece in range(ff // 2 // LANES):
            spread("down", part * (ff // 2 // LANES) + piece, grad[:, piece * LANES : (piece + 1) * LANES])
        return carry

    lax.fori_loop(0, 2, down_part, 0)
    start("down", 0)

    def feed_back(t, carry):
        rows = rows_of(t)
        gate = d_gate[rows, :].astype(F32)
        up = d_up[rows, :].astype(F32)
        sig = 1.0 / (1.0 + jnp.exp(-gate))
        d_hidden = nt(dys[rows, :], wd[...])
        dg = (d_hidden * up * (sig * (1.0 + gate * (1.0 - sig)))).astype(BF)
        du = (d_hidden * (gate * sig)).astype(BF)
        d_gate[rows, :] = dg
        d_up[rows, :] = du
        dn_own[rows, :] = (nt(dg, wg[...]) + nt(du, wu[...])).astype(BF)
        send_dn(t).start()
        for n in range(blocks):
            proceed(f"fb{n}", t == n)
        return carry

    lax.fori_loop(0, blocks, feed_back, 0)

    wide = ff // 8
    pieces = width // LANES

    def gate_up(name, source, first):
        row = chunks[name][0]

        cuts = []
        for j in range(4):
            owner = owner_of(name, first, j // 2, j % 2)
            cuts.append(source[:, pl.ds(pl.multiple_of(owner * wide, wide), wide)])
        grad = tn(jnp.concatenate(cuts, axis=1), normed2[...]).astype(BF)
        for j in range(4):
            for piece in range(pieces):
                part = grad[j * wide : (j + 1) * wide, piece * LANES : (piece + 1) * LANES]
                pack[4 * first + j, pl.ds(row + piece * wide, wide), :] = part

    gate_up("gate", d_gate, 1)
    start("gate", 0)
    proceed("g1")
    gate_up("gate", d_gate, 0)
    proceed("g0")
    gate_up("up", d_up, 1)
    start("up", 0)
    proceed("u1")
    gate_up("up", d_up, 0)
    proceed("u0")


    d_branch, d_att = normed2, att_other
    gains[...] = jnp.zeros_like(gains)

    def norm_two(t, carry):
        rows = rows_of(t)
        local = rows_of(t % half_blocks)
        is_own = t // half_blocks == core
        send_dn(t).wait_recv()
        dy = dys[rows, :].astype(F32)
        residual = res_ref[rows, :]
        dn = dn_own[rows, :].astype(F32) + dn_other[rows, :].astype(F32)
        r = lax.rsqrt(jnp.mean(residual * residual, axis=-1, keepdims=True) + EPS)
        scaled = residual * r
        e = gain_two[...] * dn
        grad = dy + r * (e - scaled * (r * jnp.mean(e * residual, axis=-1, keepdims=True)))
        small = grad.astype(BF)
        d_branch[rows, :] = small
        d_att[rows, :] = nt(small, wo[own_cols, :]).astype(BF)

        @pl.when(is_own)
        def _():
            gains[0:1, :] += jnp.sum(dn * scaled, axis=0, keepdims=True)
            d_res[local, :] = grad

        for n in range(blocks):
            proceed(f"n{n}", t == n)
        return carry

    lax.fori_loop(0, blocks, norm_two, 0)

    out_grad = tn(d_branch[...], att[...]).astype(BF)
    for piece in range(cols // LANES):
        spread("out", piece, out_grad[:, piece * LANES : (piece + 1) * LANES])
    start("out", 0)
    proceed("out")

    res_ref[:, cols:] = jnp.zeros((length, cols), F32)
    dv_ref[...] = jnp.zeros_like(dv_ref)

    def attention_back(block):
        first = window(block)
        keys = (block + 1) * TB - first
        rows = pl.ds(block * TB, TB)
        span = pl.ds(first, keys)

        def pair(j, carry):
            at = pl.multiple_of(j * LANES, LANES)
            lanes = pl.ds(at, LANES)
            k_lanes = pl.ds(pl.multiple_of(cols + at, LANES), LANES)
            q, do, k, v = q_ref[rows, lanes], d_att[rows, lanes], k_ref[span, lanes], v_ref[span, lanes]
            products = do.astype(F32) * att[rows, lanes].astype(F32)
            q_parts, do_parts, probs_parts, ds_parts, dq_parts = [], [], [], [], []
            for h, mine in enumerate((first_head, jnp.logical_not(first_head))):
                q_parts.append(jnp.where(mine, q, jnp.zeros_like(q)))
                do_parts.append(jnp.where(mine, do, jnp.zeros_like(do)))
                lse = jnp.sum(jnp.where(lane == 2 * j + h, lse_ref[rows, :], 0.0), axis=-1, keepdims=True)
                delta = jnp.sum(jnp.where(mine, products, 0.0), axis=-1, keepdims=True)
                probs = jnp.exp(nt(q_parts[h], k) + (bias_ref[:, :keys] - lse))
                ds = (probs * (nt(do_parts[h], v) - delta)).astype(BF)
                probs_parts.append(probs.astype(BF))
                ds_parts.append(ds)
                dq_parts.append(nn(ds, k))
            res_ref[rows, lanes] = jnp.where(first_head, *dq_parts)
            res_ref[span, k_lanes] += tn(jnp.concatenate(ds_parts), jnp.concatenate(q_parts))
            dv_ref[span, lanes] += tn(jnp.concatenate(probs_parts), jnp.concatenate(do_parts))
            for n in range(cols // LANES):
                proceed(f"a{block}{n}", j == n)
            return carry

        lax.fori_loop(0, cols // LANES, pair, 0)

    for block in range(blocks):
        set_bias(block)
        attention_back(block)

    def lower(t, carry):
        rows = rows_of(t)
        for sub in range(TB // 64):
            cosine, sine, low_half = angle_block(tables, t * (TB // 64) + sub)
            at = pl.ds(pl.multiple_of(t * TB + sub * 64, 64), 64)
            for tile in range(cols // LANES):
                lanes = slice(tile * LANES, (tile + 1) * LANES)
                k_lanes = slice(cols + tile * LANES, cols + (tile + 1) * LANES)
                d_gate[at, lanes] = (rotate(res_ref[at, lanes], cosine, -sine, low_half) * SCALE).astype(BF)
                d_gate[at, k_lanes] = rotate(res_ref[at, k_lanes], cosine, -sine, low_half).astype(BF)
        d_up[rows, 0:cols] = dv_ref[rows, :].astype(BF)
        return carry

    lax.fori_loop(0, blocks, lower, 0)
    proceed("lower")

    def qkv(name, source, lanes_at):
        row = chunks[name][0]

        grad = tn(source[:, lanes_at : lanes_at + cols], normed1[...]).astype(BF)
        for o in range(8):
            slot = slot_of(name, o)[0]
            for piece in range(pieces):
                part = grad[o * low : (o + 1) * low, piece * LANES : (piece + 1) * LANES]
                pack[slot, pl.ds(row + piece * low, low), :] = part
        start(name, 0)
        proceed(name)

    qkv("value", d_up, 0)
    qkv("query", d_gate, 0)
    qkv("key", d_gate, cols)

    def down_product(j, carry):
        t = ((1 - core) * half_blocks + j) % blocks
        local = rows_of(t % half_blocks)
        down = nn(hidden[rows_of(t), :], wd[...])

        @pl.when(j < half_blocks)
        def _():
            out_send[local, :] = down.astype(BF)
            send_out(t % half_blocks).start()

        @pl.when(j >= half_blocks)
        def _():
            dn_keep[local, :] += down

        for n in range(blocks):
            proceed(f"d{n}", j == n)
        return carry

    lax.fori_loop(0, blocks, down_product, 0)

    def write_block(t, carry):
        local = rows_of(t)
        send_out(t).wait_recv()
        out_got[local, :] = (dn_keep[local, :] + out_got[local, :].astype(F32)).astype(BF)
        write_out(t).start()
        return carry

    lax.fori_loop(0, half_blocks, write_block, 0)

    def finish(j, carry):
        t = ((1 - core) * half_blocks + j) % blocks
        rows = rows_of(t)
        local = rows_of(t % half_blocks)
        is_own = t // half_blocks == core
        dn = nt(d_gate[rows, 0:cols], wq[...]) + nt(d_gate[rows, cols : 2 * cols], wk[...]) + nt(d_up[rows, 0:cols], wv[...])
        x = xs[rows, :].astype(F32)
        r = lax.rsqrt(jnp.mean(x * x, axis=-1, keepdims=True) + EPS)
        gains[1:2, :] += jnp.sum(dn * (x * r), axis=0, keepdims=True)

        @pl.when(is_own)
        def _():
            dn_keep[local, :] = dn

        @pl.when(jnp.logical_not(is_own))
        def _():
            send_out(t % half_blocks).wait_send()
            out_send[local, :] = dn.astype(BF)
            send_dn1(t % half_blocks).start()

        for n in range(blocks):
            proceed(f"f{n}", j == n)
        return carry

    lax.fori_loop(0, blocks, finish, 0)
    turned = jnp.transpose(gains[...])
    turned_low = turned.astype(BF)
    rest = turned - turned_low.astype(F32)
    both = jnp.where(lane < LANES // 2, turned, pltpu.roll(rest, LANES // 2, 1)).astype(BF)
    spread("gains", 0, both)
    start("gains", 0)
    proceed("gains")

    def input_part(t, carry):
        local = rows_of(t)
        send_dn1(t).wait_recv()
        dn = dn_keep[local, :] + dn_got[local, :].astype(F32)
        x = xs[rows_of(core * half_blocks + t), :].astype(F32)
        r = lax.rsqrt(jnp.mean(x * x, axis=-1, keepdims=True) + EPS)
        e = gain_one[...] * dn
        grad = d_res[local, :] + r * e - x * (r * r * r) * jnp.mean(e * x, axis=-1, keepdims=True)
        dn_got[local, :] = grad.astype(BF)
        write_grad(t).start()
        return carry

    lax.fori_loop(0, half_blocks, input_part, 0)
    proceed("inp")
    early = chunks["query"][5]
    steps = PLAN["end"]
    last = max([i + 1 for i, (name, step) in enumerate(steps) if step == 3 and chunks[name][5] < early], default=0)
    for name, step in steps[:last]:
        advance(name, step)
    send_final(0, 0, early).start()
    for name, step in steps[last:]:
        advance(name, step)
    rows_final = final.shape[1]
    send_final(1, early, rows_final - early).start()
    mine_out = load(0, final.at[core], final_out.at[0])
    mine_out.start()
    send_final(0, 0, early).wait_recv()
    early_out = load(1, final_got.at[pl.ds(0, early)], final_out.at[1, pl.ds(0, early)])
    early_out.start()
    for name in names:
        drain(name)
    send_x.wait_send()
    send_ids.wait_send()
    send_dy.wait_send()
    for t in range(blocks):
        send_att(t).wait_send()
        send_dn(t).wait_send()
    for t in range(half_blocks):
        write_out(t).wait()
        write_grad(t).wait()
        send_dn1(t).wait_send()
    send_final(0, 0, early).wait_send()
    send_final(1, early, rows_final - early).wait()
    late = pl.ds(early, rows_final - early)
    late_out = load(2, final_got.at[late], final_out.at[1, late])
    late_out.start()
    mine_out.wait()
    early_out.wait()
    late_out.wait()


def hand_out(
    final, block_out, input_grad,
    block_out_ref, input_grad_ref, gain_one, query, key, value, out, gain_two, gate, up, down,
):
    core = lax.axis_index("seq")
    taken = other_bit(bit(lax.axis_index("dp"), 3), core)
    width = block_out.shape[1]
    chunks, _, _ = layout_of(width, width // 2, down.shape[1] // 2)
    block_out_ref[...] = block_out[...]
    input_grad_ref[...] = input_grad[...]
    targets = {"query": query, "key": key, "value": value, "out": out, "gate": gate, "up": up, "down": down}
    for name, target in targets.items():
        _, _, kind, pieces, each, at = chunks[name]
        half = each // 2
        for p in range(pieces):
            rows = pl.ds(at + p * half, half)
            if kind == "B":
                target[:, p * LANES : (p + 1) * LANES] = final[taken, rows, :]
            else:
                for whose in range(2):
                    first = ((core if whose == 0 else 1 - core) * pieces + p) * LANES
                    target[:, pl.ds(pl.multiple_of(first, LANES), LANES)] = final[whose, rows, :]
    _, _, _, _, each, at = chunks["gains"]
    rows = pl.ds(at, each // 2)
    both = jnp.transpose(final[0, rows, :] + final[1, rows, :])
    gain_two[...] = (both[0:1] + both[LANES // 2 : LANES // 2 + 1]).reshape(each // 2)
    gain_one[...] = (both[1:2] + both[LANES // 2 + 1 : LANES // 2 + 2]).reshape(each // 2)


def fused_shards(
    tokens, segment_ids, norm1_gain, w_query, w_key, w_value, w_out, norm2_gain, w_gate, w_up, w_down, out_grad,
):
    seqs, half_tokens, width = tokens.shape
    length = 2 * half_tokens
    cols = w_query.shape[1] // 2
    ff = w_gate.shape[1] // 2
    chunks, rows, rows_final = layout_of(width, cols, ff)
    core = lax.axis_index("seq")
    chip = lax.axis_index("dp")
    tables = tuple(jnp.asarray(t) for t in small_tables(length))
    any_space = pl.BlockSpec(memory_space=pl.ANY)
    vmem = pl.BlockSpec(memory_space=pltpu.VMEM)

    def low(*dims):
        return pltpu.VMEM(dims, BF)

    def full(*dims):
        return pltpu.VMEM(dims, F32)

    scratch = [
        low(length, width), low(length, width), pltpu.VMEM((1, length), jnp.int32),
        low(width, cols), low(width, cols), low(width, cols), low(width, width), low(width, ff), low(width, ff), low(ff, width),
        low(length, width), low(length, cols), low(length, cols), low(length, cols), low(length, cols), low(length, cols),
        full(length, LANES), full(TB, 3 * TB), full(1, width), full(1, width),
        full(length, width), low(length, width), low(length, ff), low(length, ff), low(length, ff), low(length, width),
        low(length, width), full(half_tokens, width), low(half_tokens, width), low(half_tokens, width), full(length, cols),
        full(half_tokens, width), low(half_tokens, width),
        full(LANES, width), low(8, rows, LANES), low(4, rows, LANES), low(2, rows, LANES), low(1, rows, LANES), low(rows, LANES),
        full(rows, LANES), full(2, rows_final, LANES), full(rows_final, LANES),
        pltpu.SemaphoreType.DMA((10,)), pltpu.SemaphoreType.DMA((17,)), pltpu.SemaphoreType.DMA((17,)),
        pltpu.SemaphoreType.DMA((4 * len(chunks),)), pltpu.SemaphoreType.DMA((4 * len(chunks),)),
    ]
    block_out, input_grad, final = pl.pallas_call(
        block_kernel,
        out_shape=(shape(half_tokens, width), shape(half_tokens, width), shape(2, rows_final, LANES, dtype=F32)),
        in_specs=[any_space] * 10 + [vmem] * 6,
        out_specs=[any_space] * 3,
        scratch_shapes=scratch,
        compiler_params=pltpu.CompilerParams(
            vmem_limit_bytes=67043328, collective_id=0, has_side_effects=True,
        ),
        name="block",
    )(
        tokens.reshape(half_tokens, width), segment_ids.reshape(1, half_tokens), out_grad.reshape(half_tokens, width),
        w_query, w_key, w_value, w_out, w_gate, w_up, w_down,
        norm1_gain, norm2_gain, *tables,
    )
    columns, columns_ff = width // 32, ff // 16
    outs = [shape(half_tokens, width), shape(half_tokens, width)] + [
        shape(*dims, dtype=F32)
        for dims in (
            (columns,), (columns, width), (columns, width), (columns, width), (columns, width), (columns,),
            (columns_ff, width), (columns_ff, width), (columns, 2 * ff),
        )
    ]
    block_out, input_grad, *summed = pl.pallas_call(
        hand_out,
        out_shape=outs,
        in_specs=[vmem] * 3,
        out_specs=[vmem] * len(outs),
        name="hand_out",
    )(final, block_out, input_grad)
    summed = [a.T if a.ndim == 2 else a for a in summed]
    return (block_out.reshape(seqs, half_tokens, width), input_grad.reshape(seqs, half_tokens, width), *summed)


def solution(mesh):
    placed = (P("dp", "seq", None), P("dp", "seq"), *([P()] * 9), P("dp", "seq", None))
    column = P(None, AX)
    chips = mesh.shape["dp"]
    body = fused_shards if chips == 16 else functools.partial(shards, chips=chips)
    return jax.shard_map(
        body,
        mesh=mesh,
        in_specs=placed,
        out_specs=(
            P("dp", "seq", None), P("dp", "seq", None), P(AX), column, column, column, column, P(AX), column, column, column,
        ),
        check_vma=False,
    )
```

```python
import functools

import jax
import jax.numpy as jnp
import numpy as np
from jax import lax
from jax.experimental import pallas as pl
from jax.experimental.pallas import tpu as pltpu
from jax.sharding import PartitionSpec as P

HD = 64
EPS = 1e-06
SCALE = 0.125
NEG = -1e30
BASE = 10000.0
AX = ("dp", "seq")
BF = jnp.bfloat16
F32 = jnp.float32
TB = 256
LANES = 128


def nn(a, b):
    return lax.dot_general(a, b, (((1,), (0,)), ((), ())), preferred_element_type=F32)


def nt(a, b):
    return lax.dot_general(a, b, (((1,), (1,)), ((), ())), preferred_element_type=F32)


def tn(a, b):
    return lax.dot_general(a, b, (((0,), (0,)), ((), ())), preferred_element_type=F32)


def small_tables(length):
    freqs = BASE ** (-np.arange(HD // 2, dtype=np.float64) * (2.0 / HD))
    lane_freqs = np.tile(freqs, 4)[None, :]
    fine = np.arange(64, dtype=np.float64)[:, None] * lane_freqs
    coarse = 64.0 * np.arange(length // 64, dtype=np.float64)[:, None] * lane_freqs
    return tuple(
        np.asarray(t, np.float32) for t in (np.cos(fine), np.sin(fine), np.cos(coarse), np.sin(coarse))
    )


def angle_block(tables, sub):
    cos_f, sin_f, cos_c, sin_c = tables
    ca = cos_c[pl.ds(sub, 1), :]
    sa = sin_c[pl.ds(sub, 1), :]
    cb = cos_f[...]
    sb = sin_f[...]
    low_half = (lax.broadcasted_iota(jnp.int32, (64, LANES), 1) % HD) < HD // 2
    cosine = ca * cb - sa * sb
    sine = sa * cb + ca * sb
    return cosine, jnp.where(low_half, -sine, sine), low_half


def rotate(v, cosine, sine, low_half):
    partner = jnp.where(low_half, pltpu.roll(v, LANES - HD // 2, 1), pltpu.roll(v, HD // 2, 1))
    return v * cosine + partner * sine


def window(block):
    return max(0, (block - 2) * TB)


def bias_of(seg_col, seg_row, block):
    first = window(block)
    keys = (block + 1) * TB - first
    rows = seg_col[pl.ds(block * TB, TB), :]
    cols = seg_row[:, pl.ds(first, keys)]
    q_at = block * TB + lax.broadcasted_iota(jnp.int32, (TB, keys), 0)
    k_at = first + lax.broadcasted_iota(jnp.int32, (TB, keys), 1)
    return jnp.where((rows == cols) & (k_at <= q_at), 0.0, NEG).astype(F32)


def forward_attention(
    core, own_ref, other_ref, gain_ref, wq_ref, wk_ref, wv_ref, cos_f, sin_f, cos_c, sin_c, seg_col, seg_row,
    normed_ref, q_ref, k_ref, v_ref, att_ref, lse_ref, bias_ref,
):
    s = core[0]
    half_tokens, width = own_ref.shape
    length = 2 * half_tokens
    cols = wq_ref.shape[1]
    tables = (cos_f, sin_f, cos_c, sin_c)

    def project(t, carry):
        rows = pl.ds(pl.multiple_of(t * TB, TB), TB)
        part = t // (half_tokens // TB)
        local = pl.ds(pl.multiple_of((t % (half_tokens // TB)) * TB, TB), TB)
        x = jnp.where(part == s, own_ref[local, :], other_ref[local, :]).astype(F32)
        r = lax.rsqrt(jnp.mean(x * x, axis=-1, keepdims=True) + EPS)
        normed = (x * r * gain_ref[...]).astype(BF)
        normed_ref[rows, :] = normed
        v_ref[rows, :] = nn(normed, wv_ref[...]).astype(BF)
        q = nn(normed, wq_ref[...]).astype(BF).astype(F32)
        k = nn(normed, wk_ref[...]).astype(BF).astype(F32)
        for sub in range(TB // 64):
            cosine, sine, low_half = angle_block(tables, t * (TB // 64) + sub)
            at = pl.ds(pl.multiple_of(t * TB + sub * 64, 64), 64)
            for tile in range(cols // LANES):
                lanes = slice(tile * LANES, (tile + 1) * LANES)
                part_rows = slice(sub * 64, (sub + 1) * 64)
                q_ref[at, lanes] = (rotate(q[part_rows, lanes], cosine, sine, low_half).astype(BF) * BF(SCALE)).astype(BF)
                k_ref[at, lanes] = rotate(k[part_rows, lanes], cosine, sine, low_half).astype(BF)
        return carry

    lax.fori_loop(0, length // TB, project, 0)

    for block in range(length // TB):
        first = window(block)
        keys = (block + 1) * TB - first
        bias_ref[:, :keys] = bias_of(seg_col, seg_row, block)
        rows = pl.ds(block * TB, TB)
        span = pl.ds(first, keys)

        def head(h, carry):
            lanes = pl.ds(pl.multiple_of((h // 2) * LANES, LANES), LANES)
            lane = lax.broadcasted_iota(jnp.int32, (1, LANES), 1)
            mine = (lane // HD) == (h % 2)
            q = q_ref[rows, lanes]
            qm = jnp.where(mine, q, jnp.zeros_like(q))
            scores = nt(qm, k_ref[span, lanes]) + bias_ref[:, :keys]
            peak = jnp.max(scores, axis=-1, keepdims=True)
            weights = jnp.exp(scores - peak)
            total = jnp.sum(weights, axis=-1, keepdims=True)
            probs = (weights * (1.0 / total)).astype(BF)
            result = nn(probs, v_ref[span, lanes]).astype(BF)
            att_ref[rows, lanes] = jnp.where(mine, result, att_ref[rows, lanes])
            lse_ref[rows, :] = jnp.where(lane == h, peak + jnp.log(total), lse_ref[rows, :])
            return carry

        lax.fori_loop(0, cols // HD, head, 0)


def feed_forward(
    core, slots_a, slots_b, own_ref, other_ref, att_own, att_other, gain_ref, wo_ref, wg_ref, wu_ref, wd_ref,
    dy_own, dy_other,
    res_ref, out_keep, out_send, dn_ref, pack_ref, normed, hidden, d_gate, d_up, dy_all,
):
    s = core[0]
    half_tokens, width = own_ref.shape
    length = 2 * half_tokens
    cols = att_own.shape[1]
    own_rows = pl.ds(pl.multiple_of(s * cols, cols), cols)
    other_rows = pl.ds(pl.multiple_of((1 - s) * cols, cols), cols)

    def block(t, carry):
        rows = pl.ds(pl.multiple_of(t * TB, TB), TB)
        part = t // (half_tokens // TB)
        local = pl.ds(pl.multiple_of((t % (half_tokens // TB)) * TB, TB), TB)
        is_own = part == s
        x = jnp.where(is_own, own_ref[local, :], other_ref[local, :]).astype(F32)
        dy = jnp.where(is_own, dy_own[local, :], dy_other[local, :])
        dy_all[rows, :] = dy
        residual = x + (nn(att_own[rows, :], wo_ref[own_rows, :]) + nn(att_other[rows, :], wo_ref[other_rows, :]))
        res_ref[rows, :] = residual
        r = lax.rsqrt(jnp.mean(residual * residual, axis=-1, keepdims=True) + EPS)
        n2 = (residual * r * gain_ref[...]).astype(BF)
        normed[rows, :] = n2
        gate = nn(n2, wg_ref[...])
        up = nn(n2, wu_ref[...])
        sig = 1.0 / (1.0 + jnp.exp(-gate))
        act = gate * sig
        hid = (act * up).astype(BF)
        hidden[rows, :] = hid
        down = nn(hid, wd_ref[...])

        @pl.when(is_own)
        def _():
            out_keep[local, :] = residual + down

        @pl.when(jnp.logical_not(is_own))
        def _():
            out_send[local, :] = down.astype(BF)

        d_hidden = nt(dy, wd_ref[...])
        dg = (d_hidden * up * (sig * (1.0 + gate * (1.0 - sig)))).astype(BF)
        du = (d_hidden * act).astype(BF)
        d_gate[rows, :] = dg
        d_up[rows, :] = du
        dn_ref[rows, :] = (nt(dg, wg_ref[...]) + nt(du, wu_ref[...])).astype(BF)
        return carry

    lax.fori_loop(0, length // TB, block, 0)

    wide = wg_ref.shape[1] // 8
    pieces = width // LANES

    def gate_up(o, carry):
        cut = pl.ds(pl.multiple_of(o * wide, wide), wide)
        slot = slots_b[o]
        for which, source in ((0, d_gate), (1, d_up)):
            grad = tn(source[:, cut], normed[...]).astype(BF)
            for piece in range(pieces):
                pack_ref[slot, pl.ds((which * pieces + piece) * wide, wide), :] = grad[:, piece * LANES : (piece + 1) * LANES]
        return carry

    lax.fori_loop(0, 8, gate_up, 0)
    low = width // 16
    base = 2 * pieces * wide
    deep = hidden.shape[1] // LANES
    for piece in range(deep):
        grad = tn(dy_all[...], hidden[:, piece * LANES : (piece + 1) * LANES]).astype(BF)
        for o in range(16):
            slot = slots_a[o]
            at = pl.multiple_of(base + (slot % 2) * (deep * low) + piece * low, 16)
            pack_ref[slot // 2, pl.ds(at, low), :] = grad[o * low : (o + 1) * low, :]


def backward_attention(
    core, slots_a, slots_b, own_ref, other_ref, gain_one, gain_two, wq_ref, wk_ref, wv_ref, wo_ref, dy_own, dy_other,
    res_ref, dn_own, dn_other, att_ref, normed_ref, q_ref, k_ref, v_ref, lse_ref, cos_f, sin_f, cos_c, sin_c, seg_col, seg_row,
    d_res, dn_keep, dn_send, pack_ref, d_branch, d_att, dq, dk, dv, dq_low, dk_low, dv_low, gains, bias_ref,
):
    s = core[0]
    half_tokens, width = own_ref.shape
    length = 2 * half_tokens
    cols = att_ref.shape[1]
    tables = (cos_f, sin_f, cos_c, sin_c)
    gains[...] = jnp.zeros_like(gains)

    def norm_two(t, carry):
        rows = pl.ds(pl.multiple_of(t * TB, TB), TB)
        part = t // (half_tokens // TB)
        local = pl.ds(pl.multiple_of((t % (half_tokens // TB)) * TB, TB), TB)
        is_own = part == s
        dy = jnp.where(is_own, dy_own[local, :], dy_other[local, :]).astype(F32)
        residual = res_ref[rows, :]
        dn = dn_own[rows, :].astype(F32) + dn_other[rows, :].astype(F32)
        r = lax.rsqrt(jnp.mean(residual * residual, axis=-1, keepdims=True) + EPS)
        scaled = residual * r
        e = gain_two[...] * dn
        gains[0:1, :] += jnp.sum(dn * scaled, axis=0, keepdims=True)
        grad = dy + r * (e - scaled * (r * jnp.mean(e * residual, axis=-1, keepdims=True)))
        low = grad.astype(BF)
        d_branch[rows, :] = low

        @pl.when(is_own)
        def _():
            d_res[local, :] = grad

        d_att[rows, :] = nt(low, wo_ref[...]).astype(BF)
        return carry

    lax.fori_loop(0, length // TB, norm_two, 0)

    dk[...] = jnp.zeros_like(dk)
    dv[...] = jnp.zeros_like(dv)
    for block in range(length // TB):
        first = window(block)
        keys = (block + 1) * TB - first
        bias_ref[:, :keys] = bias_of(seg_col, seg_row, block)
        rows = pl.ds(block * TB, TB)
        span = pl.ds(first, keys)

        def head(h, carry):
            lanes = pl.ds(pl.multiple_of((h // 2) * LANES, LANES), LANES)
            lane = lax.broadcasted_iota(jnp.int32, (1, LANES), 1)
            mine = (lane // HD) == (h % 2)
            q = q_ref[rows, lanes]
            qm = jnp.where(mine, q, jnp.zeros_like(q))
            do = d_att[rows, lanes]
            dom = jnp.where(mine, do, jnp.zeros_like(do))
            lse = jnp.sum(jnp.where(lane == h, lse_ref[rows, :], 0.0), axis=-1, keepdims=True)
            k = k_ref[span, lanes]
            probs = jnp.exp(nt(qm, k) + (bias_ref[:, :keys] - lse))
            d_probs = nt(dom, v_ref[span, lanes])
            delta = jnp.sum(probs * d_probs, axis=-1, keepdims=True)
            ds = (probs * (d_probs - delta)).astype(BF)
            part = nn(ds, k)
            dq[rows, lanes] = jnp.where(mine, part, dq[rows, lanes])
            dk[span, lanes] += tn(ds, qm)
            dv[span, lanes] += tn(probs.astype(BF), dom)
            return carry

        lax.fori_loop(0, cols // HD, head, 0)

    def finish(t, carry):
        rows = pl.ds(pl.multiple_of(t * TB, TB), TB)
        part = t // (half_tokens // TB)
        local = pl.ds(pl.multiple_of((t % (half_tokens // TB)) * TB, TB), TB)
        is_own = part == s
        for sub in range(TB // 64):
            cosine, sine, low_half = angle_block(tables, t * (TB // 64) + sub)
            at = pl.ds(pl.multiple_of(t * TB + sub * 64, 64), 64)
            for tile in range(cols // LANES):
                lanes = slice(tile * LANES, (tile + 1) * LANES)
                dq_low[at, lanes] = (rotate(dq[at, lanes], cosine, -sine, low_half) * SCALE).astype(BF)
                dk_low[at, lanes] = rotate(dk[at, lanes], cosine, -sine, low_half).astype(BF)
        dv_low[rows, :] = dv[rows, :].astype(BF)
        dn = nt(dq_low[rows, :], wq_ref[...]) + nt(dk_low[rows, :], wk_ref[...]) + nt(dv_low[rows, :], wv_ref[...])
        x = jnp.where(is_own, own_ref[local, :], other_ref[local, :]).astype(F32)
        r = lax.rsqrt(jnp.mean(x * x, axis=-1, keepdims=True) + EPS)
        gains[1:2, :] += jnp.sum(dn * (x * r), axis=0, keepdims=True)

        @pl.when(is_own)
        def _():
            dn_keep[local, :] = dn

        @pl.when(jnp.logical_not(is_own))
        def _():
            dn_send[local, :] = dn.astype(BF)

        return carry

    lax.fori_loop(0, length // TB, finish, 0)

    low = width // 16
    pieces = width // LANES
    for which, source in ((0, dq_low), (1, dk_low), (2, dv_low)):
        for piece in range(pieces):
            grad = tn(source[...], normed_ref[:, piece * LANES : (piece + 1) * LANES]).astype(BF)
            for o in range(8):
                at = (which * pieces + piece) * low
                pack_ref[slots_b[o], pl.ds(at, low), :] = grad[o * low : (o + 1) * low, :]
    turned = jnp.transpose(gains[...])
    turned_low = turned.astype(BF)
    rest = (turned - turned_low.astype(F32)).astype(BF)
    lane = lax.broadcasted_iota(jnp.int32, (1, LANES), 1)
    both = jnp.where(lane < LANES // 2, turned_low, pltpu.roll(rest.astype(F32), LANES // 2, 1).astype(BF))
    at_b = 3 * pieces * low
    size_a = (cols // LANES + 1) * low
    base = at_b + low
    for piece in range(cols // LANES):
        grad = tn(d_branch[...], att_ref[:, piece * LANES : (piece + 1) * LANES]).astype(BF)
        for o in range(16):
            slot = slots_a[o]
            at = pl.multiple_of(base + (slot % 2) * size_a + piece * low, 16)
            pack_ref[slot // 2, pl.ds(at, low), :] = grad[o * low : (o + 1) * low, :]
    for o in range(16):
        slot = slots_a[o]
        at = pl.multiple_of(base + (slot % 2) * size_a + (cols // LANES) * low, 16)
        pack_ref[slot // 2, pl.ds(at, low), :] = both[o * low : (o + 1) * low, :]

        @pl.when(s == o // 8)
        def _():
            pack_ref[slots_b[o % 8], pl.ds(at_b, low), :] = both[o * low : (o + 1) * low, :]


BIG = pltpu.CompilerParams(vmem_limit_bytes=60 * 1024 * 1024)


def shape(*dims, dtype=BF):
    return jax.ShapeDtypeStruct(dims, dtype)


def flat(dp, core):
    return 2 * dp + core


def swap_cores(chips):
    return [(flat(d, c), flat(d, 1 - c)) for d in range(chips) for c in range(2)]


ORDER = ((0, 1, 2, 3), (1, 0, 2, 3))


def swap_chips(step):
    return [(flat(d, c), flat(d ^ (1 << ORDER[c][step]), c)) for d in range(16) for c in range(2)]


def to_owner_half():
    return [(flat(d, c), flat(d ^ 8, c)) for d in range(16) for c in range(2) if d // 8 != c]


def slot_tables(chip, core, chips):
    if chips != 16:
        return jnp.arange(16, dtype=jnp.int32), jnp.arange(8, dtype=jnp.int32)
    owner = jnp.arange(16, dtype=jnp.int32)
    away = owner ^ chip
    x, y, z0, z1 = away & 1, (away >> 1) & 1, (away >> 2) & 1, (away >> 3) & 1
    first = jnp.where(core == 0, x, y)
    second = jnp.where(core == 0, y, x)
    slots_a = first * 8 + second * 4 + z0 * 2 + z1
    near = slots_a // 2
    return slots_a, jnp.where(core == 0, near[:8], near[8:])


def halve(pack):
    for step in range(3):
        half = pack.shape[0] // 2
        pack3 = pack.reshape(2, half, *pack.shape[1:])
        got = lax.ppermute(pack3[1], AX, swap_chips(step))
        total = pack3[0].astype(F32) + got.astype(F32)
        pack = total.astype(BF) if step < 2 else total
    return pack[0]


def last_step(total, size_b):
    kind_b = total[:size_b]
    kind_a = total[size_b:].reshape(2, -1, LANES)
    got_a = lax.ppermute(kind_a[1].astype(BF), AX, swap_chips(3))
    got_b = lax.ppermute(kind_b.astype(BF), AX, to_owner_half())
    return kind_a[0] + got_a.astype(F32), kind_b + got_b.astype(F32)


def shards(
    tokens, segment_ids, norm1_gain, w_query, w_key, w_value, w_out, norm2_gain, w_gate, w_up, w_down, out_grad,
    *, chips,
):
    seqs, half_tokens, width = tokens.shape
    length = 2 * half_tokens
    cols = w_query.shape[1] // 2
    ff = w_gate.shape[1] // 2
    core = lax.axis_index("seq")
    chip = lax.axis_index("dp")
    core_id = core.reshape(1).astype(jnp.int32)
    pairs = swap_cores(chips)
    own = tokens.reshape(half_tokens, width)
    dy_own = out_grad.reshape(half_tokens, width)
    ids = segment_ids.reshape(1, half_tokens)
    other = lax.ppermute(own, AX, pairs)
    ids_other = lax.ppermute(ids, AX, pairs)
    dy_other = lax.ppermute(dy_own, AX, pairs)
    seg_row = jnp.where(core == 0, jnp.concatenate([ids, ids_other], 1), jnp.concatenate([ids_other, ids], 1))
    seg_col = seg_row.reshape(length, 1)
    gain_one = norm1_gain.astype(F32).reshape(1, width)
    gain_two = norm2_gain.astype(F32).reshape(1, width)
    tables = tuple(jnp.asarray(t) for t in small_tables(length))
    slots_a, slots_b = slot_tables(chip, core, chips)
    half_w = pl.BlockSpec((width, cols), lambda g, c: (0, c[0]))
    half_wide = pl.BlockSpec((width, ff), lambda g, c, a, b: (0, c[0]))
    whole = lambda a: pl.BlockSpec(a.shape, lambda g, *_: (0,) * len(a.shape))

    def out_block(s):
        return pl.BlockSpec(s.shape, lambda g, *_: (0,) * len(s.shape))

    outs = (
        shape(length, width), shape(length, cols), shape(length, cols), shape(length, cols), shape(length, cols),
        shape(length, LANES, dtype=F32),
    )
    normed1, q, k, v, att, lse = pl.pallas_call(
        forward_attention,
        out_shape=outs,
        grid_spec=pltpu.PrefetchScalarGridSpec(
            num_scalar_prefetch=1,
            grid=(1,),
            in_specs=[whole(own), whole(other), whole(gain_one), half_w, half_w, half_w]
            + [whole(t) for t in tables]
            + [whole(seg_col), whole(seg_row)],
            out_specs=[out_block(o) for o in outs],
            scratch_shapes=[pltpu.VMEM((TB, 3 * TB), F32)],
        ),
        compiler_params=BIG,
        name="attention_forward",
    )(core_id, own, other, gain_one, w_query, w_key, w_value, *tables, seg_col, seg_row)
    att_other = lax.ppermute(att, AX, pairs)

    rows_one = 2 * (width // LANES) * (ff // 8) + 2 * (ff // LANES) * (width // 16)
    outs = (
        shape(length, width, dtype=F32), shape(half_tokens, width, dtype=F32), shape(half_tokens, width),
        shape(length, width), shape(8, rows_one, LANES),
    )
    residual, out_keep, out_send, dn, pack_one = pl.pallas_call(
        feed_forward,
        out_shape=outs,
        grid_spec=pltpu.PrefetchScalarGridSpec(
            num_scalar_prefetch=3,
            grid=(1,),
            in_specs=[whole(own), whole(other), whole(att), whole(att), whole(gain_two), whole(w_out), half_wide, half_wide,
                      pl.BlockSpec((ff, width), lambda g, c, a, b: (c[0], 0)), whole(own), whole(own)],
            out_specs=[out_block(o) for o in outs],
            scratch_shapes=[
                pltpu.VMEM((length, width), BF), pltpu.VMEM((length, ff), BF), pltpu.VMEM((length, ff), BF),
                pltpu.VMEM((length, ff), BF), pltpu.VMEM((length, width), BF),
            ],
        ),
        compiler_params=BIG,
        name="feed_forward",
    )(core_id, slots_a, slots_b, own, other, att, att_other, gain_two, w_out, w_gate, w_up, w_down, dy_own, dy_other)
    out_other = lax.ppermute(out_send, AX, pairs)
    block_out = (out_keep + out_other.astype(F32)).astype(BF)
    dn_other = lax.ppermute(dn, AX, pairs)

    low = width // 16
    size_b2 = 3 * (width // LANES) * low + low
    size_a2 = (cols // LANES + 1) * low
    outs = (
        shape(half_tokens, width, dtype=F32), shape(half_tokens, width, dtype=F32), shape(half_tokens, width),
        shape(8, size_b2 + 2 * size_a2, LANES),
    )
    half_w3 = pl.BlockSpec((width, cols), lambda g, c, a, b: (0, c[0]))
    inputs = (own, other, gain_one, gain_two, w_query, w_key, w_value, w_out, dy_own, dy_other, residual, dn, dn_other,
              att, normed1, q, k, v, lse, *tables, seg_col, seg_row)
    specs = [whole(a) for a in inputs]
    specs[4] = specs[5] = specs[6] = half_w3
    specs[7] = pl.BlockSpec((cols, width), lambda g, c, a, b: (c[0], 0))
    d_res, dn_keep, dn_send, pack_two = pl.pallas_call(
        backward_attention,
        out_shape=outs,
        grid_spec=pltpu.PrefetchScalarGridSpec(
            num_scalar_prefetch=3,
            grid=(1,),
            in_specs=specs,
            out_specs=[out_block(o) for o in outs],
            scratch_shapes=[
                pltpu.VMEM((length, width), BF), pltpu.VMEM((length, cols), BF),
                pltpu.VMEM((length, cols), F32), pltpu.VMEM((length, cols), F32), pltpu.VMEM((length, cols), F32),
                pltpu.VMEM((length, cols), BF), pltpu.VMEM((length, cols), BF), pltpu.VMEM((length, cols), BF),
                pltpu.VMEM((LANES, width), F32), pltpu.VMEM((TB, 3 * TB), F32),
            ],
        ),
        compiler_params=BIG,
        name="attention_backward",
    )(core_id, slots_a, slots_b, *inputs)
    dn1 = dn_keep + lax.ppermute(dn_send, AX, pairs).astype(F32)
    x = own.astype(F32)
    r = lax.rsqrt(jnp.mean(x * x, axis=-1, keepdims=True) + EPS)
    e = gain_one * dn1
    input_grad = (d_res + r * e - x * (r * r * r) * jnp.mean(e * x, axis=-1, keepdims=True)).astype(BF)

    pieces = width // LANES
    wide = ff // 8
    size_b1 = 2 * pieces * wide
    size_a1 = (ff // LANES) * low

    if chips == 16:
        one_a, one_b = last_step(halve(pack_one), size_b1)
        two_a, two_b = last_step(halve(pack_two), size_b2)
        holds = (chip >> 3) == core

        def share(a):
            parts = a.reshape(a.shape[0], 2, a.shape[1] // 2, LANES)
            mine = jnp.where(core == 0, parts[:, 0], parts[:, 1])
            theirs = jnp.where(core == 0, parts[:, 1], parts[:, 0])
            return mine, lax.ppermute(theirs, AX, pairs)

        def both(a):
            mine, got = share(a)
            return jnp.where(core == 0, mine, got), jnp.where(core == 0, got, mine)

        def one(a):
            mine, got = share(a)
            return jnp.where(holds, mine, got)

        down_lo, down_hi = both(one_a.reshape(ff // LANES, low, LANES))
        kind_a = two_a.reshape(cols // LANES + 1, low, LANES)
        out_lo, out_hi = both(kind_a)
        gates = one(one_b.reshape(2 * pieces, wide, LANES))
        rest = one(two_b.reshape(3 * pieces + 1, low, LANES))

        def turn(a):
            return jnp.transpose(a, (0, 2, 1)).reshape(-1, a.shape[1])

        tiles = cols // LANES
        gain1 = out_lo[tiles] + out_hi[tiles]
        gain1 = gain1[:, 1] + gain1[:, 1 + LANES // 2]
        gain2 = rest[3 * pieces]
        gain2 = gain2[:, 0] + gain2[:, LANES // 2]
        summed = (
            gain1,
            turn(rest[:pieces]),
            turn(rest[pieces : 2 * pieces]),
            turn(rest[2 * pieces : 3 * pieces]),
            turn(jnp.concatenate([out_lo[:tiles], out_hi[:tiles]])),
            gain2,
            turn(gates[:pieces]),
            turn(gates[pieces:]),
            turn(jnp.concatenate([down_lo, down_hi])),
        )
    else:
        def plain_b(rows, count, size, at):
            part = rows[:, at : at + count * size].reshape(8, count, size, LANES)
            part = jnp.transpose(part, (1, 3, 0, 2)).reshape(count * LANES, 8 * size).astype(F32)
            zero = jnp.zeros_like(part)
            return jnp.where(core == 0, jnp.concatenate([part, zero], 1), jnp.concatenate([zero, part], 1))

        def plain_a(rows, count, at, each):
            part = rows[:, at:].reshape(8, 2, each, low, LANES)[:, :, :count].reshape(16, count, low, LANES)
            part = jnp.transpose(part, (1, 3, 0, 2)).reshape(count * LANES, 16 * low).astype(F32)
            zero = jnp.zeros_like(part)
            return jnp.where(core == 0, jnp.concatenate([part, zero], 0), jnp.concatenate([zero, part], 0))

        def scatter(a):
            return lax.psum_scatter(a, AX, scatter_dimension=1, tiled=True)

        tiles = cols // LANES
        gain_a = pack_two[:, size_b2:].reshape(16, tiles + 1, low, LANES)[:, tiles].astype(F32)
        gain_a = gain_a[:, :, : LANES // 2] + gain_a[:, :, LANES // 2 :]
        gain_a = gain_a.reshape(width, LANES // 2)
        gain1 = gain_a[:, 1].reshape(1, width)
        gain2 = jnp.where(core == 0, gain_a[:, 0], 0.0).reshape(1, width)
        n = pieces * low
        summed = (
            scatter(gain1).reshape(-1),
            scatter(plain_b(pack_two, pieces, low, 0)),
            scatter(plain_b(pack_two, pieces, low, n)),
            scatter(plain_b(pack_two, pieces, low, 2 * n)),
            scatter(plain_a(pack_two, tiles, size_b2, tiles + 1)),
            scatter(gain2).reshape(-1),
            scatter(plain_b(pack_one, pieces, wide, 0)),
            scatter(plain_b(pack_one, pieces, wide, pieces * wide)),
            scatter(plain_a(pack_one, ff // LANES, size_b1, ff // LANES)),
        )
    return (block_out.reshape(seqs, half_tokens, width), input_grad.reshape(seqs, half_tokens, width), *summed)


MESH = pl.DeviceIdType.MESH


PLAN = {
    "u0": (("down", 0),),
    "a01": (("gate0", 0),),
    "a10": (("up0", 0),),
    "a20": (("down", 1),),
    "a30": (("up0", 1), ("gate1", 0), ("up1", 0),),
    "lower": (("down", 2), ("out", 0),),
    "query": (("up0", 2),),
    "key": (("up1", 1), ("gate0", 1),),
    "f1": (("out", 1),),
    "f2": (("down", 3),),
    "f3": (("gate0", 2), ("gate1", 1),),
    "gains": (("up0", 3),),
    "d1": (("value", 0),),
    "d2": (("query", 0),),
    "inp": (("gate0", 3), ("up1", 2), ("gate1", 2), ("out", 2),),
    "end": (("gains", 0), ("key", 0), ("query", 1), ("up1", 3), ("value", 1), ("gains", 1), ("gate1", 3), ("key", 1), ("query", 2), ("value", 2), ("out", 3), ("gains", 2), ("key", 2), ("query", 3), ("value", 3), ("gains", 3), ("key", 3),),
}
Z_FIRST = ("gate0", "gate1", "value", "gains",)


def bit(value, place):
    return (value // (1 << place)) % 2


def other_bit(a, b):
    return a + b - 2 * a * b


def layout_of(width, cols, ff):
    low, wide = width // 16, ff // 8
    table, row, final = {}, 0, 0
    for name, kind, pieces, each in (
        ("gate0", "B", width // LANES // 2, wide), ("gate1", "B", width // LANES // 2, wide),
        ("up0", "B", width // LANES // 2, wide), ("up1", "B", width // LANES // 2, wide), ("down", "A", ff // LANES, low),
        ("out", "A", cols // LANES, low), ("query", "B", width // LANES, low), ("key", "B", width // LANES, low),
        ("value", "B", width // LANES, low), ("gains", "A", 1, low),
    ):
        rows = pieces * each * (2 if kind == "A" else 1)
        table[name] = (row, rows, kind, pieces, each, final)
        row, final = row + rows, final + pieces * each // 2
    return table, row, final


def block_kernel(
    x_hbm, ids_hbm, dy_hbm, wq_hbm, wk_hbm, wv_hbm, wo_hbm, wg_hbm, wu_hbm, wd_hbm, gain_one_low, gain_two_low,
    cos_f, sin_f, cos_c, sin_c,
    block_out, input_grad, final_out,
    xs, dys, ids, wq, wk, wv, wo, wg, wu, wd, normed1, q_ref, k_ref, v_ref, att, att_other, lse_ref, bias_ref,
    gain_one, gain_two, res_ref, normed2, hidden, d_gate, d_up, dn_own, dn_other, d_res, out_send, out_got, dv_ref, dn_keep, dn_got,
    gains, pack, got1, got2, got3, got4, acc, final, final_got,
    load_sem, pair_send, pair_recv, hop_send, hop_recv,
):
    core = lax.axis_index("seq")
    chip = lax.axis_index("dp")
    half_tokens, width = x_hbm.shape
    length = 2 * half_tokens
    cols = wq.shape[1]
    ff = wg.shape[1]
    blocks = length // TB
    half_blocks = half_tokens // TB
    tables = (cos_f, sin_f, cos_c, sin_c)
    chunks, _, _ = layout_of(width, cols, ff)
    names = list(chunks)
    low = width // 16

    bx, by, bz, bw = (bit(chip, i) for i in range(4))
    step_x, step_y = 1 - 2 * bx, 2 * (1 - 2 * by)
    near = chip + (1 - core) * step_x + core * step_y
    aside = chip + core * step_x + (1 - core) * step_y
    above = chip + 4 * (1 - 2 * bz)
    across = chip + 8 * (1 - 2 * bw)
    partners = (near, aside, above, across)
    holds = bw == core

    def path_of(name):
        return (above, near, aside, across) if name in Z_FIRST else partners

    def slot_of(name, owner):
        kx, ky, kz = other_bit(bx, owner & 1), other_bit(by, (owner >> 1) & 1), other_bit(bz, (owner >> 2) & 1)
        first = (1 - core) * kx + core * ky
        second = core * kx + (1 - core) * ky
        slot = kz * 4 + first * 2 + second if name in Z_FIRST else first * 4 + second * 2 + kz
        return slot, other_bit(bw, (owner >> 3) & 1)

    def owner_of(name, first, second, third):
        if name in Z_FIRST:
            first, second, third = second, third, first
        kx = (1 - core) * first + core * second
        ky = core * first + (1 - core) * second
        return other_bit(bx, kx) + 2 * other_bit(by, ky) + 4 * other_bit(bz, third)

    barrier = pltpu.get_barrier_semaphore()
    everyone = [{"dp": chip, "seq": 1 - core}] + [{"dp": p, "seq": core} for p in partners]
    for device in everyone:
        pl.semaphore_signal(barrier, inc=1, device_id=device, device_id_type=MESH)

    own_rows = pl.ds(pl.multiple_of(core * half_tokens, half_tokens), half_tokens)
    own_cols = pl.ds(pl.multiple_of(core * cols, cols), cols)
    own_ff = pl.ds(pl.multiple_of(core * ff, ff), ff)

    def load(i, src, dst):
        return pltpu.make_async_copy(src, dst, load_sem.at[i])

    loads = [
        load(0, x_hbm, xs.at[own_rows]),
        load(1, wv_hbm.at[:, own_cols], wv),
        load(2, wq_hbm.at[:, own_cols], wq),
        load(3, wk_hbm.at[:, own_cols], wk),
        load(4, ids_hbm, ids.at[:, own_rows]),
        load(5, wo_hbm, wo),
        load(6, wg_hbm.at[:, own_ff], wg),
        load(7, wu_hbm.at[:, own_ff], wu),
        load(8, wd_hbm.at[own_ff, :], wd),
        load(9, dy_hbm, dys.at[own_rows]),
    ]
    for copy in loads[:5]:
        copy.start()

    def to_pair(i, src, dst):
        return pltpu.make_async_remote_copy(
            src_ref=src, dst_ref=dst, send_sem=pair_send.at[i], recv_sem=pair_recv.at[i],
            device_id={"dp": chip, "seq": 1 - core}, device_id_type=MESH,
        )

    send_x = to_pair(0, x_hbm, xs.at[own_rows])
    send_ids = to_pair(1, ids_hbm, ids.at[:, own_rows])
    send_dy = to_pair(2, dy_hbm, dys.at[own_rows])

    def rows_of(t):
        return pl.ds(pl.multiple_of(t * TB, TB), TB)

    def send_att(t):
        return to_pair(3 + t, att.at[rows_of(t)], att_other.at[rows_of(t)])

    def send_dn(t):
        return to_pair(7 + t, dn_own.at[rows_of(t)], dn_other.at[rows_of(t)])

    def send_out(t):
        return to_pair(11 + t, out_send.at[rows_of(t)], out_got.at[rows_of(t)])

    def send_dn1(t):
        return to_pair(13 + t, out_send.at[rows_of(t)], dn_got.at[rows_of(t)])

    def write_out(t):
        return pltpu.make_async_copy(out_got.at[rows_of(t)], block_out.at[rows_of(t)], load_sem.at[3 + t])

    def write_grad(t):
        return pltpu.make_async_copy(dn_got.at[rows_of(t)], input_grad.at[rows_of(t)], load_sem.at[5 + t])

    def send_final(i, first, count):
        rows = pl.ds(first, count)
        return to_pair(15 + i, final.at[1 - core, rows], final_got.at[rows])


    def hop(name, step):
        row, count, kind = chunks[name][:3]
        at = 4 * names.index(name) + step
        rows = pl.ds(row, count)
        if step < 3:
            n = 4 >> step
            src, dst = pack.at[pl.ds(n, n), rows], (got1, got2, got3)[step].at[:, rows]
        elif kind == "B":
            src, dst = pack.at[0, rows], got4.at[rows]
        else:
            src, dst = pack.at[0, pl.ds(row + count // 2, count // 2)], got4.at[pl.ds(row, count // 2)]
        return pltpu.make_async_remote_copy(
            src_ref=src, dst_ref=dst, send_sem=hop_send.at[at], recv_sem=hop_recv.at[at],
            device_id={"dp": path_of(name)[step], "seq": core}, device_id_type=MESH,
        )

    def start(name, step):
        if step == 3 and chunks[name][2] == "B":
            @pl.when(jnp.logical_not(holds))
            def _():
                hop(name, step).start()
        else:
            hop(name, step).start()

    def advance(name, step):
        row, count, kind, pieces, each, at = chunks[name]
        if step < 3:
            hop(name, step).wait_recv()
            n = 4 >> step
            size = 384 if count % 384 == 0 else (288 if count % 288 == 0 else count)
            source = (got1, got2, got3)[step]
            per = count // size

            def add(i, carry):
                slab = i // per
                rows = pl.ds(pl.multiple_of(row + (i % per) * size, 16), size)
                total = pack[slab, rows, :].astype(F32) + source[slab, rows, :].astype(F32)
                pack[slab, rows, :] = total.astype(BF)
                if step == 2:
                    acc[rows, :] = total
                return carry

            lax.fori_loop(0, n * per, add, 0)
            start(name, step + 1)
            return
        half = each // 2
        if kind == "B":
            @pl.when(holds)
            def _():
                hop(name, step).wait_recv()
                for p in range(pieces):
                    for c in range(2):
                        rows = pl.ds(row + p * each + c * half, half)
                        final[c, pl.ds(at + p * half, half), :] = acc[rows, :] + got4[rows, :].astype(F32)

            @pl.when(jnp.logical_not(holds))
            def _():
                hop(name, step).wait_send()
                for p in range(pieces):
                    for c in range(2):
                        final[c, pl.ds(at + p * half, half), :] = acc[pl.ds(row + p * each + c * half, half), :]
        else:
            hop(name, step).wait_recv()
            for p in range(pieces):
                for c in range(2):
                    rows = pl.ds(row + p * each + c * half, half)
                    final[c, pl.ds(at + p * half, half), :] = acc[rows, :] + got4[rows, :].astype(F32)

    def proceed(point, here=None):
        steps = PLAN.get(point, ())
        if not steps:
            return
        if here is None:
            for name, step in steps:
                advance(name, step)
            return

        @pl.when(here)
        def _():
            for name, step in steps:
                advance(name, step)

    def drain(name):
        for step in range(3):
            hop(name, step).wait_send()
        if chunks[name][2] == "A":
            hop(name, 3).wait_send()


    gain_one[...] = gain_one_low[...].astype(F32).reshape(1, width)
    gain_two[...] = gain_two_low[...].astype(F32).reshape(1, width)
    pl.semaphore_wait(barrier, len(everyone))
    send_x.start()
    send_ids.start()
    for copy in loads[:4]:
        copy.wait()
    for copy in loads[5:]:
        copy.start()
    send_dy.start()

    def project(j, carry):
        t = (core + j) % 2

        @pl.when(j == 1)
        def _():
            send_x.wait_recv()

        rows = pl.ds(pl.multiple_of(t * half_tokens, half_tokens), half_tokens)
        x = xs[rows, :].astype(F32)
        r = lax.rsqrt(jnp.mean(x * x, axis=-1, keepdims=True) + EPS)
        normed = (x * r * gain_one[...]).astype(BF)
        normed1[rows, :] = normed
        v_ref[rows, :] = nn(normed, wv[...]).astype(BF)
        q = nn(normed, wq[...]).astype(BF).astype(F32)
        k = nn(normed, wk[...]).astype(BF).astype(F32)
        for sub in range(half_tokens // 64):
            cosine, sine, low_half = angle_block(tables, t * (half_tokens // 64) + sub)
            at = pl.ds(pl.multiple_of(t * half_tokens + sub * 64, 64), 64)
            for tile in range(cols // LANES):
                lanes = slice(tile * LANES, (tile + 1) * LANES)
                part = slice(sub * 64, (sub + 1) * 64)
                q_ref[at, lanes] = (rotate(q[part, lanes], cosine, sine, low_half).astype(BF) * BF(SCALE)).astype(BF)
                k_ref[at, lanes] = rotate(k[part, lanes], cosine, sine, low_half).astype(BF)
        return carry

    lax.fori_loop(0, 2, project, 0)
    loads[4].wait()
    send_ids.wait_recv()
    lse_ref[...] = jnp.transpose(jnp.broadcast_to(ids[...].astype(F32), (LANES, length)))

    def set_bias(block):
        first = window(block)
        keys = (block + 1) * TB - first
        rows = lse_ref[pl.ds(block * TB, TB), LANES - 1 :]
        columns = ids[:, pl.ds(first, keys)].astype(F32)
        q_at = block * TB + lax.broadcasted_iota(jnp.int32, (TB, keys), 0)
        k_at = first + lax.broadcasted_iota(jnp.int32, (TB, keys), 1)
        bias_ref[:, :keys] = jnp.where((rows == columns) & (k_at <= q_at), 0.0, NEG).astype(F32)

    lane = lax.broadcasted_iota(jnp.int32, (1, LANES), 1)
    first_head = lane < HD
    for block in range(blocks):
        first = window(block)
        keys = (block + 1) * TB - first
        set_bias(block)
        rows = pl.ds(block * TB, TB)
        span = pl.ds(first, keys)

        def pair(j, carry, rows=rows, span=span, keys=keys):
            lanes = pl.ds(pl.multiple_of(j * LANES, LANES), LANES)
            q, k, v = q_ref[rows, lanes], k_ref[span, lanes], v_ref[span, lanes]
            results, sums = [], []
            for mine in (first_head, jnp.logical_not(first_head)):
                scores = nt(jnp.where(mine, q, jnp.zeros_like(q)), k) + bias_ref[:, :keys]
                peak = jnp.max(scores, axis=-1, keepdims=True)
                weights = jnp.exp(scores - peak)
                total = jnp.sum(weights, axis=-1, keepdims=True)
                results.append(nn(weights.astype(BF), v) * (1.0 / total))
                sums.append(peak + jnp.log(total))
            att[rows, lanes] = jnp.where(first_head, *results).astype(BF)
            old = jnp.where(lane == 2 * j + 1, sums[1], lse_ref[rows, :])
            lse_ref[rows, :] = jnp.where(lane == 2 * j, sums[0], old)
            return carry

        lax.fori_loop(0, cols // LANES, pair, 0)
        send_att(block).start()


    for copy in loads[5:]:
        copy.wait()
    send_dy.wait_recv()
    other_cols = pl.ds(pl.multiple_of((1 - core) * cols, cols), cols)

    def feed(t, carry):
        rows = pl.ds(pl.multiple_of(t * half_tokens, half_tokens), half_tokens)
        for n in range(half_blocks):
            send_att(t * half_blocks + n).wait_recv()
        x = xs[rows, :].astype(F32)
        residual = x + (nn(att[rows, :], wo[own_cols, :]) + nn(att_other[rows, :], wo[other_cols, :]))
        res_ref[rows, :] = residual

        @pl.when(t == core)
        def _():
            dn_keep[...] = residual

        r = lax.rsqrt(jnp.mean(residual * residual, axis=-1, keepdims=True) + EPS)
        n2 = (residual * r * gain_two[...]).astype(BF)
        normed2[rows, :] = n2
        gate = nn(n2, wg[...])
        up = nn(n2, wu[...])
        hidden[rows, :] = (gate * (1.0 / (1.0 + jnp.exp(-gate))) * up).astype(BF)
        d_gate[rows, :] = gate.astype(BF)
        d_up[rows, :] = up.astype(BF)
        return carry

    lax.fori_loop(0, 2, feed, 0)

    def spread(name, piece, grad):
        row, rows = chunks[name][:2]
        for o in range(16):
            slot, far = slot_of(name, o)
            at = pl.multiple_of(row + far * (rows // 2) + piece * low, 16)
            pack[slot, pl.ds(at, low), :] = grad[o * low : (o + 1) * low, :]

    def down_part(part, carry):
        at = part * (ff // 2)
        grad = tn(dys[...], hidden[:, pl.ds(pl.multiple_of(at, LANES), ff // 2)]).astype(BF)
        for piece in range(ff // 2 // LANES):
            spread("down", part * (ff // 2 // LANES) + piece, grad[:, piece * LANES : (piece + 1) * LANES])
        return carry

    lax.fori_loop(0, 2, down_part, 0)
    start("down", 0)

    def feed_back(t, carry):
        rows = rows_of(t)
        gate = d_gate[rows, :].astype(F32)
        up = d_up[rows, :].astype(F32)
        sig = 1.0 / (1.0 + jnp.exp(-gate))
        d_hidden = nt(dys[rows, :], wd[...])
        dg = (d_hidden * up * (sig * (1.0 + gate * (1.0 - sig)))).astype(BF)
        du = (d_hidden * (gate * sig)).astype(BF)
        d_gate[rows, :] = dg
        d_up[rows, :] = du
        dn_own[rows, :] = (nt(dg, wg[...]) + nt(du, wu[...])).astype(BF)
        send_dn(t).start()
        for n in range(blocks):
            proceed(f"fb{n}", t == n)
        return carry

    lax.fori_loop(0, blocks, feed_back, 0)

    wide = ff // 8
    pieces = width // LANES

    def gate_up(name, source, first):
        cuts = []
        for j in range(4):
            owner = owner_of(name + "0", first, j // 2, j % 2)
            cuts.append(source[:, pl.ds(pl.multiple_of(owner * wide, wide), wide)])
        grad = tn(jnp.concatenate(cuts, axis=1), normed2[...]).astype(BF)
        for j in range(4):
            for piece in range(pieces):
                part = grad[j * wide : (j + 1) * wide, piece * LANES : (piece + 1) * LANES]
                row = chunks[f"{name}{piece // (pieces // 2)}"][0] + piece % (pieces // 2) * wide
                pack[4 * first + j, pl.ds(row, wide), :] = part

    gate_up("gate", d_gate, 1)
    start("gate0", 0)
    start("gate1", 0)
    proceed("g1")
    gate_up("gate", d_gate, 0)
    proceed("g0")
    gate_up("up", d_up, 1)
    start("up0", 0)
    start("up1", 0)
    proceed("u1")
    gate_up("up", d_up, 0)
    proceed("u0")


    d_branch, d_att = normed2, att_other
    gains[...] = jnp.zeros_like(gains)

    def norm_two(t, carry):
        rows = rows_of(t)
        local = rows_of(t % half_blocks)
        is_own = t // half_blocks == core
        send_dn(t).wait_recv()
        dy = dys[rows, :].astype(F32)
        residual = res_ref[rows, :]
        dn = dn_own[rows, :].astype(F32) + dn_other[rows, :].astype(F32)
        r = lax.rsqrt(jnp.mean(residual * residual, axis=-1, keepdims=True) + EPS)
        scaled = residual * r
        e = gain_two[...] * dn
        grad = dy + r * (e - scaled * (r * jnp.mean(e * residual, axis=-1, keepdims=True)))
        small = grad.astype(BF)
        d_branch[rows, :] = small
        d_att[rows, :] = nt(small, wo[own_cols, :]).astype(BF)

        @pl.when(is_own)
        def _():
            gains[0:1, :] += jnp.sum(dn * scaled, axis=0, keepdims=True)
            d_res[local, :] = grad

        for n in range(blocks):
            proceed(f"n{n}", t == n)
        return carry

    lax.fori_loop(0, blocks, norm_two, 0)

    out_grad = tn(d_branch[...], att[...]).astype(BF)
    for piece in range(cols // LANES):
        spread("out", piece, out_grad[:, piece * LANES : (piece + 1) * LANES])
    start("out", 0)
    proceed("out")

    res_ref[:, cols:] = jnp.zeros((length, cols), F32)
    dv_ref[...] = jnp.zeros_like(dv_ref)

    def attention_back(block):
        first = window(block)
        keys = (block + 1) * TB - first
        rows = pl.ds(block * TB, TB)
        span = pl.ds(first, keys)

        def pair(j, carry):
            at = pl.multiple_of(j * LANES, LANES)
            lanes = pl.ds(at, LANES)
            k_lanes = pl.ds(pl.multiple_of(cols + at, LANES), LANES)
            q, do, k, v = q_ref[rows, lanes], d_att[rows, lanes], k_ref[span, lanes], v_ref[span, lanes]
            products = do.astype(F32) * att[rows, lanes].astype(F32)
            q_parts, do_parts, probs_parts, ds_parts, dq_parts = [], [], [], [], []
            for h, mine in enumerate((first_head, jnp.logical_not(first_head))):
                q_parts.append(jnp.where(mine, q, jnp.zeros_like(q)))
                do_parts.append(jnp.where(mine, do, jnp.zeros_like(do)))
                lse = jnp.sum(jnp.where(lane == 2 * j + h, lse_ref[rows, :], 0.0), axis=-1, keepdims=True)
                delta = jnp.sum(jnp.where(mine, products, 0.0), axis=-1, keepdims=True)
                probs = jnp.exp(nt(q_parts[h], k) + (bias_ref[:, :keys] - lse))
                ds = (probs * (nt(do_parts[h], v) - delta)).astype(BF)
                probs_parts.append(probs.astype(BF))
                ds_parts.append(ds)
                dq_parts.append(nn(ds, k))
            res_ref[rows, lanes] = jnp.where(first_head, *dq_parts)
            res_ref[span, k_lanes] += tn(jnp.concatenate(ds_parts), jnp.concatenate(q_parts))
            dv_ref[span, lanes] += tn(jnp.concatenate(probs_parts), jnp.concatenate(do_parts))
            for n in range(cols // LANES):
                proceed(f"a{block}{n}", j == n)
            return carry

        lax.fori_loop(0, cols // LANES, pair, 0)

    for block in range(blocks):
        set_bias(block)
        attention_back(block)

    def lower(t, carry):
        rows = rows_of(t)
        for sub in range(TB // 64):
            cosine, sine, low_half = angle_block(tables, t * (TB // 64) + sub)
            at = pl.ds(pl.multiple_of(t * TB + sub * 64, 64), 64)
            for tile in range(cols // LANES):
                lanes = slice(tile * LANES, (tile + 1) * LANES)
                k_lanes = slice(cols + tile * LANES, cols + (tile + 1) * LANES)
                d_gate[at, lanes] = (rotate(res_ref[at, lanes], cosine, -sine, low_half) * SCALE).astype(BF)
                d_gate[at, k_lanes] = rotate(res_ref[at, k_lanes], cosine, -sine, low_half).astype(BF)
        d_up[rows, 0:cols] = dv_ref[rows, :].astype(BF)
        return carry

    lax.fori_loop(0, blocks, lower, 0)
    proceed("lower")

    def qkv(name, source, lanes_at):
        row = chunks[name][0]

        grad = tn(source[:, lanes_at : lanes_at + cols], normed1[...]).astype(BF)
        for o in range(8):
            slot = slot_of(name, o)[0]
            for piece in range(pieces):
                part = grad[o * low : (o + 1) * low, piece * LANES : (piece + 1) * LANES]
                pack[slot, pl.ds(row + piece * low, low), :] = part
        start(name, 0)
        proceed(name)

    qkv("value", d_up, 0)
    qkv("query", d_gate, 0)
    qkv("key", d_gate, cols)

    def finish(j, carry):
        t = ((1 - core) * half_blocks + j) % blocks
        rows = rows_of(t)
        local = rows_of(t % half_blocks)
        is_own = t // half_blocks == core
        dn = nt(d_gate[rows, 0:cols], wq[...]) + nt(d_gate[rows, cols : 2 * cols], wk[...]) + nt(d_up[rows, 0:cols], wv[...])
        x = xs[rows, :].astype(F32)
        r = lax.rsqrt(jnp.mean(x * x, axis=-1, keepdims=True) + EPS)
        gains[1:2, :] += jnp.sum(dn * (x * r), axis=0, keepdims=True)

        @pl.when(is_own)
        def _():
            res_ref[rows, :] = dn

        @pl.when(jnp.logical_not(is_own))
        def _():
            out_send[local, :] = dn.astype(BF)
            send_dn1(t % half_blocks).start()

        for n in range(blocks):
            proceed(f"f{n}", j == n)
        return carry

    lax.fori_loop(0, blocks, finish, 0)
    turned = jnp.transpose(gains[...])
    turned_low = turned.astype(BF)
    rest = turned - turned_low.astype(F32)
    both = jnp.where(lane < LANES // 2, turned, pltpu.roll(rest, LANES // 2, 1)).astype(BF)
    spread("gains", 0, both)
    start("gains", 0)
    proceed("gains")

    def down_product(j, carry):
        t = ((1 - core) * half_blocks + j) % blocks
        local = rows_of(t % half_blocks)
        down = nn(hidden[rows_of(t), :], wd[...])

        @pl.when(j < half_blocks)
        def _():
            send_dn1(t % half_blocks).wait_send()
            out_send[local, :] = down.astype(BF)
            send_out(t % half_blocks).start()

        @pl.when(j >= half_blocks)
        def _():
            dn_keep[local, :] += down

        for n in range(blocks):
            proceed(f"d{n}", j == n)
        return carry

    lax.fori_loop(0, blocks, down_product, 0)

    def input_part(t, carry):
        local = rows_of(t)
        send_dn1(t).wait_recv()
        dn = res_ref[rows_of(core * half_blocks + t), :] + dn_got[local, :].astype(F32)
        x = xs[rows_of(core * half_blocks + t), :].astype(F32)
        r = lax.rsqrt(jnp.mean(x * x, axis=-1, keepdims=True) + EPS)
        e = gain_one[...] * dn
        grad = d_res[local, :] + r * e - x * (r * r * r) * jnp.mean(e * x, axis=-1, keepdims=True)
        dn_got[local, :] = grad.astype(BF)
        write_grad(t).start()
        return carry

    lax.fori_loop(0, half_blocks, input_part, 0)
    def write_block(t, carry):
        local = rows_of(t)
        send_out(t).wait_recv()
        out_got[local, :] = (dn_keep[local, :] + out_got[local, :].astype(F32)).astype(BF)
        write_out(t).start()
        return carry

    lax.fori_loop(0, half_blocks, write_block, 0)

    proceed("inp")
    early = chunks["query"][5]
    steps = PLAN["end"]
    last = max([i + 1 for i, (name, step) in enumerate(steps) if step == 3 and chunks[name][5] < early], default=0)
    for name, step in steps[:last]:
        advance(name, step)
    send_final(0, 0, early).start()
    for name, step in steps[last:]:
        advance(name, step)
    rows_final = final.shape[1]
    send_final(1, early, rows_final - early).start()
    mine_out = load(0, final.at[core], final_out.at[0])
    mine_out.start()
    send_final(0, 0, early).wait_recv()
    early_out = load(1, final_got.at[pl.ds(0, early)], final_out.at[1, pl.ds(0, early)])
    early_out.start()
    for name in names:
        drain(name)
    send_x.wait_send()
    send_ids.wait_send()
    send_dy.wait_send()
    for t in range(blocks):
        send_att(t).wait_send()
        send_dn(t).wait_send()
    for t in range(half_blocks):
        write_out(t).wait()
        write_grad(t).wait()
        send_out(t).wait_send()
    send_final(0, 0, early).wait_send()
    send_final(1, early, rows_final - early).wait()
    late = pl.ds(early, rows_final - early)
    late_out = load(2, final_got.at[late], final_out.at[1, late])
    late_out.start()
    mine_out.wait()
    early_out.wait()
    late_out.wait()


def hand_out(
    final, block_out, input_grad,
    block_out_ref, input_grad_ref, gain_one, query, key, value, out, gain_two, gate, up, down,
):
    core = lax.axis_index("seq")
    taken = other_bit(bit(lax.axis_index("dp"), 3), core)
    width = block_out.shape[1]
    chunks, _, _ = layout_of(width, width // 2, down.shape[1] // 2)
    block_out_ref[...] = block_out[...]
    input_grad_ref[...] = input_grad[...]
    half_pieces = width // LANES // 2
    targets = (
        ("query", query, 0), ("key", key, 0), ("value", value, 0), ("out", out, 0), ("down", down, 0),
        ("gate0", gate, 0), ("gate1", gate, half_pieces), ("up0", up, 0), ("up1", up, half_pieces),
    )
    for name, target, skipped in targets:
        _, _, kind, pieces, each, at = chunks[name]
        half = each // 2
        for p in range(pieces):
            rows = pl.ds(at + p * half, half)
            if kind == "B":
                target[:, (skipped + p) * LANES : (skipped + p + 1) * LANES] = final[taken, rows, :]
            else:
                for whose in range(2):
                    first = ((core if whose == 0 else 1 - core) * pieces + p) * LANES
                    target[:, pl.ds(pl.multiple_of(first, LANES), LANES)] = final[whose, rows, :]
    _, _, _, _, each, at = chunks["gains"]
    rows = pl.ds(at, each // 2)
    both = jnp.transpose(final[0, rows, :] + final[1, rows, :])
    gain_two[...] = (both[0:1] + both[LANES // 2 : LANES // 2 + 1]).reshape(each // 2)
    gain_one[...] = (both[1:2] + both[LANES // 2 + 1 : LANES // 2 + 2]).reshape(each // 2)


def fused_shards(
    tokens, segment_ids, norm1_gain, w_query, w_key, w_value, w_out, norm2_gain, w_gate, w_up, w_down, out_grad,
):
    seqs, half_tokens, width = tokens.shape
    length = 2 * half_tokens
    cols = w_query.shape[1] // 2
    ff = w_gate.shape[1] // 2
    chunks, rows, rows_final = layout_of(width, cols, ff)
    core = lax.axis_index("seq")
    chip = lax.axis_index("dp")
    tables = tuple(jnp.asarray(t) for t in small_tables(length))
    any_space = pl.BlockSpec(memory_space=pl.ANY)
    vmem = pl.BlockSpec(memory_space=pltpu.VMEM)

    def low(*dims):
        return pltpu.VMEM(dims, BF)

    def full(*dims):
        return pltpu.VMEM(dims, F32)

    scratch = [
        low(length, width), low(length, width), pltpu.VMEM((1, length), jnp.int32),
        low(width, cols), low(width, cols), low(width, cols), low(width, width), low(width, ff), low(width, ff), low(ff, width),
        low(length, width), low(length, cols), low(length, cols), low(length, cols), low(length, cols), low(length, cols),
        full(length, LANES), full(TB, 3 * TB), full(1, width), full(1, width),
        full(length, width), low(length, width), low(length, ff), low(length, ff), low(length, ff), low(length, width),
        low(length, width), full(half_tokens, width), low(half_tokens, width), low(half_tokens, width), full(length, cols),
        full(half_tokens, width), low(half_tokens, width),
        full(LANES, width), low(8, rows, LANES), low(4, rows, LANES), low(2, rows, LANES), low(1, rows, LANES), low(rows, LANES),
        full(rows, LANES), full(2, rows_final, LANES), full(rows_final, LANES),
        pltpu.SemaphoreType.DMA((10,)), pltpu.SemaphoreType.DMA((17,)), pltpu.SemaphoreType.DMA((17,)),
        pltpu.SemaphoreType.DMA((4 * len(chunks),)), pltpu.SemaphoreType.DMA((4 * len(chunks),)),
    ]
    block_out, input_grad, final = pl.pallas_call(
        block_kernel,
        out_shape=(shape(half_tokens, width), shape(half_tokens, width), shape(2, rows_final, LANES, dtype=F32)),
        in_specs=[any_space] * 10 + [vmem] * 6,
        out_specs=[any_space] * 3,
        scratch_shapes=scratch,
        compiler_params=pltpu.CompilerParams(
            vmem_limit_bytes=67043328, collective_id=0, has_side_effects=True,
        ),
        name="block",
    )(
        tokens.reshape(half_tokens, width), segment_ids.reshape(1, half_tokens), out_grad.reshape(half_tokens, width),
        w_query, w_key, w_value, w_out, w_gate, w_up, w_down,
        norm1_gain, norm2_gain, *tables,
    )
    columns, columns_ff = width // 32, ff // 16
    outs = [shape(half_tokens, width), shape(half_tokens, width)] + [
        shape(*dims, dtype=F32)
        for dims in (
            (columns,), (columns, width), (columns, width), (columns, width), (columns, width), (columns,),
            (columns_ff, width), (columns_ff, width), (columns, 2 * ff),
        )
    ]
    block_out, input_grad, *summed = pl.pallas_call(
        hand_out,
        out_shape=outs,
        in_specs=[vmem] * 3,
        out_specs=[vmem] * len(outs),
        name="hand_out",
    )(final, block_out, input_grad)
    summed = [a.T if a.ndim == 2 else a for a in summed]
    return (block_out.reshape(seqs, half_tokens, width), input_grad.reshape(seqs, half_tokens, width), *summed)


def solution(mesh):
    placed = (P("dp", "seq", None), P("dp", "seq"), *([P()] * 9), P("dp", "seq", None))
    column = P(None, AX)
    chips = mesh.shape["dp"]
    body = fused_shards if chips == 16 else functools.partial(shards, chips=chips)
    return jax.shard_map(
        body,
        mesh=mesh,
        in_specs=placed,
        out_specs=(
            P("dp", "seq", None), P("dp", "seq", None), P(AX), column, column, column, column, P(AX), column, column, column,
        ),
        check_vma=False,
    )
```
